32 devices in a mesh: seq: 32 (over z, y, x, core).
Axes of the slice: x: 2, y: 2, z: 4, core: 2. Of those that a mesh axis runs over, the one named last changes fastest.
Arguments:
- queries: bfloat16 [8192, 8, 128], P('seq'), may hold values from -132 to 132
- keys: bfloat16 [16384, 8, 128], P('seq'), may hold values from -6 to 6
- values: bfloat16 [16384, 8, 128], P('seq'), may hold values from -6 to 6
- routes: int32 [8192, 8], P('seq'), may hold values from 0 to 63, all different within a row; in each aligned block of 256 rows (0 to 255, 256 to 511, ...) at most 40 rows name the same one
Outputs:
- attended: bfloat16 [8192, 8, 128], P('seq')
The draws below stay inside these ranges and needn't reach their ends.
Inputs may be any that keep to these rules, and one draw needn't show every extreme that they name: `routes`: each row names 8 different heads; among the 256 rows of one device no head is named more than 40 times, a bound that some block reaches.
All inputs are finite; a program needn't handle non-finite values.
Results may differ from the reference program's by a relative error of at most 0.0065.
Values may be sent and summed in bfloat16 or wider, within the bound.
A program may use at most 64 MiB of HBM per device.

```python
import math
import jax
import jax.numpy as jnp
import numpy as np
from jax import lax

HEADS = 64
KV_HEADS = 8
HEAD_DIM = 128
ROUTED = 8
HOPS = 4
MOST = 40
QRY_DEV = 256
CTX_DEV = 512
CONTEXT = 16384
QUERIES = 8192


def base_keys(key):
    shards = CONTEXT // CTX_DEV
    normal_keys = jax.random.truncated_normal(jax.random.fold_in(key, 11), -6.0, 6.0, (shards, CTX_DEV, KV_HEADS, HEAD_DIM), jnp.float32)
    return normal_keys


def draw_keys(key, part):
    return base_keys(key).reshape(CONTEXT, KV_HEADS, HEAD_DIM).astype(jnp.bfloat16)


def draw_queries(key, part):
    shards = CONTEXT // CTX_DEV
    drawn = jax.random.truncated_normal(jax.random.fold_in(key, 13), -6.0, 6.0, (shards, QRY_DEV, ROUTED, HEAD_DIM), jnp.float32)
    return drawn.reshape(QUERIES, ROUTED, HEAD_DIM).astype(jnp.bfloat16)


def shard_levels(own_key, extent, cuts, least, high):
    factor_of, own = 1.0, jax.random.fold_in(own_key, 6)
    for axis_at, parts in cuts:
        steps = jnp.exp(jax.random.uniform(jax.random.fold_in(own, axis_at), (parts,), jnp.float32, least / len(cuts), high / len(cuts)))
        factor_of = factor_of * jnp.repeat(steps, extent[axis_at] // parts).reshape([-1 if axis == axis_at else 1 for axis in range(len(extent))])
    return factor_of


def shared_out(rng, own, number, rows, count, top, limit, slope):
    ranking = jax.random.permutation(rng, count)
    crowded, common = load_shares(count, rows * top, limit, slope, True), load_shares(count, rows * top, limit, slope, False)
    places = jnp.arange(count)

    def named(lengths, offset_by):
        used = int((lengths > 0).sum())
        fixed = max(1, used // 4)
        passed = fixed + (places - fixed + offset_by * (used - fixed)) % max(1, count - fixed)
        return jnp.zeros((count,), jnp.int32).at[ranking[jnp.where(places < fixed, places, passed)]].set(jnp.asarray(lengths, jnp.int32))

    lengths = jnp.where(number % 4 == 0, named(crowded, number // 4), named(common, number - number // 4 - 1))
    mixed = jax.random.permutation(jax.random.fold_in(own, 3), count)
    giver, receiver = mixed[0:count // 2 * 2:2], mixed[1:count // 2 * 2:2]
    margin = jnp.minimum(lengths[giver] - 1, limit - lengths[receiver]) // 2
    margin = jnp.where((giver == ranking[0]) | (receiver == ranking[0]) | (lengths[receiver] == 0), 0, jnp.maximum(margin, 0))
    passed = jax.random.randint(jax.random.fold_in(own, 4), (count // 2,), 0, 1 << 20) % (margin + 1)
    lengths = lengths.at[giver].add(-passed).at[receiver].add(passed)
    items = jnp.searchsorted(jnp.cumsum(lengths), jnp.arange(rows * top), side="right").astype(jnp.int32)
    listing = items.reshape(top, rows).T
    listing = listing[jax.random.permutation(jax.random.fold_in(own, 1), rows)]
    offset_by = jax.random.randint(jax.random.fold_in(own, 2), (rows, 1), 0, top)
    return jnp.take_along_axis(listing, (jnp.arange(top)[None, :] + offset_by) % top, axis=1)


def load_shares(count, total, bound, skew, full):
    loads = [(1 << 20) // math.isqrt(grade ** skew) + 1 for grade in range(1, count + 1)]
    largest = bound if full else min(bound, max(-(-total // count), total * loads[0] // sum(loads)))
    least = 1 if total - largest >= count - 1 else 0
    given, spare = [largest] + [least] * (count - 1), total - largest - least * (count - 1)
    while spare > 0:
        free = [i for i in range(1, count) if given[i] < largest] or [i for i in range(1, count) if given[i] < bound]
        mass, left = sum([loads[i] for i in free]), spare
        for i in free:
            addition = min(bound - given[i], max(1, left * loads[i] // mass), spare)
            given[i] = given[i] + addition
            spare = spare - addition
    return np.array(given)


def centred(own_key, shape, width, reach, pieces=(), held_as=jnp.bfloat16):
    loudness = shard_levels(own_key, shape, pieces, -0.22, 0.18) if pieces else 1.0
    values = jax.random.normal(own_key, shape, jnp.float32) * width * loudness
    return jnp.minimum(jnp.maximum(values, -reach), reach).astype(held_as)


def setup_inputs(seed: int = 0) -> dict:
    seeds = jax.random.split(jax.random.key(seed), 5)
    queries = draw_queries(jax.random.fold_in(seeds[4], 71), 0)
    keys = draw_keys(jax.random.fold_in(seeds[4], 71), 0)
    values = centred(seeds[2], (CONTEXT, KV_HEADS, HEAD_DIM), 1.0, 6.0, ((0, 32),))
    routes_keys = jax.random.split(jax.random.fold_in(seeds[3], 1), QUERIES // QRY_DEV)
    routes_turns = jax.random.permutation(jax.random.fold_in(seeds[3], 3), QUERIES // QRY_DEV)
    routes = jax.vmap(lambda own, number: shared_out(jax.random.fold_in(seeds[3], 2), own, number, QRY_DEV, HEADS, ROUTED, MOST, 2))(routes_keys, routes_turns).reshape((QUERIES, ROUTED))
    return {"queries": queries, "keys": keys, "values": values, "routes": routes}


def slot_index(routes_dev):
    flat_heads = routes_dev.reshape(-1)
    heads_all = jnp.arange(HEADS, dtype=jnp.int32)
    onehot = (flat_heads[:, None] == heads_all[None, :]).astype(jnp.int32)
    before = jnp.cumsum(onehot, axis=0) - onehot
    within = lax.optimization_barrier(jnp.sum(before * onehot, axis=1)).astype(jnp.int32)
    return (flat_heads * MOST + within).astype(jnp.int32)

def one_shard(arguments):
    device, query_dev, routes_dev, padded_keys, padded_values = arguments
    slots = slot_index(routes_dev)
    flat = query_dev.reshape(-1, HEAD_DIM)
    packed = jnp.zeros((HEADS * MOST, HEAD_DIM), jnp.float32).at[slots].set(flat.astype(jnp.float32))
    tokens_of = jnp.repeat(jnp.arange(QRY_DEV, dtype=jnp.int32), ROUTED)
    positions = jnp.zeros((HEADS * MOST,), jnp.int32).at[slots].set(tokens_of)
    packed = packed.reshape(KV_HEADS, -1, HEAD_DIM)
    positions = positions.reshape(KV_HEADS, -1)
    window = HOPS + 1
    start = (device * CTX_DEV).astype(jnp.int32)
    win_keys = lax.dynamic_slice_in_dim(padded_keys, start, window * CTX_DEV, 0).astype(jnp.float32)
    win_values = lax.dynamic_slice_in_dim(padded_values, start, window * CTX_DEV, 0).astype(jnp.float32)
    scores = jnp.einsum('gqd,kgd->gqk', packed, win_keys) / jnp.sqrt(jnp.float32(HEAD_DIM))
    column = jnp.arange(window * CTX_DEV, dtype=jnp.int32)
    shard_of = column // CTX_DEV
    inside = device - HOPS + shard_of >= 0
    offset = CTX_DEV - QRY_DEV
    causal = (shard_of < HOPS)[None, None, :] | ((column - HOPS * CTX_DEV)[None, None, :] <= (positions + offset)[:, :, None])
    allowed = inside[None, None, :] & causal
    scores = jnp.where(allowed, scores, jnp.float32(-1e+30))
    highest = lax.optimization_barrier(jnp.max(scores, axis=2))
    weights = jnp.where(allowed, jnp.exp(scores - highest[:, :, None]), jnp.float32(0.0))
    total = lax.optimization_barrier(jnp.sum(weights, axis=2))
    rounded = weights.astype(jnp.bfloat16).astype(jnp.float32)
    output = jnp.einsum('gqk,kgd->gqd', rounded, win_values) / total[:, :, None]
    output = output.astype(jnp.bfloat16).reshape(-1, HEAD_DIM)
    return output[slots].reshape(QRY_DEV, ROUTED, HEAD_DIM)

def reference(queries, keys, values, routes):
    shards = CONTEXT // CTX_DEV
    front = jnp.zeros((HOPS * CTX_DEV, KV_HEADS, HEAD_DIM), keys.dtype)
    padded_keys = jnp.concatenate([front, keys], axis=0)
    padded_values = jnp.concatenate([front, values], axis=0)
    query_all = queries.reshape(shards, QRY_DEV, ROUTED, HEAD_DIM)
    routes_all = routes.reshape(shards, QRY_DEV, ROUTED)
    devices = jnp.arange(shards, dtype=jnp.int32)
    result = lax.map(lambda item: one_shard((item[0], item[1], item[2], padded_keys, padded_values)), (devices, query_all, routes_all))
    return result.reshape(QUERIES, ROUTED, HEAD_DIM)
```

```python
import functools
import math

import jax
import jax.numpy as jnp
from jax import lax
from jax.experimental import pallas as pl
from jax.experimental.pallas import tpu as pltpu
from jax.sharding import PartitionSpec as P

HEADS = 64
MOST = 40
LANES = 128
LOW = -1e30
MESH = pl.DeviceIdType.MESH


def dot(a, b):
    return lax.dot_general(a, b, (((1,), (0,)), ((), ())), preferred_element_type=jnp.float32)


def dot_t(a, b):
    return lax.dot_general(a, b, (((1,), (1,)), ((), ())), preferred_element_type=jnp.float32)


def remote(src, dst, send, recv, device):
    return pltpu.make_async_remote_copy(
        src_ref=src, dst_ref=dst, send_sem=send, recv_sem=recv,
        device_id=(device,), device_id_type=MESH,
    )


def attend(q, k, v, scale, mask=None):
    s = dot_t(q, k) * scale
    if mask is not None:
        s = mask(s)
    top = jnp.max(s, axis=1, keepdims=True)
    p = jnp.exp2(s - top).astype(jnp.bfloat16)
    ones = jnp.ones(v.shape, jnp.bfloat16)
    both = dot(p, jnp.concatenate([v, ones], axis=1))
    width = v.shape[1]
    total = both[:, width:]
    return both[:, :width] / total, top + jnp.log2(total)


def squeeze(lse, padded):
    rows = lse.shape[0]
    return jnp.concatenate([lse, jnp.zeros((padded - rows, LANES), jnp.float32)], axis=0).T[:1]


def widen(row, rows):
    return jnp.concatenate([jnp.broadcast_to(row, (8, row.shape[1]))] * (LANES // 8), axis=0).T[:rows]


def merge(parts):
    top = functools.reduce(jnp.maximum, [lse for _, lse in parts])
    weights = [jnp.exp2(lse - top) for _, lse in parts]
    total = functools.reduce(jnp.add, weights)
    mixed = functools.reduce(jnp.add, [o.astype(jnp.float32) * w for (o, _), w in zip(parts, weights)])
    return mixed / total, top + jnp.log2(total)


def kernel(
    n, q_in, routes_t, k_hbm, v_hbm, out,
    raw, wide, rights, slot_rows, slots, q, pos, kall, vall,
    qc, qd, oa, la, oc, tc, od, ld, td, rx, sx, rc, sc, rd, sd, fin, acc,
    raw_sem, kv_send, kv_recv, qn_send, qd_send, qc_recv, qd_recv, relay_send,
    oc_send, tc_send, od_send, td_send,
    rx_recv, sx_recv, rc_recv, sc_recv, rd_recv, sd_recv,
):
    tokens, routed, width = q_in.shape
    groups, capacity, _ = q.shape
    context = kall.shape[2]
    padded = tc.shape[2]
    per_group = HEADS // groups
    chips = n // 2
    me = lax.axis_index("seq")
    c = me // 2
    k = me % 2
    partner = c * 2 + 1 - k
    even = c % 2 == 0
    odd = c % 2 == 1
    scale = jnp.float32(math.log2(math.e) / math.sqrt(width))
    below = c >= 2
    above = c + 2 < chips
    mate = jnp.where(even, c + 1, c - 1) * 2 + k
    feeds = jnp.logical_or(even, c + 1 < chips)
    down = (c - 2) * 2 + k
    up = (c + 2) * 2 + k

    barrier = pltpu.get_barrier_semaphore()

    def signal(device):
        pl.semaphore_signal(barrier, inc=1, device_id=(device,), device_id_type=MESH)

    signal(partner)
    signal(mate)

    @pl.when(below)
    def _():
        signal(down)

    @pl.when(above)
    def _():
        signal(up)

    raws = [pltpu.make_async_copy(a, raw.at[i], raw_sem.at[i]) for i, a in enumerate((k_hbm, v_hbm))]
    for one in raws:
        one.start()

    group_of = routes_t[...] // per_group
    group = lax.broadcasted_iota(jnp.int32, (groups, tokens), 0)
    hots = [(group_of[r : r + 1] == group).astype(jnp.float32) for r in range(routed)]
    count = functools.reduce(jnp.add, hots)
    row = lax.broadcasted_iota(jnp.int32, (tokens, tokens), 0)
    col = lax.broadcasted_iota(jnp.int32, (tokens, tokens), 1)
    upper = (row < col).astype(jnp.float32).astype(jnp.bfloat16)
    rank = dot(count.astype(jnp.bfloat16), upper) + (group * capacity).astype(jnp.float32)
    rows = []
    for r in range(routed):
        rows.append(jnp.sum(hots[r] * rank, axis=0, keepdims=True))
        rank = rank + hots[r]
    slot_all = jnp.concatenate(rows, axis=0)
    slot_rows[...] = slot_all
    slots[...] = jnp.concatenate([slot_all] * (LANES // routed), axis=0).T

    wide[pl.ds(0, tokens)] = q_in[...].astype(jnp.float32)
    token = lax.broadcasted_iota(jnp.int32, (tokens, width), 0).astype(jnp.float32).astype(jnp.bfloat16)
    for r in range(routed):
        rights[pl.ds(r * tokens, tokens), :width] = wide[pl.ds(0, tokens), r, :].astype(jnp.bfloat16)
        rights[pl.ds(r * tokens, tokens), width:] = token

    pl.semaphore_wait(barrier, 2 + below.astype(jnp.int32) + above.astype(jnp.int32))

    def query_down(g):
        return remote(q.at[g], qd.at[g], qd_send.at[g], qd_recv.at[g], down)

    def query_near(g):
        return remote(q.at[g], qc.at[g], qn_send.at[g], qc_recv.at[g], mate)

    place = lax.broadcasted_iota(jnp.int32, (capacity, tokens), 0).astype(jnp.float32)

    def pack(g, carry):
        at = (g * capacity).astype(jnp.float32)
        here = jnp.concatenate(
            [
                (place == slot_rows[r : r + 1] - at).astype(jnp.float32).astype(jnp.bfloat16)
                for r in range(routed)
            ],
            axis=1,
        )
        both = dot(here, rights[...])
        q[g] = both[:, :width].astype(jnp.bfloat16)
        pos[g] = both[:, width:]

        @pl.when(below)
        def _():
            query_down(g).start()

        @pl.when(odd)
        def _():
            query_near(g).start()

        return carry

    lax.fori_loop(0, groups, pack, 0)

    part = 128

    def turn(i, to):
        def body(s, carry):
            at = pl.multiple_of(s * part, part)
            wide[pl.ds(0, part)] = raw[i, pl.ds(at, part)].astype(jnp.float32)
            for g in range(groups):
                to[g, k, pl.ds(at, part), :] = wide[pl.ds(0, part), g, :].astype(jnp.bfloat16)
            return carry

        lax.fori_loop(0, context // part, body, 0)

    def kv_copy(i):
        a = (kall, vall)[i]
        return remote(a.at[:, k], a.at[:, k], kv_send.at[i], kv_recv.at[i], partner)

    def kv_arrival(i):
        a = (kall, vall)[i]
        return remote(a.at[:, 1 - k], a.at[:, 1 - k], kv_send.at[i], kv_recv.at[i], partner)

    for i, to in enumerate((kall, vall)):
        raws[i].wait()
        turn(i, to)
        kv_copy(i).start()
    for i in range(2):
        kv_arrival(i).wait_recv()

    column = lax.broadcasted_iota(jnp.int32, (capacity, tokens), 1).astype(jnp.float32)

    def all_of(a, g):
        return a[g].reshape(2 * context, width)

    def own(g, keys, values):
        limit = jnp.concatenate([pos[g]] * (tokens // LANES), axis=1)

        def mask(s):
            free = s.shape[1] - tokens
            tail = jnp.where(column <= limit, s[:, free:], jnp.float32(LOW))
            return jnp.concatenate([s[:, :free], tail], axis=1)

        oa[g], la[g] = attend(q[g], keys, values, scale, mask)

    def relay(g):
        return remote(qd.at[g], qc.at[g], relay_send.at[g], qc_recv.at[g], mate)

    def c_near(g):
        return (
            remote(oc.at[g], rc.at[g], oc_send.at[g], rc_recv.at[g], mate),
            remote(tc.at[g], sc.at[g], tc_send.at[g], sc_recv.at[g], mate),
        )

    def c_relay(g):
        return (
            remote(oc.at[g], rx.at[g], oc_send.at[g], rx_recv.at[g], mate),
            remote(tc.at[g], sx.at[g], tc_send.at[g], sx_recv.at[g], mate),
        )

    def d_copies(g):
        return (
            remote(od.at[g], rd.at[g], od_send.at[g], rd_recv.at[g], up),
            remote(td.at[g], sd.at[g], td_send.at[g], sd_recv.at[g], up),
        )

    def start(copies):
        for one in copies:
            one.start()

    lag, delay = 0, 4

    def step(i, carry):
        @pl.when(jnp.logical_and(i < groups, above))
        def _():
            remote(q.at[i], qd.at[i], qd_send.at[i], qd_recv.at[i], partner).wait_recv()

            @pl.when(even)
            def _():
                relay(i).start()

            def put(out, lse):
                od[i] = out.astype(jnp.bfloat16)
                ld[i] = lse

            @pl.when(k == 0)
            def _():
                put(*attend(qd[i], all_of(kall, i), all_of(vall, i), scale))

            @pl.when(k == 1)
            def _():
                put(*attend(qd[i], kall[i, 1], vall[i, 1], scale))

            @pl.when(odd)
            def _():
                td[i] = squeeze(ld[i], padded)
                start(d_copies(i))

        @pl.when(jnp.logical_and(jnp.logical_and(i >= lag, i < groups + lag), feeds))
        def _():
            g = i - lag
            remote(q.at[g], qc.at[g], qn_send.at[g], qc_recv.at[g], partner).wait_recv()
            o, lse = attend(qc[g], all_of(kall, g), all_of(vall, g), scale)
            oc[g] = o.astype(jnp.bfloat16)
            tc[g] = squeeze(lse, padded)

            @pl.when(even)
            def _():
                start(c_near(g))

            @pl.when(odd)
            def _():
                start(c_relay(g))

        @pl.when(i < groups)
        def _():
            @pl.when(k == 0)
            def _():
                own(i, kall[i, 0], vall[i, 0])

            @pl.when(k == 1)
            def _():
                own(i, all_of(kall, i), all_of(vall, i))

        @pl.when(jnp.logical_and(jnp.logical_and(i >= delay, even), above))
        def _():
            g = i - delay
            remote(oc.at[g], rx.at[g], oc_send.at[g], rx_recv.at[g], partner).wait_recv()
            remote(tc.at[g], sx.at[g], tc_send.at[g], sx_recv.at[g], partner).wait_recv()
            o, lse = merge([(od[g], ld[g]), (rx[g], widen(sx[g], capacity))])
            od[g] = o.astype(jnp.bfloat16)
            td[g] = squeeze(lse, padded)
            start(d_copies(g))

        return carry

    lax.fori_loop(0, groups + delay, step, 0)

    def absent(o, t):
        o[...] = jnp.zeros(o.shape, o.dtype)
        t[...] = jnp.full(t.shape, LOW, t.dtype)

    @pl.when(even)
    def _():
        absent(rc, sc)

    @pl.when(jnp.logical_not(below))
    def _():
        absent(rd, sd)

    def finish(g, carry):
        @pl.when(odd)
        def _():
            remote(oc.at[g], rc.at[g], oc_send.at[g], rc_recv.at[g], partner).wait_recv()
            remote(tc.at[g], sc.at[g], tc_send.at[g], sc_recv.at[g], partner).wait_recv()

        @pl.when(below)
        def _():
            remote(od.at[g], rd.at[g], od_send.at[g], rd_recv.at[g], partner).wait_recv()
            remote(td.at[g], sd.at[g], td_send.at[g], sd_recv.at[g], partner).wait_recv()

        parts = [
            (oa[g], la[g]), (rc[g], widen(sc[g], capacity)), (rd[g], widen(sd[g], capacity))
        ]
        fin[pl.ds(pl.multiple_of(g * capacity, 16), capacity), :] = merge(parts)[0].astype(jnp.bfloat16)
        return carry

    tile = 256
    tiles = groups * capacity // tile
    lane = lax.broadcasted_iota(jnp.int32, (tokens, tile), 1).astype(jnp.float32)
    done = 0
    stops = [2, 4, 6, 8] if groups == 8 else [groups]
    for s, stop in enumerate(stops):
        lax.fori_loop(stops[s - 1] if s else 0, stop, finish, 0)
        last = stop == groups
        upto = tiles if last else stop * capacity // tile
        for r in range(routed):
            slot = slots[:, r : r + 1]
            here = jnp.concatenate(
                [
                    (lane == slot - t * tile).astype(jnp.float32).astype(jnp.bfloat16)
                    for t in range(done, upto)
                ],
                axis=1,
            )
            part_sum = dot(here, fin[done * tile : upto * tile, :])
            total = part_sum if s == 0 else acc[r] + part_sum
            if last:
                wide[pl.ds(0, tokens), r, :] = total
            else:
                acc[r] = total
        done = upto
    out[...] = wide[pl.ds(0, tokens)].astype(jnp.bfloat16)

    for i in range(2):
        kv_copy(i).wait_send()

    def sent(there, make):
        @pl.when(there)
        def _():
            def body(g, carry):
                for one in make(g):
                    one.wait_send()
                return carry

            lax.fori_loop(0, groups, body, 0)

    sent(below, lambda g: (query_down(g),))
    sent(odd, lambda g: (query_near(g),))
    sent(jnp.logical_and(even, above), lambda g: (relay(g),))
    sent(above, d_copies)
    sent(even, c_near)
    sent(jnp.logical_and(odd, feeds), c_relay)


def shards(n, queries, keys, values, routes):
    tokens, routed, width = queries.shape
    context, groups, _ = keys.shape
    capacity = HEADS // groups * MOST
    padded = -(-capacity // LANES) * LANES
    vmem = pl.BlockSpec(memory_space=pltpu.VMEM)
    hbm = pl.BlockSpec(memory_space=pl.ANY)
    bf = lambda *shape: pltpu.VMEM(shape, jnp.bfloat16)
    f32 = lambda *shape: pltpu.VMEM(shape, jnp.float32)
    sem = lambda *shape: pltpu.SemaphoreType.DMA(shape)
    chunks = lambda: bf(groups, capacity, width)
    stats = lambda: f32(groups, 1, padded)
    full = lambda: f32(groups, capacity, width)
    return pl.pallas_call(
        functools.partial(kernel, n),
        out_shape=jax.ShapeDtypeStruct((tokens, routed, width), jnp.bfloat16),
        in_specs=[vmem, vmem, hbm, hbm],
        out_specs=vmem,
        scratch_shapes=[
            bf(2, context, groups, width), f32(tokens, groups, width), bf(routed * tokens, 2 * width),
            f32(routed, tokens), f32(tokens, LANES), chunks(), full(),
            bf(groups, 2, context, width), bf(groups, 2, context, width),
            chunks(), chunks(), full(), full(), chunks(), stats(), chunks(), full(), stats(),
            chunks(), stats(), chunks(), stats(), chunks(), stats(),
            bf(groups * capacity, width), f32(routed, tokens, width),
        ] + [sem(2)] * 3 + [sem(groups)] * 15,
        compiler_params=pltpu.CompilerParams(
            collective_id=0, has_side_effects=True, vmem_limit_bytes=60 * 1024 * 1024
        ),
        name="fused",
    )(queries, routes.T, keys, values)


def solution(mesh):
    n = mesh.shape["seq"]
    placed = (P("seq", None, None), P("seq", None, None), P("seq", None, None), P("seq", None))
    return jax.shard_map(
        functools.partial(shards, n),
        mesh=mesh,
        in_specs=placed,
        out_specs=P("seq", None, None),
        check_vma=False,
    )
```

```python
import functools
import math

import jax
import jax.numpy as jnp
from jax import lax
from jax.experimental import pallas as pl
from jax.experimental.pallas import tpu as pltpu
from jax.sharding import PartitionSpec as P

HEADS = 64
MOST = 40
LANES = 128
LOW = -1e30
MESH = pl.DeviceIdType.MESH


def dot(a, b):
    return lax.dot_general(a, b, (((1,), (0,)), ((), ())), preferred_element_type=jnp.float32)


def dot_t(a, b):
    return lax.dot_general(a, b, (((1,), (1,)), ((), ())), preferred_element_type=jnp.float32)


def remote(src, dst, send, recv, device):
    return pltpu.make_async_remote_copy(
        src_ref=src, dst_ref=dst, send_sem=send, recv_sem=recv,
        device_id=(device,), device_id_type=MESH,
    )


def attend(q, k, v, scale, mask=None):
    s = dot_t(q, k) * scale
    if mask is not None:
        s = mask(s)
    top = jnp.max(s, axis=1, keepdims=True)
    p = jnp.exp2(s - top).astype(jnp.bfloat16)
    ones = jnp.ones(v.shape, jnp.bfloat16)
    both = dot(p, jnp.concatenate([v, ones], axis=1))
    width = v.shape[1]
    total = both[:, width:]
    return both[:, :width] / total, top + jnp.log2(total)


def squeeze(lse, padded):
    rows = lse.shape[0]
    return jnp.concatenate([lse, jnp.zeros((padded - rows, LANES), jnp.float32)], axis=0).T[:1]


def widen(row, rows):
    return jnp.concatenate([jnp.broadcast_to(row, (8, row.shape[1]))] * (LANES // 8), axis=0).T[:rows]


def merge(parts):
    top = functools.reduce(jnp.maximum, [lse for _, lse in parts])
    weights = [jnp.exp2(lse - top) for _, lse in parts]
    total = functools.reduce(jnp.add, weights)
    mixed = functools.reduce(jnp.add, [o.astype(jnp.float32) * w for (o, _), w in zip(parts, weights)])
    return mixed / total, top + jnp.log2(total)


def kernel(
    n, q_in, routes_t, k_hbm, v_hbm, out,
    raw, wide, rights, slot_rows, slots, qq, pos, kall, vall,
    qc, op, lp, oc, tc, od, td, rx, sx, rc, sc, rd, sd, fin, acc,
    raw_sem, kv_send, kv_recv, qn_send, qd_send, qc_recv, qd_recv, relay_send,
    oc_send, tc_send, od_send, td_send,
    rx_recv, sx_recv, rc_recv, sc_recv, rd_recv, sd_recv,
):
    tokens, routed, width = q_in.shape
    groups, capacity = qq.shape[1:3]
    q, qd = qq.at[1], qq.at[0]
    context = kall.shape[2]
    padded = tc.shape[2]
    per_group = HEADS // groups
    chips = n // 2
    me = lax.axis_index("seq")
    c = me // 2
    k = me % 2
    partner = c * 2 + 1 - k
    even = c % 2 == 0
    odd = c % 2 == 1
    scale = jnp.float32(math.log2(math.e) / math.sqrt(width))
    below = c >= 2
    above = c + 2 < chips
    mate = jnp.where(even, c + 1, c - 1) * 2 + k
    feeds = jnp.logical_or(even, c + 1 < chips)
    down = (c - 2) * 2 + k
    up = (c + 2) * 2 + k

    barrier = pltpu.get_barrier_semaphore()

    def signal(device):
        pl.semaphore_signal(barrier, inc=1, device_id=(device,), device_id_type=MESH)

    signal(partner)
    signal(mate)

    @pl.when(below)
    def _():
        signal(down)

    @pl.when(above)
    def _():
        signal(up)

    raws = [pltpu.make_async_copy(a, raw.at[i], raw_sem.at[i]) for i, a in enumerate((k_hbm, v_hbm))]
    for one in raws:
        one.start()

    group_of = routes_t[...] // per_group
    group = lax.broadcasted_iota(jnp.int32, (groups, tokens), 0)
    hots = [(group_of[r : r + 1] == group).astype(jnp.float32) for r in range(routed)]
    count = functools.reduce(jnp.add, hots)
    row = lax.broadcasted_iota(jnp.int32, (tokens, tokens), 0)
    col = lax.broadcasted_iota(jnp.int32, (tokens, tokens), 1)
    upper = (row < col).astype(jnp.float32).astype(jnp.bfloat16)
    rank = dot(count.astype(jnp.bfloat16), upper) + (group * capacity).astype(jnp.float32)
    rows = []
    for r in range(routed):
        rows.append(jnp.sum(hots[r] * rank, axis=0, keepdims=True))
        rank = rank + hots[r]
    slot_all = jnp.concatenate(rows, axis=0)
    slot_rows[...] = slot_all
    slots[...] = jnp.concatenate([slot_all] * (LANES // routed), axis=0).T

    wide[pl.ds(0, tokens * routed), :] = q_in[...].astype(jnp.float32).reshape(tokens * routed, width)
    token = lax.broadcasted_iota(jnp.int32, (tokens, width), 0).astype(jnp.float32).astype(jnp.bfloat16)
    for r in range(routed):
        rights[pl.ds(r * tokens, tokens), :width] = wide[pl.ds(r, tokens, stride=routed), :].astype(jnp.bfloat16)
        rights[pl.ds(r * tokens, tokens), width:] = token

    pl.semaphore_wait(barrier, 2 + below.astype(jnp.int32) + above.astype(jnp.int32))

    def query_down(g):
        return remote(q.at[g], qd.at[g], qd_send.at[g], qd_recv.at[g], down)

    def query_near(g):
        return remote(q.at[g], qc.at[g], qn_send.at[g], qc_recv.at[g], mate)

    place = lax.broadcasted_iota(jnp.int32, (capacity, tokens), 0).astype(jnp.float32)

    def pack(g, carry):
        at = (g * capacity).astype(jnp.float32)
        here = jnp.concatenate(
            [
                (place == slot_rows[r : r + 1] - at).astype(jnp.float32).astype(jnp.bfloat16)
                for r in range(routed)
            ],
            axis=1,
        )
        both = dot(here, rights[...])
        q[g] = both[:, :width].astype(jnp.bfloat16)
        pos[g] = both[:, width:]

        @pl.when(below)
        def _():
            query_down(g).start()

        @pl.when(odd)
        def _():
            query_near(g).start()

        return carry

    lax.fori_loop(0, groups, pack, 0)

    part = 128

    def turn(i, to):
        def body(s, carry):
            at = pl.multiple_of(s * part, part)
            wide[pl.ds(0, part * groups), :] = raw[i, pl.ds(at, part)].astype(jnp.float32).reshape(part * groups, width)
            for g in range(groups):
                to[g, k, pl.ds(at, part), :] = wide[pl.ds(g, part, stride=groups), :].astype(jnp.bfloat16)
            return carry

        lax.fori_loop(0, context // part, body, 0)

    def kv_copy(i):
        a = (kall, vall)[i]
        return remote(a.at[:, k], a.at[:, k], kv_send.at[i], kv_recv.at[i], partner)

    def kv_arrival(i):
        a = (kall, vall)[i]
        return remote(a.at[:, 1 - k], a.at[:, 1 - k], kv_send.at[i], kv_recv.at[i], partner)

    for i, to in enumerate((kall, vall)):
        raws[i].wait()
        turn(i, to)
        kv_copy(i).start()
    for i in range(2):
        kv_arrival(i).wait_recv()

    column = lax.broadcasted_iota(jnp.int32, (capacity, tokens), 1).astype(jnp.float32)

    def all_of(a, g):
        return a[g].reshape(2 * context, width)

    def masked(bias):
        def of(g):
            limit = jnp.concatenate([pos[g] + bias] * (tokens // LANES), axis=1)

            def mask(x):
                free = x.shape[1] - tokens
                tail = jnp.where(column <= limit, x[:, free:], jnp.float32(LOW))
                return jnp.concatenate([x[:, :free], tail], axis=1)

            return mask

        return of

    first = masked(jnp.where(k == 1, jnp.float32(0), jnp.float32(2 * tokens)))
    second = masked(jnp.where(k == 0, jnp.float32(0), jnp.float32(2 * tokens)))

    def both_shards(g):
        return attend(qq[k, g], all_of(kall, g), all_of(vall, g), scale, first(g))

    def one_shard(g):
        return attend(qq[1 - k, g], kall[g, k], vall[g, k], scale, second(g))

    def nearer(g):
        return attend(qc[g], all_of(kall, g), all_of(vall, g), scale)

    def relay(g):
        return remote(qd.at[g], qc.at[g], relay_send.at[g], qc_recv.at[g], mate)

    def c_near(g):
        return (
            remote(oc.at[g], rc.at[g], oc_send.at[g], rc_recv.at[g], mate),
            remote(tc.at[g], sc.at[g], tc_send.at[g], sc_recv.at[g], mate),
        )

    def c_relay(g):
        return (
            remote(oc.at[g], rx.at[g], oc_send.at[g], rx_recv.at[g], mate),
            remote(tc.at[g], sx.at[g], tc_send.at[g], sx_recv.at[g], mate),
        )

    def d_copies(g):
        return (
            remote(od.at[g], rd.at[g], od_send.at[g], rd_recv.at[g], up),
            remote(td.at[g], sd.at[g], td_send.at[g], sd_recv.at[g], up),
        )

    def start(copies):
        for one in copies:
            one.start()

    @pl.when(jnp.logical_not(above))
    def _():
        qq[0] = jnp.zeros(qq.shape[1:], qq.dtype)

    @pl.when(jnp.logical_not(feeds))
    def _():
        qc[...] = jnp.zeros(qc.shape, qc.dtype)

    pair = 2
    steps = groups // pair

    def arrive_far(i):
        @pl.when(above)
        def _():
            for u in range(pair):
                g = i * pair + u
                remote(q.at[g], qd.at[g], qd_send.at[g], qd_recv.at[g], partner).wait_recv()

                @pl.when(even)
                def _():
                    relay(g).start()

    def arrive_near(i):
        @pl.when(feeds)
        def _():
            for u in range(pair):
                g = i * pair + u
                remote(q.at[g], qc.at[g], qn_send.at[g], qc_recv.at[g], partner).wait_recv()

    def send_far(i):
        @pl.when(jnp.logical_and(odd, above))
        def _():
            for u in range(pair):
                g = i * pair + u
                od[g] = op[0, g].astype(jnp.bfloat16)
                td[g] = squeeze(lp[0, g], padded)
                start(d_copies(g))

    def send_near(i):
        @pl.when(even)
        def _():
            for u in range(pair):
                start(c_near(i * pair + u))

    def send_relay(i):
        @pl.when(jnp.logical_and(odd, feeds))
        def _():
            for u in range(pair):
                start(c_relay(i * pair + u))

    def block(far, near):
        got = []
        if far is not None:
            for u in range(pair):
                g = far * pair + u
                got.append((k, g, both_shards(g)))
                got.append((1 - k, g, one_shard(g)))
        close = []
        if near is not None:
            for u in range(pair):
                close.append((near * pair + u, nearer(near * pair + u)))
        for at, g, (o, lse) in got:
            op[at, g] = o
            lp[at, g] = lse
        for g, (o, lse) in close:
            oc[g] = o.astype(jnp.bfloat16)
            tc[g] = squeeze(lse, padded)

    arrive_far(0)
    block(0, None)
    send_far(0)

    def step(i, carry):
        arrive_far(i)
        arrive_near(i - 1)
        block(i, i - 1)
        send_far(i)
        send_relay(i - 1)
        return carry

    lax.fori_loop(1, steps, step, 0)
    for i in range(steps - 1):
        send_near(i)
    arrive_near(steps - 1)
    block(None, steps - 1)
    send_near(steps - 1)
    send_relay(steps - 1)

    @pl.when(jnp.logical_and(even, above))
    def _():
        def join(g, carry):
            remote(oc.at[g], rx.at[g], oc_send.at[g], rx_recv.at[g], partner).wait_recv()
            remote(tc.at[g], sx.at[g], tc_send.at[g], sx_recv.at[g], partner).wait_recv()
            o, lse = merge([(op[0, g], lp[0, g]), (rx[g], widen(sx[g], capacity))])
            od[g] = o.astype(jnp.bfloat16)
            td[g] = squeeze(lse, padded)
            start(d_copies(g))
            return carry

        lax.fori_loop(0, groups, join, 0)

    def absent(o, t):
        o[...] = jnp.zeros(o.shape, o.dtype)
        t[...] = jnp.full(t.shape, LOW, t.dtype)

    @pl.when(even)
    def _():
        absent(rc, sc)

    @pl.when(jnp.logical_not(below))
    def _():
        absent(rd, sd)

    def finish(g, carry):
        @pl.when(odd)
        def _():
            remote(oc.at[g], rc.at[g], oc_send.at[g], rc_recv.at[g], partner).wait_recv()
            remote(tc.at[g], sc.at[g], tc_send.at[g], sc_recv.at[g], partner).wait_recv()

        @pl.when(below)
        def _():
            remote(od.at[g], rd.at[g], od_send.at[g], rd_recv.at[g], partner).wait_recv()
            remote(td.at[g], sd.at[g], td_send.at[g], sd_recv.at[g], partner).wait_recv()

        parts = [
            (op[1, g], lp[1, g]), (rc[g], widen(sc[g], capacity)), (rd[g], widen(sd[g], capacity))
        ]
        fin[pl.ds(pl.multiple_of(g * capacity, 16), capacity), :] = merge(parts)[0].astype(jnp.bfloat16)
        return carry

    tile = 256
    tiles = groups * capacity // tile
    lane = lax.broadcasted_iota(jnp.int32, (tokens, tile), 1).astype(jnp.float32)
    done = 0
    stops = [2, 4, 6, 8] if groups == 8 else [groups]
    for s, stop in enumerate(stops):
        lax.fori_loop(stops[s - 1] if s else 0, stop, finish, 0)
        last = stop == groups
        upto = tiles if last else stop * capacity // tile
        for r in range(routed):
            slot = jnp.broadcast_to(slots[:, r : r + 1], (tokens, tile))
            here = jnp.concatenate(
                [
                    (lane + t * tile == slot).astype(jnp.float32).astype(jnp.bfloat16)
                    for t in range(done, upto)
                ],
                axis=1,
            )
            part_sum = dot(here, fin[done * tile : upto * tile, :])
            total = part_sum if s == 0 else acc[r] + part_sum
            if last:
                wide[pl.ds(r, tokens, stride=routed), :] = total
            else:
                acc[r] = total
        done = upto
    out[...] = wide[pl.ds(0, tokens * routed), :].reshape(tokens, routed, width).astype(jnp.bfloat16)

    for i in range(2):
        kv_copy(i).wait_send()

    def sent(there, make):
        @pl.when(there)
        def _():
            def body(g, carry):
                for one in make(g):
                    one.wait_send()
                return carry

            lax.fori_loop(0, groups, body, 0)

    sent(below, lambda g: (query_down(g),))
    sent(odd, lambda g: (query_near(g),))
    sent(jnp.logical_and(even, above), lambda g: (relay(g),))
    sent(above, d_copies)
    sent(even, c_near)
    sent(jnp.logical_and(odd, feeds), c_relay)


def shards(n, queries, keys, values, routes):
    tokens, routed, width = queries.shape
    context, groups, _ = keys.shape
    capacity = HEADS // groups * MOST
    padded = -(-capacity // LANES) * LANES
    vmem = pl.BlockSpec(memory_space=pltpu.VMEM)
    hbm = pl.BlockSpec(memory_space=pl.ANY)
    bf = lambda *shape: pltpu.VMEM(shape, jnp.bfloat16)
    f32 = lambda *shape: pltpu.VMEM(shape, jnp.float32)
    sem = lambda *shape: pltpu.SemaphoreType.DMA(shape)
    chunks = lambda: bf(groups, capacity, width)
    stats = lambda: f32(groups, 1, padded)
    full = lambda: f32(groups, capacity, width)
    return pl.pallas_call(
        functools.partial(kernel, n),
        out_shape=jax.ShapeDtypeStruct((tokens, routed, width), jnp.bfloat16),
        in_specs=[vmem, vmem, hbm, hbm],
        out_specs=vmem,
        scratch_shapes=[
            bf(2, context, groups, width), f32(max(tokens * routed, LANES * groups), width), bf(routed * tokens, 2 * width),
            f32(routed, tokens), f32(tokens, LANES), bf(2, groups, capacity, width), full(),
            bf(groups, 2, context, width), bf(groups, 2, context, width),
            chunks(), f32(2, groups, capacity, width), f32(2, groups, capacity, width),
            chunks(), stats(), chunks(), stats(),
            chunks(), stats(), chunks(), stats(), chunks(), stats(),
            bf(groups * capacity, width), f32(routed, tokens, width),
        ] + [sem(2)] * 3 + [sem(groups)] * 15,
        compiler_params=pltpu.CompilerParams(
            collective_id=0, has_side_effects=True, vmem_limit_bytes=60 * 1024 * 1024
        ),
        name="fused",
    )(queries, routes.T, keys, values)


def solution(mesh):
    n = mesh.shape["seq"]
    placed = (P("seq", None, None), P("seq", None, None), P("seq", None, None), P("seq", None))
    return jax.shard_map(
        functools.partial(shards, n),
        mesh=mesh,
        in_specs=placed,
        out_specs=P("seq", None, None),
        check_vma=False,
    )
```

```python
import functools
import math

import jax
import jax.numpy as jnp
from jax import lax
from jax.experimental import pallas as pl
from jax.experimental.pallas import tpu as pltpu
from jax.sharding import PartitionSpec as P

HEADS = 64
MOST = 40
LANES = 128
LOW = -1e30
MESH = pl.DeviceIdType.MESH


def dot(a, b):
    return lax.dot_general(a, b, (((1,), (0,)), ((), ())), preferred_element_type=jnp.float32)


def dot_t(a, b):
    return lax.dot_general(a, b, (((1,), (1,)), ((), ())), preferred_element_type=jnp.float32)


def remote(src, dst, send, recv, device):
    return pltpu.make_async_remote_copy(
        src_ref=src, dst_ref=dst, send_sem=send, recv_sem=recv,
        device_id=(device,), device_id_type=MESH,
    )


def attend(q, k, v, scale, mask=None):
    s = dot_t(q, k) * scale
    if mask is not None:
        s = mask(s)
    top = jnp.max(s, axis=1, keepdims=True)
    p = jnp.exp2(s - top).astype(jnp.bfloat16)
    ones = jnp.ones(v.shape, jnp.bfloat16)
    both = dot(p, jnp.concatenate([v, ones], axis=1))
    width = v.shape[1]
    total = both[:, width:]
    return both[:, :width] / total, top + jnp.log2(total)


def squeeze(lse, padded):
    rows = lse.shape[0]
    return jnp.concatenate([lse, jnp.zeros((padded - rows, LANES), jnp.float32)], axis=0).T[:1]


def widen(row, rows):
    return jnp.concatenate([jnp.broadcast_to(row, (8, row.shape[1]))] * (LANES // 8), axis=0).T[:rows]


def merge(parts):
    top = functools.reduce(jnp.maximum, [lse for _, lse in parts])
    weights = [jnp.exp2(lse - top) for _, lse in parts]
    total = functools.reduce(jnp.add, weights)
    mixed = functools.reduce(jnp.add, [o.astype(jnp.float32) * w for (o, _), w in zip(parts, weights)])
    return mixed / total, top + jnp.log2(total)


def kernel(
    n, q_in, routes_t, k_hbm, v_hbm, out,
    raw, wide, rights, slot_rows, slots, qq, pos, kall, vall,
    qc, op, lp, oc, tc, od, td, rx, sx, rc, sc, rd, sd, fin, acc,
    raw_sem, kv_send, kv_recv, qn_send, qd_send, qc_recv, qd_recv, relay_send,
    oc_send, tc_send, od_send, td_send,
    rx_recv, sx_recv, rc_recv, sc_recv, rd_recv, sd_recv,
):
    tokens, routed, width = q_in.shape
    groups, capacity = qq.shape[1:3]
    q, qd = qq.at[1], qq.at[0]
    context = kall.shape[2]
    padded = tc.shape[2]
    per_group = HEADS // groups
    chips = n // 2
    me = lax.axis_index("seq")
    c = me // 2
    k = me % 2
    partner = c * 2 + 1 - k
    even = c % 2 == 0
    odd = c % 2 == 1
    scale = jnp.float32(math.log2(math.e) / math.sqrt(width))
    below = c >= 2
    above = c + 2 < chips
    mate = jnp.where(even, c + 1, c - 1) * 2 + k
    feeds = jnp.logical_or(even, c + 1 < chips)
    down = (c - 2) * 2 + k
    up = (c + 2) * 2 + k

    barrier = pltpu.get_barrier_semaphore()

    def signal(device):
        pl.semaphore_signal(barrier, inc=1, device_id=(device,), device_id_type=MESH)

    signal(partner)
    signal(mate)

    @pl.when(below)
    def _():
        signal(down)

    @pl.when(above)
    def _():
        signal(up)

    raws = [pltpu.make_async_copy(a, raw.at[i], raw_sem.at[i]) for i, a in enumerate((k_hbm, v_hbm))]
    for one in raws:
        one.start()

    group_of = routes_t[...] // per_group
    group = lax.broadcasted_iota(jnp.int32, (groups, tokens), 0)
    hots = [(group_of[r : r + 1] == group).astype(jnp.float32) for r in range(routed)]
    count = functools.reduce(jnp.add, hots)
    row = lax.broadcasted_iota(jnp.int32, (tokens, tokens), 0)
    col = lax.broadcasted_iota(jnp.int32, (tokens, tokens), 1)
    upper = (row < col).astype(jnp.float32).astype(jnp.bfloat16)
    rank = dot(count.astype(jnp.bfloat16), upper) + (group * capacity).astype(jnp.float32)
    rows = []
    for r in range(routed):
        rows.append(jnp.sum(hots[r] * rank, axis=0, keepdims=True))
        rank = rank + hots[r]
    slot_all = jnp.concatenate(rows, axis=0)
    slot_rows[...] = slot_all
    slots[...] = jnp.concatenate([slot_all] * (LANES // routed), axis=0).T

    wide[pl.ds(0, tokens * routed), :] = q_in[...].astype(jnp.float32).reshape(tokens * routed, width)
    token = lax.broadcasted_iota(jnp.int32, (tokens, width), 0).astype(jnp.float32).astype(jnp.bfloat16)
    for r in range(routed):
        rights[pl.ds(r * tokens, tokens), :width] = wide[pl.ds(r, tokens, stride=routed), :].astype(jnp.bfloat16)
        rights[pl.ds(r * tokens, tokens), width:] = token

    pl.semaphore_wait(barrier, 2 + below.astype(jnp.int32) + above.astype(jnp.int32))

    def query_down(g):
        return remote(q.at[g], qd.at[g], qd_send.at[g], qd_recv.at[g], down)

    def query_near(g):
        return remote(q.at[g], qc.at[g], qn_send.at[g], qc_recv.at[g], mate)

    place = lax.broadcasted_iota(jnp.int32, (capacity, tokens), 0).astype(jnp.float32)

    def pack(g, carry):
        at = (g * capacity).astype(jnp.float32)
        here = jnp.concatenate(
            [
                (place == slot_rows[r : r + 1] - at).astype(jnp.float32).astype(jnp.bfloat16)
                for r in range(routed)
            ],
            axis=1,
        )
        both = dot(here, rights[...])
        q[g] = both[:, :width].astype(jnp.bfloat16)
        pos[g] = both[:, width:]

        @pl.when(below)
        def _():
            query_down(g).start()

        @pl.when(odd)
        def _():
            query_near(g).start()

        return carry

    lax.fori_loop(0, groups, pack, 0)

    part = 128

    def turn(i, to):
        def body(s, carry):
            at = pl.multiple_of(s * part, part)
            wide[pl.ds(0, part * groups), :] = raw[i, pl.ds(at, part)].astype(jnp.float32).reshape(part * groups, width)
            for g in range(groups):
                to[g, k, pl.ds(at, part), :] = wide[pl.ds(g, part, stride=groups), :].astype(jnp.bfloat16)
            return carry

        lax.fori_loop(0, context // part, body, 0)

    def kv_copy(i):
        a = (kall, vall)[i]
        return remote(a.at[:, k], a.at[:, k], kv_send.at[i], kv_recv.at[i], partner)

    def kv_arrival(i):
        a = (kall, vall)[i]
        return remote(a.at[:, 1 - k], a.at[:, 1 - k], kv_send.at[i], kv_recv.at[i], partner)

    for i, to in enumerate((kall, vall)):
        raws[i].wait()
        turn(i, to)
        kv_copy(i).start()
    for i in range(2):
        kv_arrival(i).wait_recv()

    column = lax.broadcasted_iota(jnp.int32, (capacity, tokens), 1).astype(jnp.float32)

    def all_of(a, g):
        return a[g].reshape(2 * context, width)

    def masked(bias):
        def of(g):
            limit = jnp.concatenate([pos[g] + bias] * (tokens // LANES), axis=1)

            def mask(x):
                free = x.shape[1] - tokens
                tail = jnp.where(column <= limit, x[:, free:], jnp.float32(LOW))
                return jnp.concatenate([x[:, :free], tail], axis=1)

            return mask

        return of

    first = masked(jnp.where(k == 1, jnp.float32(0), jnp.float32(2 * tokens)))
    second = masked(jnp.where(k == 0, jnp.float32(0), jnp.float32(2 * tokens)))

    def both_shards(g):
        return attend(qq[k, g], all_of(kall, g), all_of(vall, g), scale, first(g))

    def one_shard(g):
        return attend(qq[1 - k, g], kall[g, k], vall[g, k], scale, second(g))

    def nearer(g):
        return attend(qc[g], all_of(kall, g), all_of(vall, g), scale)

    def relay(g):
        return remote(qd.at[g], qc.at[g], relay_send.at[g], qc_recv.at[g], mate)

    def c_near(g):
        return (
            remote(oc.at[g], rc.at[g], oc_send.at[g], rc_recv.at[g], mate),
            remote(tc.at[g], sc.at[g], tc_send.at[g], sc_recv.at[g], mate),
        )

    def c_relay(g):
        return (
            remote(oc.at[g], rx.at[g], oc_send.at[g], rx_recv.at[g], mate),
            remote(tc.at[g], sx.at[g], tc_send.at[g], sx_recv.at[g], mate),
        )

    def d_copies(g):
        return (
            remote(od.at[g], rd.at[g], od_send.at[g], rd_recv.at[g], up),
            remote(td.at[g], sd.at[g], td_send.at[g], sd_recv.at[g], up),
        )

    def start(copies):
        for one in copies:
            one.start()

    @pl.when(jnp.logical_not(above))
    def _():
        qq[0] = jnp.zeros(qq.shape[1:], qq.dtype)

    @pl.when(jnp.logical_not(feeds))
    def _():
        qc[...] = jnp.zeros(qc.shape, qc.dtype)

    pair = 2
    steps = groups // pair

    def arrive_far(i):
        @pl.when(above)
        def _():
            for u in range(pair):
                g = i * pair + u
                remote(q.at[g], qd.at[g], qd_send.at[g], qd_recv.at[g], partner).wait_recv()

                @pl.when(even)
                def _():
                    relay(g).start()

    def arrive_near(i):
        @pl.when(feeds)
        def _():
            for u in range(pair):
                g = i * pair + u
                remote(q.at[g], qc.at[g], qn_send.at[g], qc_recv.at[g], partner).wait_recv()

    def send_far(i):
        @pl.when(jnp.logical_and(odd, above))
        def _():
            for u in range(pair):
                g = i * pair + u
                od[g] = op[0, g].astype(jnp.bfloat16)
                td[g] = squeeze(lp[0, g], padded)

    def release(upto_far, upto_near, from_far=0, from_near=0):
        def go(make, a, b):
            def body(g, carry):
                start(make(g))
                return carry

            lax.fori_loop(a * pair, b * pair, body, 0)

        @pl.when(jnp.logical_and(odd, above))
        def _():
            go(d_copies, from_far, upto_far)

        @pl.when(even)
        def _():
            go(c_near, from_near, upto_near)

    def send_relay(i):
        @pl.when(jnp.logical_and(odd, feeds))
        def _():
            for u in range(pair):
                start(c_relay(i * pair + u))

    def block(far, near):
        got = []
        if far is not None:
            for u in range(pair):
                g = far * pair + u
                got.append((k, g, both_shards(g)))
                got.append((1 - k, g, one_shard(g)))
        close = []
        if near is not None:
            for u in range(pair):
                close.append((near * pair + u, nearer(near * pair + u)))
        for at, g, (o, lse) in got:
            op[at, g] = o
            lp[at, g] = lse
        for g, (o, lse) in close:
            oc[g] = o.astype(jnp.bfloat16)
            tc[g] = squeeze(lse, padded)

    arrive_far(0)
    block(0, None)
    send_far(0)

    def step(i, carry):
        arrive_far(i)

        @pl.when(i == steps - 1)
        def _():
            release(steps - 1, steps - 2)

        arrive_near(i - 1)
        block(i, i - 1)
        send_far(i)
        send_relay(i - 1)
        return carry

    lax.fori_loop(1, steps, step, 0)
    release(steps, steps - 1, steps - 1, steps - 2)
    arrive_near(steps - 1)
    block(None, steps - 1)
    release(steps, steps, steps, steps - 1)
    send_relay(steps - 1)

    @pl.when(jnp.logical_and(even, above))
    def _():
        def join(g, carry):
            remote(oc.at[g], rx.at[g], oc_send.at[g], rx_recv.at[g], partner).wait_recv()
            remote(tc.at[g], sx.at[g], tc_send.at[g], sx_recv.at[g], partner).wait_recv()
            o, lse = merge([(op[0, g], lp[0, g]), (rx[g], widen(sx[g], capacity))])
            od[g] = o.astype(jnp.bfloat16)
            td[g] = squeeze(lse, padded)
            start(d_copies(g))
            return carry

        lax.fori_loop(0, groups, join, 0)

    def absent(o, t):
        o[...] = jnp.zeros(o.shape, o.dtype)
        t[...] = jnp.full(t.shape, LOW, t.dtype)

    @pl.when(even)
    def _():
        absent(rc, sc)

    @pl.when(jnp.logical_not(below))
    def _():
        absent(rd, sd)

    def finish(g, carry):
        @pl.when(odd)
        def _():
            remote(oc.at[g], rc.at[g], oc_send.at[g], rc_recv.at[g], partner).wait_recv()
            remote(tc.at[g], sc.at[g], tc_send.at[g], sc_recv.at[g], partner).wait_recv()

        @pl.when(below)
        def _():
            remote(od.at[g], rd.at[g], od_send.at[g], rd_recv.at[g], partner).wait_recv()
            remote(td.at[g], sd.at[g], td_send.at[g], sd_recv.at[g], partner).wait_recv()

        parts = [
            (op[1, g], lp[1, g]), (rc[g], widen(sc[g], capacity)), (rd[g], widen(sd[g], capacity))
        ]
        fin[pl.ds(pl.multiple_of(g * capacity, 16), capacity), :] = merge(parts)[0].astype(jnp.bfloat16)
        return carry

    tile = 256
    tiles = groups * capacity // tile
    lane = lax.broadcasted_iota(jnp.int32, (tokens, tile), 1).astype(jnp.float32)
    done = 0
    stops = [2, 4, 6, 8] if groups == 8 else [groups]
    for s, stop in enumerate(stops):
        lax.fori_loop(stops[s - 1] if s else 0, stop, finish, 0)
        last = stop == groups
        upto = tiles if last else stop * capacity // tile
        for r in range(routed):
            slot = jnp.broadcast_to(slots[:, r : r + 1], (tokens, tile))
            here = jnp.concatenate(
                [
                    (lane + t * tile == slot).astype(jnp.float32).astype(jnp.bfloat16)
                    for t in range(done, upto)
                ],
                axis=1,
            )
            part_sum = dot(here, fin[done * tile : upto * tile, :])
            total = part_sum if s == 0 else acc[r] + part_sum
            if last:
                wide[pl.ds(r, tokens, stride=routed), :] = total
            else:
                acc[r] = total
        done = upto
    out[...] = wide[pl.ds(0, tokens * routed), :].reshape(tokens, routed, width).astype(jnp.bfloat16)

    for i in range(2):
        kv_copy(i).wait_send()

    def sent(there, make):
        @pl.when(there)
        def _():
            def body(g, carry):
                for one in make(g):
                    one.wait_send()
                return carry

            lax.fori_loop(0, groups, body, 0)

    sent(below, lambda g: (query_down(g),))
    sent(odd, lambda g: (query_near(g),))
    sent(jnp.logical_and(even, above), lambda g: (relay(g),))
    sent(above, d_copies)
    sent(even, c_near)
    sent(jnp.logical_and(odd, feeds), c_relay)


def shards(n, queries, keys, values, routes):
    tokens, routed, width = queries.shape
    context, groups, _ = keys.shape
    capacity = HEADS // groups * MOST
    padded = -(-capacity // LANES) * LANES
    vmem = pl.BlockSpec(memory_space=pltpu.VMEM)
    hbm = pl.BlockSpec(memory_space=pl.ANY)
    bf = lambda *shape: pltpu.VMEM(shape, jnp.bfloat16)
    f32 = lambda *shape: pltpu.VMEM(shape, jnp.float32)
    sem = lambda *shape: pltpu.SemaphoreType.DMA(shape)
    chunks = lambda: bf(groups, capacity, width)
    stats = lambda: f32(groups, 1, padded)
    full = lambda: f32(groups, capacity, width)
    return pl.pallas_call(
        functools.partial(kernel, n),
        out_shape=jax.ShapeDtypeStruct((tokens, routed, width), jnp.bfloat16),
        in_specs=[vmem, vmem, hbm, hbm],
        out_specs=vmem,
        scratch_shapes=[
            bf(2, context, groups, width), f32(max(tokens * routed, LANES * groups), width), bf(routed * tokens, 2 * width),
            f32(routed, tokens), f32(tokens, LANES), bf(2, groups, capacity, width), full(),
            bf(groups, 2, context, width), bf(groups, 2, context, width),
            chunks(), f32(2, groups, capacity, width), f32(2, groups, capacity, width),
            chunks(), stats(), chunks(), stats(),
            chunks(), stats(), chunks(), stats(), chunks(), stats(),
            bf(groups * capacity, width), f32(routed, tokens, width),
        ] + [sem(2)] * 3 + [sem(groups)] * 15,
        compiler_params=pltpu.CompilerParams(
            collective_id=0, has_side_effects=True, vmem_limit_bytes=60 * 1024 * 1024
        ),
        name="fused",
    )(queries, routes.T, keys, values)


def solution(mesh):
    n = mesh.shape["seq"]
    placed = (P("seq", None, None), P("seq", None, None), P("seq", None, None), P("seq", None))
    return jax.shard_map(
        functools.partial(shards, n),
        mesh=mesh,
        in_specs=placed,
        out_specs=P("seq", None, None),
        check_vma=False,
    )
```

```python
import functools
import math

import jax
import jax.numpy as jnp
from jax import lax
from jax.experimental import pallas as pl
from jax.experimental.pallas import tpu as pltpu
from jax.sharding import PartitionSpec as P

HEADS = 64
MOST = 40
LANES = 128
LOW = -1e30
MESH = pl.DeviceIdType.MESH


def dot(a, b):
    return lax.dot_general(a, b, (((1,), (0,)), ((), ())), preferred_element_type=jnp.float32)


def dot_t(a, b):
    return lax.dot_general(a, b, (((1,), (1,)), ((), ())), preferred_element_type=jnp.float32)


def remote(src, dst, send, recv, device):
    return pltpu.make_async_remote_copy(
        src_ref=src, dst_ref=dst, send_sem=send, recv_sem=recv,
        device_id=(device,), device_id_type=MESH,
    )


def attend(q, k, v, scale, mask=None):
    s = dot_t(q, k) * scale
    if mask is not None:
        s = mask(s)
    top = jnp.max(s, axis=1, keepdims=True)
    p = jnp.exp2(s - top).astype(jnp.bfloat16)
    ones = jnp.ones(v.shape, jnp.bfloat16)
    both = dot(p, jnp.concatenate([v, ones], axis=1))
    width = v.shape[1]
    total = both[:, width:]
    return both[:, :width] / total, top + jnp.log2(total)


def squeeze(lse, padded):
    rows = lse.shape[0]
    return jnp.concatenate([lse, jnp.zeros((padded - rows, LANES), jnp.float32)], axis=0).T[:1]


def widen(row, rows):
    return jnp.concatenate([jnp.broadcast_to(row, (8, row.shape[1]))] * (LANES // 8), axis=0).T[:rows]


def merge(parts):
    top = functools.reduce(jnp.maximum, [lse for _, lse in parts])
    weights = [jnp.exp2(lse - top) for _, lse in parts]
    total = functools.reduce(jnp.add, weights)
    mixed = functools.reduce(jnp.add, [o.astype(jnp.float32) * w for (o, _), w in zip(parts, weights)])
    return mixed / total, top + jnp.log2(total)


def kernel(
    n, q_hbm, routes_hbm, k_hbm, v_hbm, out,
    q_in, routes_t, raw, wide, rights, slot_rows, slots, qq, pos, kall, vall,
    qc, op, lp, oc, tc, od, td, rx, sx, rc, sc, rd, sd, fin, acc,
    in_sem, raw_sem, kv_send, kv_recv, qn_send, qd_send, qc_recv, qd_recv, relay_send,
    oc_send, tc_send, od_send, td_send,
    rx_recv, sx_recv, rc_recv, sc_recv, rd_recv, sd_recv,
):
    tokens, routed, width = q_in.shape
    groups, capacity = qq.shape[1:3]
    q, qd = qq.at[1], qq.at[0]
    context = kall.shape[2]
    padded = tc.shape[2]
    per_group = HEADS // groups
    chips = n // 2
    me = lax.axis_index("seq")
    c = me // 2
    k = me % 2
    partner = c * 2 + 1 - k
    even = c % 2 == 0
    odd = c % 2 == 1
    scale = jnp.float32(math.log2(math.e) / math.sqrt(width))
    below = c >= 2
    above = c + 2 < chips
    mate = jnp.where(even, c + 1, c - 1) * 2 + k
    feeds = jnp.logical_or(even, c + 1 < chips)
    down = (c - 2) * 2 + k
    up = (c + 2) * 2 + k

    barrier = pltpu.get_barrier_semaphore()

    def signal(device):
        pl.semaphore_signal(barrier, inc=1, device_id=(device,), device_id_type=MESH)

    signal(partner)
    signal(mate)

    @pl.when(below)
    def _():
        signal(down)

    @pl.when(above)
    def _():
        signal(up)

    ins = [
        pltpu.make_async_copy(a, b, in_sem.at[i])
        for i, (a, b) in enumerate(((routes_hbm, routes_t), (q_hbm, q_in)))
    ]
    raws = [pltpu.make_async_copy(a, raw.at[i], raw_sem.at[i]) for i, a in enumerate((k_hbm, v_hbm))]
    for one in ins + raws:
        one.start()
    ins[0].wait()

    group_of = routes_t[...] // per_group
    group = lax.broadcasted_iota(jnp.int32, (groups, tokens), 0)
    hots = [(group_of[r : r + 1] == group).astype(jnp.float32) for r in range(routed)]
    count = functools.reduce(jnp.add, hots)
    row = lax.broadcasted_iota(jnp.int32, (tokens, tokens), 0)
    col = lax.broadcasted_iota(jnp.int32, (tokens, tokens), 1)
    upper = (row < col).astype(jnp.float32).astype(jnp.bfloat16)
    rank = dot(count.astype(jnp.bfloat16), upper) + (group * capacity).astype(jnp.float32)
    rows = []
    for r in range(routed):
        rows.append(jnp.sum(hots[r] * rank, axis=0, keepdims=True))
        rank = rank + hots[r]
    slot_all = jnp.concatenate(rows, axis=0)
    slot_rows[...] = slot_all
    slots[...] = jnp.concatenate([slot_all] * (LANES // routed), axis=0).T

    ins[1].wait()
    wide[pl.ds(0, tokens * routed), :] = q_in[...].astype(jnp.float32).reshape(tokens * routed, width)
    token = lax.broadcasted_iota(jnp.int32, (tokens, width), 0).astype(jnp.float32).astype(jnp.bfloat16)
    for r in range(routed):
        rights[pl.ds(r * tokens, tokens), :width] = wide[pl.ds(r, tokens, stride=routed), :].astype(jnp.bfloat16)
        rights[pl.ds(r * tokens, tokens), width:] = token

    pl.semaphore_wait(barrier, 2 + below.astype(jnp.int32) + above.astype(jnp.int32))

    def query_down(g):
        return remote(q.at[g], qd.at[g], qd_send.at[g], qd_recv.at[g], down)

    def query_near(g):
        return remote(q.at[g], qc.at[g], qn_send.at[g], qc_recv.at[g], mate)

    place = lax.broadcasted_iota(jnp.int32, (capacity, tokens), 0).astype(jnp.float32)

    def pack(g, carry):
        at = (g * capacity).astype(jnp.float32)
        here = jnp.concatenate(
            [
                (place == slot_rows[r : r + 1] - at).astype(jnp.float32).astype(jnp.bfloat16)
                for r in range(routed)
            ],
            axis=1,
        )
        both = dot(here, rights[...])
        q[g] = both[:, :width].astype(jnp.bfloat16)
        pos[g] = both[:, width:]

        @pl.when(below)
        def _():
            query_down(g).start()

        @pl.when(odd)
        def _():
            query_near(g).start()

        return carry

    lax.fori_loop(0, groups, pack, 0)

    part = 128

    def turn(i, to):
        def body(s, carry):
            at = pl.multiple_of(s * part, part)
            wide[pl.ds(0, part * groups), :] = raw[i, pl.ds(at, part)].astype(jnp.float32).reshape(part * groups, width)
            for g in range(groups):
                to[g, k, pl.ds(at, part), :] = wide[pl.ds(g, part, stride=groups), :].astype(jnp.bfloat16)
            return carry

        lax.fori_loop(0, context // part, body, 0)

    def kv_copy(i):
        a = (kall, vall)[i]
        return remote(a.at[:, k], a.at[:, k], kv_send.at[i], kv_recv.at[i], partner)

    def kv_arrival(i):
        a = (kall, vall)[i]
        return remote(a.at[:, 1 - k], a.at[:, 1 - k], kv_send.at[i], kv_recv.at[i], partner)

    for i, to in enumerate((kall, vall)):
        raws[i].wait()
        turn(i, to)
        kv_copy(i).start()
    for i in range(2):
        kv_arrival(i).wait_recv()

    column = lax.broadcasted_iota(jnp.int32, (capacity, tokens), 1).astype(jnp.float32)

    def all_of(a, g):
        return a[g].reshape(2 * context, width)

    def masked(bias):
        def of(g):
            limit = jnp.concatenate([pos[g] + bias] * (tokens // LANES), axis=1)

            def mask(x):
                free = x.shape[1] - tokens
                tail = jnp.where(column <= limit, x[:, free:], jnp.float32(LOW))
                return jnp.concatenate([x[:, :free], tail], axis=1)

            return mask

        return of

    first = masked(jnp.where(k == 1, jnp.float32(0), jnp.float32(2 * tokens)))
    second = masked(jnp.where(k == 0, jnp.float32(0), jnp.float32(2 * tokens)))

    def both_shards(g):
        return attend(qq[k, g], all_of(kall, g), all_of(vall, g), scale, first(g))

    def one_shard(g):
        return attend(qq[1 - k, g], kall[g, k], vall[g, k], scale, second(g))

    def nearer(g):
        return attend(qc[g], all_of(kall, g), all_of(vall, g), scale)

    def relay(g):
        return remote(qd.at[g], qc.at[g], relay_send.at[g], qc_recv.at[g], mate)

    def c_near(g):
        return (
            remote(oc.at[g], rc.at[g], oc_send.at[g], rc_recv.at[g], mate),
            remote(tc.at[g], sc.at[g], tc_send.at[g], sc_recv.at[g], mate),
        )

    def c_relay(g):
        return (
            remote(oc.at[g], rx.at[g], oc_send.at[g], rx_recv.at[g], mate),
            remote(tc.at[g], sx.at[g], tc_send.at[g], sx_recv.at[g], mate),
        )

    def d_copies(g):
        return (
            remote(od.at[g], rd.at[g], od_send.at[g], rd_recv.at[g], up),
            remote(td.at[g], sd.at[g], td_send.at[g], sd_recv.at[g], up),
        )

    def start(copies):
        for one in copies:
            one.start()

    @pl.when(jnp.logical_not(above))
    def _():
        qq[0] = jnp.zeros(qq.shape[1:], qq.dtype)

    @pl.when(jnp.logical_not(feeds))
    def _():
        qc[...] = jnp.zeros(qc.shape, qc.dtype)

    pair = 2
    steps = groups // pair

    def arrive_far(i):
        @pl.when(above)
        def _():
            for u in range(pair):
                g = i * pair + u
                remote(q.at[g], qd.at[g], qd_send.at[g], qd_recv.at[g], partner).wait_recv()

                @pl.when(even)
                def _():
                    relay(g).start()

    def arrive_near(i):
        @pl.when(feeds)
        def _():
            for u in range(pair):
                g = i * pair + u
                remote(q.at[g], qc.at[g], qn_send.at[g], qc_recv.at[g], partner).wait_recv()

    def send_far(i):
        @pl.when(jnp.logical_and(odd, above))
        def _():
            for u in range(pair):
                g = i * pair + u
                od[g] = op[0, g].astype(jnp.bfloat16)
                td[g] = squeeze(lp[0, g], padded)

    def release(upto_far, upto_near, from_far=0, from_near=0):
        def go(make, a, b):
            def body(g, carry):
                start(make(g))
                return carry

            lax.fori_loop(a * pair, b * pair, body, 0)

        @pl.when(jnp.logical_and(odd, above))
        def _():
            go(d_copies, from_far, upto_far)

        @pl.when(even)
        def _():
            go(c_near, from_near, upto_near)

    def send_relay(i):
        @pl.when(jnp.logical_and(odd, feeds))
        def _():
            for u in range(pair):
                start(c_relay(i * pair + u))

    def block(far, near):
        got = []
        if far is not None:
            for u in range(pair):
                g = far * pair + u
                got.append((k, g, both_shards(g)))
                got.append((1 - k, g, one_shard(g)))
        close = []
        if near is not None:
            for u in range(pair):
                close.append((near * pair + u, nearer(near * pair + u)))
        for at, g, (o, lse) in got:
            op[at, g] = o
            lp[at, g] = lse
        for g, (o, lse) in close:
            oc[g] = o.astype(jnp.bfloat16)
            tc[g] = squeeze(lse, padded)

    arrive_far(0)
    block(0, None)
    send_far(0)

    def step(i, carry):
        arrive_far(i)

        @pl.when(i == steps - 1)
        def _():
            release(steps - 1, steps - 2)

        arrive_near(i - 1)
        block(i, i - 1)
        send_far(i)
        send_relay(i - 1)
        return carry

    lax.fori_loop(1, steps, step, 0)
    release(steps, steps - 1, steps - 1, steps - 2)
    arrive_near(steps - 1)
    block(None, steps - 1)
    release(steps, steps, steps, steps - 1)
    send_relay(steps - 1)

    for i in range(2):
        kv_copy(i).wait_send()

    def sent(there, make):
        @pl.when(there)
        def _():
            def body(g, carry):
                for one in make(g):
                    one.wait_send()
                return carry

            lax.fori_loop(0, groups, body, 0)

    sent(below, lambda g: (query_down(g),))
    sent(odd, lambda g: (query_near(g),))
    sent(jnp.logical_and(even, above), lambda g: (relay(g),))

    @pl.when(jnp.logical_and(even, above))
    def _():
        def join(g, carry):
            remote(oc.at[g], rx.at[g], oc_send.at[g], rx_recv.at[g], partner).wait_recv()
            remote(tc.at[g], sx.at[g], tc_send.at[g], sx_recv.at[g], partner).wait_recv()
            o, lse = merge([(op[0, g], lp[0, g]), (rx[g], widen(sx[g], capacity))])
            od[g] = o.astype(jnp.bfloat16)
            td[g] = squeeze(lse, padded)
            start(d_copies(g))
            return carry

        lax.fori_loop(0, groups, join, 0)

    def absent(o, t):
        o[...] = jnp.zeros(o.shape, o.dtype)
        t[...] = jnp.full(t.shape, LOW, t.dtype)

    @pl.when(even)
    def _():
        absent(rc, sc)

    @pl.when(jnp.logical_not(below))
    def _():
        absent(rd, sd)

    def finish(g, carry):
        @pl.when(odd)
        def _():
            remote(oc.at[g], rc.at[g], oc_send.at[g], rc_recv.at[g], partner).wait_recv()
            remote(tc.at[g], sc.at[g], tc_send.at[g], sc_recv.at[g], partner).wait_recv()

        @pl.when(below)
        def _():
            remote(od.at[g], rd.at[g], od_send.at[g], rd_recv.at[g], partner).wait_recv()
            remote(td.at[g], sd.at[g], td_send.at[g], sd_recv.at[g], partner).wait_recv()

        parts = [
            (op[1, g], lp[1, g]), (rc[g], widen(sc[g], capacity)), (rd[g], widen(sd[g], capacity))
        ]
        fin[pl.ds(pl.multiple_of(g * capacity, 16), capacity), :] = merge(parts)[0].astype(jnp.bfloat16)
        return carry

    sent(jnp.logical_and(odd, feeds), c_relay)

    tile = 256
    tiles = groups * capacity // tile
    lane = lax.broadcasted_iota(jnp.int32, (tokens, tile), 1).astype(jnp.float32)
    done = 0
    stops = [2, 4, 6, 7, 8] if groups == 8 else [groups]
    for s, stop in enumerate(stops):
        lax.fori_loop(stops[s - 1] if s else 0, stop, finish, 0)
        last = stop == groups
        upto = tiles if last else stop * capacity // tile
        for r in range(routed):
            slot = jnp.broadcast_to(slots[:, r : r + 1], (tokens, tile))
            here = jnp.concatenate(
                [
                    (lane + t * tile == slot).astype(jnp.float32).astype(jnp.bfloat16)
                    for t in range(done, upto)
                ],
                axis=1,
            )
            part_sum = dot(here, fin[done * tile : upto * tile, :])
            total = part_sum if s == 0 else acc[r] + part_sum
            if last:
                wide[pl.ds(r, tokens, stride=routed), :] = total
            else:
                acc[r] = total
        done = upto
    out[...] = wide[pl.ds(0, tokens * routed), :].reshape(tokens, routed, width).astype(jnp.bfloat16)

    sent(above, d_copies)
    sent(even, c_near)


def shards(n, queries, keys, values, routes):
    tokens, routed, width = queries.shape
    context, groups, _ = keys.shape
    capacity = HEADS // groups * MOST
    padded = -(-capacity // LANES) * LANES
    vmem = pl.BlockSpec(memory_space=pltpu.VMEM)
    hbm = pl.BlockSpec(memory_space=pltpu.HBM)
    bf = lambda *shape: pltpu.VMEM(shape, jnp.bfloat16)
    f32 = lambda *shape: pltpu.VMEM(shape, jnp.float32)
    sem = lambda *shape: pltpu.SemaphoreType.DMA(shape)
    chunks = lambda: bf(groups, capacity, width)
    stats = lambda: f32(groups, 1, padded)
    full = lambda: f32(groups, capacity, width)
    return pl.pallas_call(
        functools.partial(kernel, n),
        out_shape=jax.ShapeDtypeStruct((tokens, routed, width), jnp.bfloat16),
        in_specs=[hbm] * 4,
        out_specs=vmem,
        scratch_shapes=[
            bf(tokens, routed, width), pltpu.VMEM((routed, tokens), jnp.int32),
            bf(2, context, groups, width), f32(max(tokens * routed, LANES * groups), width), bf(routed * tokens, 2 * width),
            f32(routed, tokens), f32(tokens, LANES), bf(2, groups, capacity, width), full(),
            bf(groups, 2, context, width), bf(groups, 2, context, width),
            chunks(), f32(2, groups, capacity, width), f32(2, groups, capacity, width),
            chunks(), stats(), chunks(), stats(),
            chunks(), stats(), chunks(), stats(), chunks(), stats(),
            bf(groups * capacity, width), f32(routed, tokens, width),
        ] + [sem(2)] * 4 + [sem(groups)] * 15,
        compiler_params=pltpu.CompilerParams(
            collective_id=0, has_side_effects=True, vmem_limit_bytes=48 * 1024 * 1024
        ),
        name="fused",
    )(*(pltpu.with_memory_space_constraint(a, pltpu.HBM) for a in (queries, routes.T, keys, values)))


def solution(mesh):
    n = mesh.shape["seq"]
    placed = (P("seq", None, None), P("seq", None, None), P("seq", None, None), P("seq", None))
    return jax.shard_map(
        functools.partial(shards, n),
        mesh=mesh,
        in_specs=placed,
        out_specs=P("seq", None, None),
        check_vma=False,
    )
```

```python
import functools
import math

import jax
import jax.numpy as jnp
from jax import lax
from jax.experimental import pallas as pl
from jax.experimental.pallas import tpu as pltpu
from jax.sharding import PartitionSpec as P

HEADS = 64
MOST = 40
LANES = 128
LOW = -1e30
BLOCK = 16
TABLE = 256
MESH = pl.DeviceIdType.MESH


def dot(a, b):
    return lax.dot_general(a, b, (((1,), (0,)), ((), ())), preferred_element_type=jnp.float32)


def dot_t(a, b):
    return lax.dot_general(a, b, (((1,), (1,)), ((), ())), preferred_element_type=jnp.float32)


def remote(src, dst, send, recv, device):
    return pltpu.make_async_remote_copy(
        src_ref=src, dst_ref=dst, send_sem=send, recv_sem=recv,
        device_id=(device,), device_id_type=MESH,
    )


def attend(q, k, v, scale, mask=None):
    s = dot_t(q, k) * scale
    if mask is not None:
        s = mask(s)
    top = jnp.max(s, axis=1, keepdims=True)
    p = jnp.exp2(s - top).astype(jnp.bfloat16)
    ones = jnp.ones(v.shape, jnp.bfloat16)
    both = dot(p, jnp.concatenate([v, ones], axis=1))
    width = v.shape[1]
    total = both[:, width:]
    return both[:, :width] / total, top + jnp.log2(total)


def squeeze(lse, padded):
    rows = lse.shape[0]
    return jnp.concatenate([lse, jnp.zeros((padded - rows, LANES), jnp.float32)], axis=0).T[:1]


def widen(row, rows):
    return jnp.concatenate([jnp.broadcast_to(row, (8, row.shape[1]))] * (LANES // 8), axis=0).T[:rows]


def merge(parts):
    top = functools.reduce(jnp.maximum, [lse for _, lse in parts])
    weights = [jnp.exp2(lse - top) for _, lse in parts]
    total = functools.reduce(jnp.add, weights)
    mixed = functools.reduce(jnp.add, [o.astype(jnp.float32) * w for (o, _), w in zip(parts, weights)])
    return mixed / total, top + jnp.log2(total)


def kernel(
    n, q_hbm, routes_hbm, k_hbm, v_hbm, out,
    q_in, routes_t, raw, wide, rights, slot_rows, slots, wq, wc, pos, kall, vall,
    tab, tab_d, tab_c, at_own, at_d, at_c,
    qd, qc, op, lp, cp, lc, oc, tc, od, td, rx, sx, rc, sc, rd, sd, fin, acc,
    in_sem, tab_sem, tab_far, tab_near, tab_relay, raw_sem, kv_send, kv_recv, qn_send, qd_send, qc_recv, qd_recv, relay_send,
    oc_send, tc_send, od_send, td_send,
    rx_recv, sx_recv, rc_recv, sc_recv, rd_recv, sd_recv,
):
    tokens, routed, width = q_in.shape
    groups = kall.shape[0]
    chunks, per_block = qd.shape[:2]
    capacity = per_block * BLOCK
    context = kall.shape[2]
    padded = tc.shape[2]
    per_group = HEADS // groups
    chips = n // 2
    me = lax.axis_index("seq")
    c = me // 2
    k = me % 2
    partner = c * 2 + 1 - k
    even = c % 2 == 0
    odd = c % 2 == 1
    scale = jnp.float32(math.log2(math.e) / math.sqrt(width))
    below = c >= 2
    above = c + 2 < chips
    mate = jnp.where(even, c + 1, c - 1) * 2 + k
    feeds = jnp.logical_or(even, c + 1 < chips)
    down = (c - 2) * 2 + k
    up = (c + 2) * 2 + k

    barrier = pltpu.get_barrier_semaphore()

    def signal(device):
        pl.semaphore_signal(barrier, inc=1, device_id=(device,), device_id_type=MESH)

    signal(partner)
    signal(mate)

    @pl.when(below)
    def _():
        signal(down)

    @pl.when(above)
    def _():
        signal(up)

    ins = [
        pltpu.make_async_copy(a, b, in_sem.at[i])
        for i, (a, b) in enumerate(((routes_hbm, routes_t), (q_hbm, q_in)))
    ]
    raws = [pltpu.make_async_copy(a, raw.at[i], raw_sem.at[i]) for i, a in enumerate((k_hbm, v_hbm))]
    for one in ins + raws:
        one.start()
    ins[0].wait()

    group_of = routes_t[...] // per_group
    group = lax.broadcasted_iota(jnp.int32, (groups, tokens), 0)
    hots = [(group_of[r : r + 1] == group).astype(jnp.float32) for r in range(routed)]
    count = functools.reduce(jnp.add, hots)
    row = lax.broadcasted_iota(jnp.int32, (tokens, tokens), 0)
    col = lax.broadcasted_iota(jnp.int32, (tokens, tokens), 1)
    upper = (row < col).astype(jnp.float32).astype(jnp.bfloat16)
    many = functools.reduce(
        jnp.add, [(group_of[r : r + 1] == group).astype(jnp.int32) for r in range(routed)]
    )
    blocks = (jnp.sum(many, axis=1, keepdims=True) + (BLOCK - 1)) // BLOCK
    blocks = jnp.broadcast_to(blocks, (groups, TABLE))
    starts = [jnp.zeros((1, TABLE), jnp.int32)]
    for g in range(1, groups):
        starts.append(starts[-1] + blocks[g - 1 : g])
    place = lax.broadcasted_iota(jnp.int32, (1, TABLE), 1)
    source = place
    first_block = starts[0]
    for g in range(1, groups):
        source = source + jnp.where(place >= starts[g], per_block - blocks[g - 1 : g], 0)
        first_block = jnp.where(place >= g, starts[g], first_block)
    source = jnp.minimum(source, groups * per_block - 1)
    first_block = jnp.minimum(first_block, chunks * per_block)
    tab[...] = jnp.concatenate([source, first_block], axis=1)
    base = jnp.concatenate(starts, axis=0)[:, :1].astype(jnp.float32) * BLOCK
    rank = dot(count.astype(jnp.bfloat16), upper) + base
    rows = []
    for r in range(routed):
        rows.append(jnp.sum(hots[r] * rank, axis=0, keepdims=True))
        rank = rank + hots[r]
    slot_all = jnp.concatenate(rows, axis=0)
    slot_rows[...] = slot_all
    slots[...] = jnp.concatenate([slot_all] * (LANES // routed), axis=0).T

    ins[1].wait()
    wide[pl.ds(0, tokens * routed), :] = q_in[...].astype(jnp.float32).reshape(tokens * routed, width)
    token = lax.broadcasted_iota(jnp.int32, (tokens, width), 0).astype(jnp.float32).astype(jnp.bfloat16)
    for r in range(routed):
        rights[pl.ds(r * tokens, tokens), :width] = wide[pl.ds(r, tokens, stride=routed), :].astype(jnp.bfloat16)
        rights[pl.ds(r * tokens, tokens), width:] = token

    pl.semaphore_wait(barrier, 2 + below.astype(jnp.int32) + above.astype(jnp.int32))

    def rows_of(j):
        return pl.ds(j * per_block, per_block)

    def split(x):
        return x.reshape(x.shape[0] // BLOCK, BLOCK, width)

    def flat(x):
        return x.reshape(x.shape[0] * BLOCK, width)

    halves = 2
    part_rows = per_block // halves

    def part_of(h):
        return pl.ds(h * part_rows, part_rows)

    def query_part(j, h):
        return wq.at[1, pl.ds(j * per_block + h * part_rows, part_rows)]

    def query_down(j):
        return [
            remote(query_part(j, h), qd.at[j, part_of(h)], qd_send.at[j, h], qd_recv.at[j, h], down)
            for h in range(halves)
        ]

    def query_near(j):
        return [
            remote(query_part(j, h), qc.at[j, part_of(h)], qn_send.at[j, h], qc_recv.at[j, h], mate)
            for h in range(halves)
        ]

    def relay_part(j, h):
        return remote(qd.at[j, part_of(h)], qc.at[j, part_of(h)], relay_send.at[j, h], qc_recv.at[j, h], mate)

    def relay(j):
        return [relay_part(j, h) for h in range(halves)]

    def start(copies):
        for one in copies:
            one.start()

    def table_down():
        return remote(tab, tab_d, tab_far.at[0], tab_far.at[1], down)

    def table_near():
        return remote(tab, tab_c, tab_near.at[0], tab_near.at[1], mate)

    def table_relay():
        return remote(tab_d, tab_c, tab_relay.at[0], tab_near.at[1], mate)

    @pl.when(below)
    def _():
        table_down().start()

    @pl.when(odd)
    def _():
        table_near().start()

    place = lax.broadcasted_iota(jnp.int32, (capacity, tokens), 0).astype(jnp.float32)

    def pack(g, carry):
        at = (g * capacity).astype(jnp.float32)
        here = jnp.concatenate(
            [
                (place == slot_rows[r : r + 1] - at).astype(jnp.float32).astype(jnp.bfloat16)
                for r in range(routed)
            ],
            axis=1,
        )
        both = dot(here, rights[...])
        wq[1, rows_of(g)] = split(both[:, :width].astype(jnp.bfloat16))
        pos[rows_of(g)] = split(both[:, width:])

        @pl.when(below)
        def _():
            start(query_down(g))

        @pl.when(odd)
        def _():
            start(query_near(g))

        return carry

    lax.fori_loop(0, chunks, pack, 0)

    local = [
        pltpu.make_async_copy(a, b, tab_sem.at[i])
        for i, (a, b) in enumerate(((tab_d, at_d), (tab, at_own), (tab_c, at_c)))
    ]
    local[1].start()
    rest = (groups - chunks) * per_block
    wq[1, pl.ds(chunks * per_block, rest)] = jnp.zeros((rest, BLOCK, width), wq.dtype)
    pos[pl.ds(chunks * per_block, rest)] = jnp.zeros((rest, BLOCK, width), pos.dtype)
    wq[0] = jnp.zeros(wq.shape[1:], wq.dtype)
    wc[...] = jnp.zeros(wc.shape, wc.dtype)

    def each(a, b, body):
        def go(j, carry):
            body(j)
            return carry

        lax.fori_loop(a, b, go, 0)

    @pl.when(above)
    def _():
        remote(tab, tab_d, tab_far.at[0], tab_far.at[1], partner).wait_recv()

        @pl.when(even)
        def _():
            table_relay().start()

    @pl.when(jnp.logical_not(above))
    def _():
        tab_d[...] = tab[...]

    local[0].start()
    local[0].wait()
    local[1].wait()

    def absent(o, t):
        o[...] = jnp.zeros(o.shape, o.dtype)
        t[...] = jnp.full(t.shape, LOW, t.dtype)

    @pl.when(even)
    def _():
        absent(rc, sc)

    @pl.when(jnp.logical_not(below))
    def _():
        absent(rd, sd)

    def far_chunk(j):
        @pl.when(jnp.logical_and(above, j < chunks))
        def _():
            for h in range(halves):
                remote(
                    qd.at[j, part_of(h)], qd.at[j, part_of(h)], qd_send.at[j, h], qd_recv.at[j, h], partner
                ).wait_recv()

                @pl.when(even)
                def _(h=h):
                    relay_part(j, h).start()

            wq[0, rows_of(j)] = qd[j]

    far_chunk(jnp.int32(0))

    part = 128

    def turn(i, to):
        def body(s, carry):
            at = pl.multiple_of(s * part, part)
            wide[pl.ds(0, part * groups), :] = raw[i, pl.ds(at, part)].astype(jnp.float32).reshape(part * groups, width)
            for g in range(groups):
                to[g, k, pl.ds(at, part), :] = wide[pl.ds(g, part, stride=groups), :].astype(jnp.bfloat16)
            return carry

        lax.fori_loop(0, context // part, body, 0)

    def kv_copy(i):
        a = (kall, vall)[i]
        return remote(a.at[:, k], a.at[:, k], kv_send.at[i], kv_recv.at[i], partner)

    def kv_arrival(i):
        a = (kall, vall)[i]
        return remote(a.at[:, 1 - k], a.at[:, 1 - k], kv_send.at[i], kv_recv.at[i], partner)

    for i, to in enumerate((kall, vall)):
        raws[i].wait()
        turn(i, to)
        kv_copy(i).start()
    far_chunk(jnp.int32(1))
    for i in range(2):
        kv_arrival(i).wait_recv()

    column = lax.broadcasted_iota(jnp.int32, (capacity, tokens), 1).astype(jnp.float32)

    def all_of(a, g):
        return a[g].reshape(2 * context, width)

    def window(table, g):
        return pl.ds(table[0, TABLE + g], per_block)

    def masked(bias):
        def of(g):
            limit = flat(pos[window(at_own, g)]) + bias
            limit = jnp.concatenate([limit] * (tokens // LANES), axis=1)

            def mask(x):
                free = x.shape[1] - tokens
                tail = jnp.where(column <= limit, x[:, free:], jnp.float32(LOW))
                return jnp.concatenate([x[:, :free], tail], axis=1)

            return mask

        return of

    first = masked(jnp.where(k == 1, jnp.float32(0), jnp.float32(2 * tokens)))
    second = masked(jnp.where(k == 0, jnp.float32(0), jnp.float32(2 * tokens)))

    def queries_of(which, g):
        at = jnp.where(which == 1, at_own[0, TABLE + g], at_d[0, TABLE + g])
        return flat(wq[which, pl.ds(at, per_block)])

    def both_shards(g):
        return attend(queries_of(k, g), all_of(kall, g), all_of(vall, g), scale, first(g))

    def one_shard(g):
        return attend(queries_of(1 - k, g), kall[g, k], vall[g, k], scale, second(g))

    def nearer(g):
        return attend(flat(wc[window(at_c, g)]), all_of(kall, g), all_of(vall, g), scale)

    def gather(ref, table, j, *lead):
        return jnp.concatenate([ref[(*lead, table[0, j * per_block + b])] for b in range(per_block)], axis=0)

    def c_near(g):
        return (
            remote(oc.at[g], rc.at[g], oc_send.at[g], rc_recv.at[g], mate),
            remote(tc.at[g], sc.at[g], tc_send.at[g], sc_recv.at[g], mate),
        )

    def c_relay(g):
        return (
            remote(oc.at[g], rx.at[g], oc_send.at[g], rx_recv.at[g], mate),
            remote(tc.at[g], sx.at[g], tc_send.at[g], sx_recv.at[g], mate),
        )

    def d_copies(g):
        return (
            remote(od.at[g], rd.at[g], od_send.at[g], rd_recv.at[g], up),
            remote(td.at[g], sd.at[g], td_send.at[g], sd_recv.at[g], up),
        )

    pair = 2
    steps = groups // pair

    def complete(p):
        if p == steps - 1:
            return chunks
        return max(0, tokens * routed - capacity * (groups - pair * (p + 1))) // capacity

    def pick(values, i):
        out_ = jnp.int32(values[-1])
        for at, value in enumerate(values[:-1]):
            out_ = jnp.where(i == at, jnp.int32(value), out_)
        return out_

    ends = [complete(p) for p in range(steps)]
    begins = [0] + ends[:-1]
    comes = [min(pair * p, chunks) for p in range(steps + 1)]

    def arrive_near(i):
        @pl.when(feeds)
        def _():
            def one(j):
                for h in range(halves):
                    remote(
                        qc.at[j, part_of(h)], qc.at[j, part_of(h)], qn_send.at[j, h], qc_recv.at[j, h], partner
                    ).wait_recv()
                wc[rows_of(j)] = qc[j]

            each(pick(comes[:-1], i), pick(comes[1:], i), one)

    loose = (chunks - 1) // pair - 1

    def far_results(i):
        @pl.when(jnp.logical_and(odd, above))
        def _():
            def one(j):
                od[j] = gather(op, at_d, j, 0).astype(jnp.bfloat16)
                td[j] = squeeze(gather(lp, at_d, j, 0), padded)

                @pl.when(i >= loose)
                def _():
                    start(d_copies(j))

            each(pick(begins, i), pick(ends, i), one)

    def near_results(i, free):
        def one(j):
            oc[j] = gather(cp, at_c, j)
            tc[j] = squeeze(gather(lc, at_c, j), padded)

            @pl.when(odd)
            def _():
                @pl.when(feeds)
                def _():
                    start(c_relay(j))

            @pl.when(jnp.logical_and(even, free))
            def _():
                start(c_near(j))

        each(pick(begins, i), pick(ends, i), one)

    def block_far(i):
        got = []
        for u in range(pair):
            g = i * pair + u
            got.append((k, g, both_shards(g)))
            got.append((1 - k, g, one_shard(g)))
        for at, g, (o, lse) in got:
            op[at, rows_of(g)] = split(o)
            lp[at, rows_of(g)] = split(lse)

    def block_near(i):
        got = [(i * pair + u, nearer(i * pair + u)) for u in range(pair)]
        for g, (o, lse) in got:
            cp[rows_of(g)] = split(o.astype(jnp.bfloat16))
            lc[rows_of(g)] = split(lse)

    @pl.when(feeds)
    def _():
        remote(tab, tab_c, tab_near.at[0], tab_near.at[1], partner).wait_recv()

    @pl.when(jnp.logical_not(feeds))
    def _():
        tab_c[...] = tab[...]

    local[2].start()
    local[2].wait()

    def step(i, carry):
        block_far(i)
        far_chunk(pair * i + pair)

        @pl.when(i == loose)
        def _():
            @pl.when(jnp.logical_and(odd, above))
            def _():
                each(0, ends[loose - 1], lambda j: start(d_copies(j)))

            @pl.when(jnp.logical_and(even, above))
            def _():
                each(0, ends[loose - 1], lambda j: start(c_near(j)))

        arrive_near(i)
        block_near(i)
        near_results(i, jnp.logical_or(i >= loose, jnp.logical_not(above)))
        far_chunk(pair * i + pair + 1)
        far_results(i)
        return carry

    lax.fori_loop(0, steps, step, 0)

    for i in range(2):
        kv_copy(i).wait_send()

    def sent(there, make):
        @pl.when(there)
        def _():
            def body(g, carry):
                for one in make(g):
                    one.wait_send()
                return carry

            lax.fori_loop(0, chunks, body, 0)

    sent(below, query_down)
    sent(odd, query_near)
    sent(jnp.logical_and(even, above), relay)

    @pl.when(below)
    def _():
        table_down().wait_send()

    @pl.when(odd)
    def _():
        table_near().wait_send()

    @pl.when(jnp.logical_and(even, above))
    def _():
        table_relay().wait_send()

    def join(g):
        @pl.when(jnp.logical_and(jnp.logical_and(even, above), g < chunks))
        def _():
            remote(oc.at[g], rx.at[g], oc_send.at[g], rx_recv.at[g], partner).wait_recv()
            remote(tc.at[g], sx.at[g], tc_send.at[g], sx_recv.at[g], partner).wait_recv()
            mine = (gather(op, at_d, g, 0), gather(lp, at_d, g, 0))
            o, lse = merge([mine, (rx[g], widen(sx[g], capacity))])
            od[g] = o.astype(jnp.bfloat16)
            td[g] = squeeze(lse, padded)
            start(d_copies(g))

    ahead = 2
    for g in range(ahead):
        join(jnp.int32(g))

    def finish(g, carry):
        join(g + ahead)

        @pl.when(odd)
        def _():
            remote(oc.at[g], rc.at[g], oc_send.at[g], rc_recv.at[g], partner).wait_recv()
            remote(tc.at[g], sc.at[g], tc_send.at[g], sc_recv.at[g], partner).wait_recv()

        @pl.when(below)
        def _():
            remote(od.at[g], rd.at[g], od_send.at[g], rd_recv.at[g], partner).wait_recv()
            remote(td.at[g], sd.at[g], td_send.at[g], sd_recv.at[g], partner).wait_recv()

        parts = [
            (gather(op, at_own, g, 1), gather(lp, at_own, g, 1)),
            (rc[g], widen(sc[g], capacity)),
            (rd[g], widen(sd[g], capacity)),
        ]
        fin[pl.ds(pl.multiple_of(g * capacity, BLOCK), capacity), :] = merge(parts)[0].astype(jnp.bfloat16)
        return carry

    sent(jnp.logical_and(odd, feeds), c_relay)

    tile = 256
    tiles = fin.shape[0] // tile
    fin[pl.ds(chunks * capacity, tiles * tile - chunks * capacity), :] = jnp.zeros(
        (tiles * tile - chunks * capacity, width), fin.dtype
    )
    lane = lax.broadcasted_iota(jnp.int32, (tokens, tile), 1).astype(jnp.float32)
    done = 0
    stops = [*range(2, chunks, 2), chunks]
    for s, stop in enumerate(stops):
        lax.fori_loop(stops[s - 1] if s else 0, stop, finish, 0)
        last = stop == chunks
        upto = tiles if last else stop * capacity // tile
        for r in range(routed):
            slot = jnp.broadcast_to(slots[:, r : r + 1], (tokens, tile))
            here = jnp.concatenate(
                [
                    (lane + t * tile == slot).astype(jnp.float32).astype(jnp.bfloat16)
                    for t in range(done, upto)
                ],
                axis=1,
            )
            part_sum = dot(here, fin[done * tile : upto * tile, :])
            total = part_sum if s == 0 else acc[r] + part_sum
            if last:
                wide[pl.ds(r, tokens, stride=routed), :] = total
            else:
                acc[r] = total
        done = upto
    out[...] = wide[pl.ds(0, tokens * routed), :].reshape(tokens, routed, width).astype(jnp.bfloat16)

    sent(above, d_copies)
    sent(even, c_near)


def shards(n, queries, keys, values, routes):
    tokens, routed, width = queries.shape
    context, groups, _ = keys.shape
    capacity = HEADS // groups * MOST
    padded = -(-capacity // LANES) * LANES
    count = -(-(tokens * routed + groups * BLOCK) // capacity)
    cut = (groups * capacity // BLOCK, BLOCK, width)
    vmem = pl.BlockSpec(memory_space=pltpu.VMEM)
    hbm = pl.BlockSpec(memory_space=pltpu.HBM)
    bf = lambda *shape: pltpu.VMEM(shape, jnp.bfloat16)
    f32 = lambda *shape: pltpu.VMEM(shape, jnp.float32)
    sem = lambda *shape: pltpu.SemaphoreType.DMA(shape)
    table = lambda: pltpu.VMEM((1, 2 * TABLE), jnp.int32)
    scalars = lambda: pltpu.SMEM((1, 2 * TABLE), jnp.int32)
    chunks = lambda: bf(count, capacity, width)
    stats = lambda: f32(count, 1, padded)
    return pl.pallas_call(
        functools.partial(kernel, n),
        out_shape=jax.ShapeDtypeStruct((tokens, routed, width), jnp.bfloat16),
        in_specs=[hbm] * 4,
        out_specs=vmem,
        scratch_shapes=[
            bf(tokens, routed, width), pltpu.VMEM((routed, tokens), jnp.int32),
            bf(2, context, groups, width), f32(max(tokens * routed, LANES * groups), width), bf(routed * tokens, 2 * width),
            f32(routed, tokens), f32(tokens, LANES), bf(2, *cut), bf(*cut), f32(*cut),
            bf(groups, 2, context, width), bf(groups, 2, context, width),
            table(), table(), table(), scalars(), scalars(), scalars(),
            bf(count, capacity // BLOCK, BLOCK, width), bf(count, capacity // BLOCK, BLOCK, width),
            f32(2, *cut), f32(2, *cut), bf(*cut), f32(*cut),
            chunks(), stats(), chunks(), stats(),
            chunks(), stats(), chunks(), stats(), chunks(), stats(),
            bf(-(-count * capacity // 256) * 256, width), f32(routed, tokens, width),
        ] + [sem(2), sem(3), sem(2), sem(2), sem(1)] + [sem(2)] * 3
        + [sem(count, 2)] * 5 + [sem(count)] * 10,
        compiler_params=pltpu.CompilerParams(
            collective_id=0, has_side_effects=True, vmem_limit_bytes=48 * 1024 * 1024
        ),
        name="fused",
    )(*(pltpu.with_memory_space_constraint(a, pltpu.HBM) for a in (queries, routes.T, keys, values)))


def solution(mesh):
    n = mesh.shape["seq"]
    placed = (P("seq", None, None), P("seq", None, None), P("seq", None, None), P("seq", None))
    return jax.shard_map(
        functools.partial(shards, n),
        mesh=mesh,
        in_specs=placed,
        out_specs=P("seq", None, None),
        check_vma=False,
    )
```

```python
import functools
import math

import jax
import jax.numpy as jnp
from jax import lax
from jax.experimental import pallas as pl
from jax.experimental.pallas import tpu as pltpu
from jax.sharding import PartitionSpec as P

HEADS = 64
MOST = 40
LANES = 128
LOW = -1e30
BLOCK = 16
TABLE = 256
MESH = pl.DeviceIdType.MESH


def dot(a, b):
    return lax.dot_general(a, b, (((1,), (0,)), ((), ())), preferred_element_type=jnp.float32)


def dot_t(a, b):
    return lax.dot_general(a, b, (((1,), (1,)), ((), ())), preferred_element_type=jnp.float32)


def remote(src, dst, send, recv, device):
    return pltpu.make_async_remote_copy(
        src_ref=src, dst_ref=dst, send_sem=send, recv_sem=recv,
        device_id=(device,), device_id_type=MESH,
    )


def attend(q, k, v, scale, mask=None):
    s = dot_t(q, k) * scale
    if mask is not None:
        s = mask(s)
    top = jnp.max(s, axis=1, keepdims=True)
    p = jnp.exp2(s - top).astype(jnp.bfloat16)
    ones = jnp.ones(v.shape, jnp.bfloat16)
    both = dot(p, jnp.concatenate([v, ones], axis=1))
    width = v.shape[1]
    total = both[:, width:]
    return both[:, :width] / total, top + jnp.log2(total)


def squeeze(lse, padded):
    rows = lse.shape[0]
    return jnp.concatenate([lse, jnp.zeros((padded - rows, LANES), jnp.float32)], axis=0).T[:1]


def widen(row, rows):
    return jnp.concatenate([jnp.broadcast_to(row, (8, row.shape[1]))] * (LANES // 8), axis=0).T[:rows]


def merge(parts):
    top = functools.reduce(jnp.maximum, [lse for _, lse in parts])
    weights = [jnp.exp2(lse - top) for _, lse in parts]
    total = functools.reduce(jnp.add, weights)
    mixed = functools.reduce(jnp.add, [o.astype(jnp.float32) * w for (o, _), w in zip(parts, weights)])
    return mixed / total, top + jnp.log2(total)


def kernel(
    n, q_hbm, routes_hbm, k_hbm, v_hbm, out,
    q_in, routes_t, raw, wide, rights, slot_rows, slots, wq, wc, pos, kall, vall,
    tab, tab_d, tab_c, at_own, at_d, at_c,
    qd, qc, op, lp, cp, lc, oc, tc, od, td, rx, sx, rc, sc, rd, sd, fin, acc,
    in_sem, tab_sem, tab_far, tab_near, tab_relay, raw_sem, kv_send, kv_recv, qn_send, qd_send, qc_recv, qd_recv, relay_send,
    oc_send, tc_send, od_send, td_send,
    rx_recv, sx_recv, rc_recv, sc_recv, rd_recv, sd_recv,
):
    tokens, routed, width = q_in.shape
    groups = kall.shape[0]
    chunks, per_block = qd.shape[:2]
    capacity = per_block * BLOCK
    context = kall.shape[2]
    padded = tc.shape[2]
    per_group = HEADS // groups
    chips = n // 2
    me = lax.axis_index("seq")
    c = me // 2
    k = me % 2
    partner = c * 2 + 1 - k
    even = c % 2 == 0
    odd = c % 2 == 1
    scale = jnp.float32(math.log2(math.e) / math.sqrt(width))
    below = c >= 2
    above = c + 2 < chips
    mate = jnp.where(even, c + 1, c - 1) * 2 + k
    feeds = jnp.logical_or(even, c + 1 < chips)
    down = (c - 2) * 2 + k
    up = (c + 2) * 2 + k

    barrier = pltpu.get_barrier_semaphore()

    def signal(device):
        pl.semaphore_signal(barrier, inc=1, device_id=(device,), device_id_type=MESH)

    signal(partner)
    signal(mate)

    @pl.when(below)
    def _():
        signal(down)

    @pl.when(above)
    def _():
        signal(up)

    ins = [
        pltpu.make_async_copy(a, b, in_sem.at[i])
        for i, (a, b) in enumerate(((routes_hbm, routes_t), (q_hbm, q_in)))
    ]
    raws = [pltpu.make_async_copy(a, raw.at[i], raw_sem.at[i]) for i, a in enumerate((k_hbm, v_hbm))]
    for one in ins + raws:
        one.start()
    ins[0].wait()

    group_of = routes_t[...] // per_group
    group = lax.broadcasted_iota(jnp.int32, (groups, tokens), 0)
    hots = [(group_of[r : r + 1] == group).astype(jnp.float32) for r in range(routed)]
    count = functools.reduce(jnp.add, hots)
    row = lax.broadcasted_iota(jnp.int32, (tokens, tokens), 0)
    col = lax.broadcasted_iota(jnp.int32, (tokens, tokens), 1)
    upper = (row < col).astype(jnp.float32).astype(jnp.bfloat16)
    many = functools.reduce(
        jnp.add, [(group_of[r : r + 1] == group).astype(jnp.int32) for r in range(routed)]
    )
    blocks = (jnp.sum(many, axis=1, keepdims=True) + (BLOCK - 1)) // BLOCK
    blocks = jnp.broadcast_to(blocks, (groups, TABLE))
    starts = [jnp.zeros((1, TABLE), jnp.int32)]
    for g in range(1, groups):
        starts.append(starts[-1] + blocks[g - 1 : g])
    place = lax.broadcasted_iota(jnp.int32, (1, TABLE), 1)
    source = place
    first_block = starts[0]
    for g in range(1, groups):
        source = source + jnp.where(place >= starts[g], per_block - blocks[g - 1 : g], 0)
        first_block = jnp.where(place >= g, starts[g], first_block)
    source = jnp.minimum(source, groups * per_block - 1)
    first_block = jnp.minimum(first_block, chunks * per_block)
    tab[...] = jnp.concatenate([source, first_block], axis=1)
    base = jnp.concatenate(starts, axis=0)[:, :1].astype(jnp.float32) * BLOCK
    rank = dot(count.astype(jnp.bfloat16), upper) + base
    rows = []
    for r in range(routed):
        rows.append(jnp.sum(hots[r] * rank, axis=0, keepdims=True))
        rank = rank + hots[r]
    slot_all = jnp.concatenate(rows, axis=0)
    slot_rows[...] = slot_all
    slots[...] = jnp.concatenate([slot_all] * (LANES // routed), axis=0).T

    ins[1].wait()
    wide[pl.ds(0, tokens * routed), :] = q_in[...].astype(jnp.float32).reshape(tokens * routed, width)
    token = lax.broadcasted_iota(jnp.int32, (tokens, width), 0).astype(jnp.float32).astype(jnp.bfloat16)
    for r in range(routed):
        rights[pl.ds(r * tokens, tokens), :width] = wide[pl.ds(r, tokens, stride=routed), :].astype(jnp.bfloat16)
        rights[pl.ds(r * tokens, tokens), width:] = token

    pl.semaphore_wait(barrier, 2 + below.astype(jnp.int32) + above.astype(jnp.int32))

    def rows_of(j):
        return pl.ds(j * per_block, per_block)

    def split(x):
        return x.reshape(x.shape[0] // BLOCK, BLOCK, width)

    def flat(x):
        return x.reshape(x.shape[0] * BLOCK, width)

    halves = 2
    part_rows = per_block // halves

    def part_of(h):
        return pl.ds(h * part_rows, part_rows)

    def query_part(j, h):
        return wq.at[1, pl.ds(j * per_block + h * part_rows, part_rows)]

    def query_down(j):
        return [
            remote(query_part(j, h), qd.at[j, part_of(h)], qd_send.at[0], qd_recv.at[j, h], down)
            for h in range(halves)
        ]

    def query_near(j):
        return [
            remote(query_part(j, h), qc.at[j, part_of(h)], qn_send.at[0], qc_recv.at[j, h], mate)
            for h in range(halves)
        ]

    def relay_part(j, h):
        return remote(qd.at[j, part_of(h)], qc.at[j, part_of(h)], relay_send.at[0], qc_recv.at[j, h], mate)

    def relay(j):
        return [relay_part(j, h) for h in range(halves)]

    def start(copies):
        for one in copies:
            one.start()

    def table_down():
        return remote(tab, tab_d, tab_far.at[0], tab_far.at[1], down)

    def table_near():
        return remote(tab, tab_c, tab_near.at[0], tab_near.at[1], mate)

    def table_relay():
        return remote(tab_d, tab_c, tab_relay.at[0], tab_near.at[1], mate)

    @pl.when(below)
    def _():
        table_down().start()

    @pl.when(odd)
    def _():
        table_near().start()

    place = lax.broadcasted_iota(jnp.int32, (capacity, tokens), 0).astype(jnp.float32)

    def pack(g, carry):
        at = (g * capacity).astype(jnp.float32)
        here = jnp.concatenate(
            [
                (place == slot_rows[r : r + 1] - at).astype(jnp.float32).astype(jnp.bfloat16)
                for r in range(routed)
            ],
            axis=1,
        )
        both = dot(here, rights[...])
        wq[1, rows_of(g)] = split(both[:, :width].astype(jnp.bfloat16))
        pos[rows_of(g)] = split(both[:, width:])

        @pl.when(below)
        def _():
            start(query_down(g))

        @pl.when(odd)
        def _():
            start(query_near(g))

        return carry

    soon = min(3, chunks)
    lax.fori_loop(0, soon, pack, 0)

    part = 128

    def turn(i, to):
        def body(s, carry):
            at = pl.multiple_of(s * part, part)
            wide[pl.ds(0, part * groups), :] = raw[i, pl.ds(at, part)].astype(jnp.float32).reshape(part * groups, width)
            for g in range(groups):
                to[g, k, pl.ds(at, part), :] = wide[pl.ds(g, part, stride=groups), :].astype(jnp.bfloat16)
            return carry

        lax.fori_loop(0, context // part, body, 0)

    def kv_copy(i):
        a = (kall, vall)[i]
        return remote(a.at[:, k], a.at[:, k], kv_send.at[i], kv_recv.at[i], partner)

    def kv_arrival(i):
        a = (kall, vall)[i]
        return remote(a.at[:, 1 - k], a.at[:, 1 - k], kv_send.at[i], kv_recv.at[i], partner)

    for i, to in enumerate((kall, vall)):
        raws[i].wait()
        turn(i, to)
        kv_copy(i).start()
    lax.fori_loop(soon, chunks, pack, 0)

    local = [
        pltpu.make_async_copy(a, b, tab_sem.at[i])
        for i, (a, b) in enumerate(((tab_d, at_d), (tab, at_own), (tab_c, at_c)))
    ]
    local[1].start()
    rest = (groups - chunks) * per_block
    wq[1, pl.ds(chunks * per_block, rest)] = jnp.zeros((rest, BLOCK, width), wq.dtype)
    pos[pl.ds(chunks * per_block, rest)] = jnp.zeros((rest, BLOCK, width), pos.dtype)
    wq[0, pl.ds(chunks * per_block, rest)] = jnp.zeros((rest, BLOCK, width), wq.dtype)
    wc[pl.ds(chunks * per_block, rest)] = jnp.zeros((rest, BLOCK, width), wc.dtype)

    @pl.when(jnp.logical_not(above))
    def _():
        wq[0] = jnp.zeros(wq.shape[1:], wq.dtype)

    @pl.when(jnp.logical_not(feeds))
    def _():
        wc[...] = jnp.zeros(wc.shape, wc.dtype)

    def each(a, b, body):
        def go(j, carry):
            body(j)
            return carry

        lax.fori_loop(a, b, go, 0)

    @pl.when(above)
    def _():
        remote(tab, tab_d, tab_far.at[0], tab_far.at[1], partner).wait_recv()

        @pl.when(even)
        def _():
            table_relay().start()

    @pl.when(jnp.logical_not(above))
    def _():
        tab_d[...] = tab[...]

    local[0].start()
    local[0].wait()
    local[1].wait()

    def far_chunk(j):
        @pl.when(jnp.logical_and(above, j < chunks))
        def _():
            for h in range(halves):
                remote(
                    qd.at[j, part_of(h)], qd.at[j, part_of(h)], qd_send.at[0], qd_recv.at[j, h], partner
                ).wait_recv()

                @pl.when(even)
                def _(h=h):
                    relay_part(j, h).start()

            wq[0, rows_of(j)] = qd[j]

    far_chunk(jnp.int32(0))

    far_chunk(jnp.int32(1))
    for i in range(2):
        kv_arrival(i).wait_recv()

    column = lax.broadcasted_iota(jnp.int32, (capacity, tokens), 1).astype(jnp.float32)

    def all_of(a, g):
        return a[g].reshape(2 * context, width)

    def window(table, g):
        return pl.ds(table[0, TABLE + g], per_block)

    def masked(bias):
        def of(g):
            limit = flat(pos[window(at_own, g)]) + bias
            limit = jnp.concatenate([limit] * (tokens // LANES), axis=1)

            def mask(x):
                free = x.shape[1] - tokens
                tail = jnp.where(column <= limit, x[:, free:], jnp.float32(LOW))
                return jnp.concatenate([x[:, :free], tail], axis=1)

            return mask

        return of

    first = masked(jnp.where(k == 1, jnp.float32(0), jnp.float32(2 * tokens)))
    second = masked(jnp.where(k == 0, jnp.float32(0), jnp.float32(2 * tokens)))

    def queries_of(which, g):
        at = jnp.where(which == 1, at_own[0, TABLE + g], at_d[0, TABLE + g])
        return flat(wq[which, pl.ds(at, per_block)])

    def both_shards(g):
        return attend(queries_of(k, g), all_of(kall, g), all_of(vall, g), scale, first(g))

    def one_shard(g):
        return attend(queries_of(1 - k, g), kall[g, k], vall[g, k], scale, second(g))

    def nearer(g):
        return attend(flat(wc[window(at_c, g)]), all_of(kall, g), all_of(vall, g), scale)

    def gather(ref, table, j, *lead):
        return jnp.concatenate([ref[(*lead, table[0, j * per_block + b])] for b in range(per_block)], axis=0)

    def c_near(g):
        return (
            remote(oc.at[g], rc.at[g], oc_send.at[0], rc_recv.at[g], mate),
            remote(tc.at[g], sc.at[g], tc_send.at[0], sc_recv.at[g], mate),
        )

    def c_relay(g):
        return (
            remote(oc.at[g], rx.at[g], oc_send.at[0], rx_recv.at[g], mate),
            remote(tc.at[g], sx.at[g], tc_send.at[0], sx_recv.at[g], mate),
        )

    def d_copies(g):
        return (
            remote(od.at[g], rd.at[g], od_send.at[0], rd_recv.at[g], up),
            remote(td.at[g], sd.at[g], td_send.at[0], sd_recv.at[g], up),
        )

    pair = 2
    steps = groups // pair

    def complete(p):
        if p == steps - 1:
            return chunks
        return max(0, tokens * routed - capacity * (groups - pair * (p + 1))) // capacity

    def pick(values, i):
        out_ = jnp.int32(values[-1])
        for at, value in enumerate(values[:-1]):
            out_ = jnp.where(i == at, jnp.int32(value), out_)
        return out_

    ends = [complete(p) for p in range(steps)]
    begins = [0] + ends[:-1]
    comes = [min(pair * p, chunks) for p in range(steps + 1)]

    def arrive_near(i):
        @pl.when(feeds)
        def _():
            def one(j):
                for h in range(halves):
                    remote(
                        qc.at[j, part_of(h)], qc.at[j, part_of(h)], qn_send.at[0], qc_recv.at[j, h], partner
                    ).wait_recv()
                wc[rows_of(j)] = qc[j]

            each(pick(comes[:-1], i), pick(comes[1:], i), one)

    loose = (chunks - 1) // pair - 1

    def far_results(i):
        @pl.when(jnp.logical_and(odd, above))
        def _():
            def one(j):
                od[j] = gather(op, at_d, j, 0).astype(jnp.bfloat16)
                td[j] = squeeze(gather(lp, at_d, j, 0), padded)

                @pl.when(i >= loose)
                def _():
                    start(d_copies(j))

            each(pick(begins, i), pick(ends, i), one)

    def near_results(i, free):
        def one(j):
            oc[j] = gather(cp, at_c, j)
            tc[j] = squeeze(gather(lc, at_c, j), padded)

            @pl.when(odd)
            def _():
                @pl.when(feeds)
                def _():
                    start(c_relay(j))

            @pl.when(jnp.logical_and(even, free))
            def _():
                start(c_near(j))

        each(pick(begins, i), pick(ends, i), one)

    def block_far(i):
        got = []
        for u in range(pair):
            g = i * pair + u
            got.append((k, g, both_shards(g)))
            got.append((1 - k, g, one_shard(g)))
        for at, g, (o, lse) in got:
            op[at, rows_of(g)] = split(o)
            lp[at, rows_of(g)] = split(lse)

    def block_near(i):
        got = [(i * pair + u, nearer(i * pair + u)) for u in range(pair)]
        for g, (o, lse) in got:
            cp[rows_of(g)] = split(o.astype(jnp.bfloat16))
            lc[rows_of(g)] = split(lse)

    @pl.when(feeds)
    def _():
        remote(tab, tab_c, tab_near.at[0], tab_near.at[1], partner).wait_recv()

    @pl.when(jnp.logical_not(feeds))
    def _():
        tab_c[...] = tab[...]

    local[2].start()
    local[2].wait()

    def step(i, carry):
        block_far(i)
        far_chunk(pair * i + pair)

        @pl.when(i == loose)
        def _():
            @pl.when(jnp.logical_and(odd, above))
            def _():
                each(0, ends[loose - 1], lambda j: start(d_copies(j)))

            @pl.when(jnp.logical_and(even, above))
            def _():
                each(0, ends[loose - 1], lambda j: start(c_near(j)))

        arrive_near(i)
        block_near(i)
        near_results(i, jnp.logical_or(i >= loose, jnp.logical_not(above)))
        far_chunk(pair * i + pair + 1)
        far_results(i)
        return carry

    lax.fori_loop(0, steps, step, 0)

    for i in range(2):
        kv_copy(i).wait_send()

    def sent(there, *flows):
        @pl.when(there)
        def _():
            for ref, sem in flows:
                remote(ref, ref, sem.at[0], sem.at[0], partner).wait_send()

    sent(below, (qd, qd_send))
    sent(odd, (qd, qn_send))
    sent(jnp.logical_and(even, above), (qd, relay_send))

    @pl.when(below)
    def _():
        table_down().wait_send()

    @pl.when(odd)
    def _():
        table_near().wait_send()

    @pl.when(jnp.logical_and(even, above))
    def _():
        table_relay().wait_send()

    def join(g):
        @pl.when(jnp.logical_and(jnp.logical_and(even, above), g < chunks))
        def _():
            remote(oc.at[g], rx.at[g], oc_send.at[0], rx_recv.at[g], partner).wait_recv()
            remote(tc.at[g], sx.at[g], tc_send.at[0], sx_recv.at[g], partner).wait_recv()
            mine = (gather(op, at_d, g, 0), gather(lp, at_d, g, 0))
            o, lse = merge([mine, (rx[g], widen(sx[g], capacity))])
            od[g] = o.astype(jnp.bfloat16)
            td[g] = squeeze(lse, padded)
            start(d_copies(g))

    def absent(o, t):
        o[...] = jnp.zeros(o.shape, o.dtype)
        t[...] = jnp.full(t.shape, LOW, t.dtype)

    @pl.when(even)
    def _():
        absent(rc, sc)

    @pl.when(jnp.logical_not(below))
    def _():
        absent(rd, sd)

    ahead = 4
    for g in range(ahead):
        join(jnp.int32(g))

    def finish(g, carry):
        join(g + ahead)

        @pl.when(odd)
        def _():
            remote(oc.at[g], rc.at[g], oc_send.at[0], rc_recv.at[g], partner).wait_recv()
            remote(tc.at[g], sc.at[g], tc_send.at[0], sc_recv.at[g], partner).wait_recv()

        @pl.when(below)
        def _():
            remote(od.at[g], rd.at[g], od_send.at[0], rd_recv.at[g], partner).wait_recv()
            remote(td.at[g], sd.at[g], td_send.at[0], sd_recv.at[g], partner).wait_recv()

        parts = [
            (gather(op, at_own, g, 1), gather(lp, at_own, g, 1)),
            (rc[g], widen(sc[g], capacity)),
            (rd[g], widen(sd[g], capacity)),
        ]
        fin[pl.ds(pl.multiple_of(g * capacity, BLOCK), capacity), :] = merge(parts)[0].astype(jnp.bfloat16)
        return carry

    sent(jnp.logical_and(odd, feeds), (oc, oc_send), (tc, tc_send))

    tile = 256
    tiles = fin.shape[0] // tile
    fin[pl.ds(chunks * capacity, tiles * tile - chunks * capacity), :] = jnp.zeros(
        (tiles * tile - chunks * capacity, width), fin.dtype
    )
    lane = lax.broadcasted_iota(jnp.int32, (tokens, tile), 1).astype(jnp.float32)
    done = 0
    stops = [*range(2, chunks, 2), chunks]
    for s, stop in enumerate(stops):
        lax.fori_loop(stops[s - 1] if s else 0, stop, finish, 0)
        last = stop == chunks
        upto = tiles if last else stop * capacity // tile
        for r in range(routed):
            slot = jnp.broadcast_to(slots[:, r : r + 1], (tokens, tile))
            here = jnp.concatenate(
                [
                    (lane + t * tile == slot).astype(jnp.float32).astype(jnp.bfloat16)
                    for t in range(done, upto)
                ],
                axis=1,
            )
            part_sum = dot(here, fin[done * tile : upto * tile, :])
            total = part_sum if s == 0 else acc[r] + part_sum
            if last:
                wide[pl.ds(r, tokens, stride=routed), :] = total
            else:
                acc[r] = total
        done = upto
    out[...] = wide[pl.ds(0, tokens * routed), :].reshape(tokens, routed, width).astype(jnp.bfloat16)

    sent(above, (od, od_send), (td, td_send))
    sent(even, (oc, oc_send), (tc, tc_send))


def shards(n, queries, keys, values, routes):
    tokens, routed, width = queries.shape
    context, groups, _ = keys.shape
    capacity = HEADS // groups * MOST
    padded = -(-capacity // LANES) * LANES
    count = -(-(tokens * routed + groups * BLOCK) // capacity)
    cut = (groups * capacity // BLOCK, BLOCK, width)
    vmem = pl.BlockSpec(memory_space=pltpu.VMEM)
    hbm = pl.BlockSpec(memory_space=pltpu.HBM)
    bf = lambda *shape: pltpu.VMEM(shape, jnp.bfloat16)
    f32 = lambda *shape: pltpu.VMEM(shape, jnp.float32)
    sem = lambda *shape: pltpu.SemaphoreType.DMA(shape)
    table = lambda: pltpu.VMEM((1, 2 * TABLE), jnp.int32)
    scalars = lambda: pltpu.SMEM((1, 2 * TABLE), jnp.int32)
    chunks = lambda: bf(count, capacity, width)
    stats = lambda: f32(count, 1, padded)
    return pl.pallas_call(
        functools.partial(kernel, n),
        out_shape=jax.ShapeDtypeStruct((tokens, routed, width), jnp.bfloat16),
        in_specs=[hbm] * 4,
        out_specs=vmem,
        scratch_shapes=[
            bf(tokens, routed, width), pltpu.VMEM((routed, tokens), jnp.int32),
            bf(2, context, groups, width), f32(max(tokens * routed, LANES * groups), width), bf(routed * tokens, 2 * width),
            f32(routed, tokens), f32(tokens, LANES), bf(2, *cut), bf(*cut), f32(*cut),
            bf(groups, 2, context, width), bf(groups, 2, context, width),
            table(), table(), table(), scalars(), scalars(), scalars(),
            bf(count, capacity // BLOCK, BLOCK, width), bf(count, capacity // BLOCK, BLOCK, width),
            f32(2, *cut), f32(2, *cut), bf(*cut), f32(*cut),
            chunks(), stats(), chunks(), stats(),
            chunks(), stats(), chunks(), stats(), chunks(), stats(),
            bf(-(-count * capacity // 256) * 256, width), f32(routed, tokens, width),
        ] + [sem(2), sem(3), sem(2), sem(2), sem(1)] + [sem(2)] * 3
        + [sem(1)] * 2 + [sem(count, 2)] * 2 + [sem(1)] * 5 + [sem(count)] * 6,
        compiler_params=pltpu.CompilerParams(
            collective_id=0, has_side_effects=True, vmem_limit_bytes=48 * 1024 * 1024
        ),
        name="fused",
    )(*(pltpu.with_memory_space_constraint(a, pltpu.HBM) for a in (queries, routes.T, keys, values)))


def solution(mesh):
    n = mesh.shape["seq"]
    placed = (P("seq", None, None), P("seq", None, None), P("seq", None, None), P("seq", None))
    return jax.shard_map(
        functools.partial(shards, n),
        mesh=mesh,
        in_specs=placed,
        out_specs=P("seq", None, None),
        check_vma=False,
    )
```

```python
import functools
import math

import jax
import jax.numpy as jnp
from jax import lax
from jax.experimental import pallas as pl
from jax.experimental.pallas import tpu as pltpu
from jax.sharding import PartitionSpec as P

HEADS = 64
MOST = 40
LANES = 128
LOW = -1e30
BLOCK = 16
TABLE = 256
MESH = pl.DeviceIdType.MESH


def dot(a, b):
    return lax.dot_general(a, b, (((1,), (0,)), ((), ())), preferred_element_type=jnp.float32)


def dot_t(a, b):
    return lax.dot_general(a, b, (((1,), (1,)), ((), ())), preferred_element_type=jnp.float32)


def remote(src, dst, send, recv, device):
    return pltpu.make_async_remote_copy(
        src_ref=src, dst_ref=dst, send_sem=send, recv_sem=recv,
        device_id=(device,), device_id_type=MESH,
    )


def attend(q, k, v, scale, mask=None):
    s = dot_t(q, k) * scale
    if mask is not None:
        s = mask(s)
    top = jnp.max(s, axis=1, keepdims=True)
    p = jnp.exp2(s - top).astype(jnp.bfloat16)
    ones = jnp.ones(v.shape, jnp.bfloat16)
    both = dot(p, jnp.concatenate([v, ones], axis=1))
    width = v.shape[1]
    total = both[:, width:]
    return both[:, :width] / total, top + jnp.log2(total)


def squeeze(lse, padded):
    rows = lse.shape[0]
    return jnp.concatenate([lse, jnp.zeros((padded - rows, LANES), jnp.float32)], axis=0).T[:1]


def widen(row, rows):
    return jnp.concatenate([jnp.broadcast_to(row, (8, row.shape[1]))] * (LANES // 8), axis=0).T[:rows]


def merge(parts):
    top = functools.reduce(jnp.maximum, [lse for _, lse in parts])
    weights = [jnp.exp2(lse - top) for _, lse in parts]
    total = functools.reduce(jnp.add, weights)
    mixed = functools.reduce(jnp.add, [o.astype(jnp.float32) * w for (o, _), w in zip(parts, weights)])
    return mixed / total, top + jnp.log2(total)


def kernel(
    n, q_hbm, routes_hbm, k_hbm, v_hbm, out,
    q_in, routes_t, raw, wide, rights, slot_rows, slots, wq, wc, pos, kall, vall,
    tab, tab_d, tab_c, at_own, at_d, at_c,
    qd, qc, op, lp, cp, lc, oc, tc, od, td, rx, sx, rc, sc, rd, sd, fin, acc,
    in_sem, tab_sem, tab_far, tab_near, tab_relay, raw_sem, kv_send, kv_recv, qn_send, qd_send, qc_recv, qd_recv, relay_send,
    oc_send, tc_send, od_send, td_send,
    rx_recv, sx_recv, rc_recv, sc_recv, rd_recv, sd_recv,
):
    tokens, routed, width = q_in.shape
    groups = kall.shape[0]
    chunks, per_block = qd.shape[:2]
    capacity = per_block * BLOCK
    context = kall.shape[2]
    padded = tc.shape[2]
    per_group = HEADS // groups
    chips = n // 2
    me = lax.axis_index("seq")
    c = me // 2
    k = me % 2
    partner = c * 2 + 1 - k
    even = c % 2 == 0
    odd = c % 2 == 1
    scale = jnp.float32(math.log2(math.e) / math.sqrt(width))
    below = c >= 2
    above = c + 2 < chips
    mate = jnp.where(even, c + 1, c - 1) * 2 + k
    feeds = jnp.logical_or(even, c + 1 < chips)
    down = (c - 2) * 2 + k
    up = (c + 2) * 2 + k

    barrier = pltpu.get_barrier_semaphore()

    def signal(device):
        pl.semaphore_signal(barrier, inc=1, device_id=(device,), device_id_type=MESH)

    signal(partner)
    signal(mate)

    @pl.when(below)
    def _():
        signal(down)

    @pl.when(above)
    def _():
        signal(up)

    ins = [
        pltpu.make_async_copy(a, b, in_sem.at[i])
        for i, (a, b) in enumerate(((routes_hbm, routes_t), (q_hbm, q_in)))
    ]
    raws = [pltpu.make_async_copy(a, raw.at[i], raw_sem.at[i]) for i, a in enumerate((k_hbm, v_hbm))]
    for one in ins + raws:
        one.start()
    ins[0].wait()

    group_of = routes_t[...] // per_group
    group = lax.broadcasted_iota(jnp.int32, (groups, tokens), 0)
    hots = [(group_of[r : r + 1] == group).astype(jnp.float32) for r in range(routed)]
    count = functools.reduce(jnp.add, hots)
    row = lax.broadcasted_iota(jnp.int32, (tokens, tokens), 0)
    col = lax.broadcasted_iota(jnp.int32, (tokens, tokens), 1)
    upper = (row < col).astype(jnp.float32).astype(jnp.bfloat16)
    many = functools.reduce(
        jnp.add, [(group_of[r : r + 1] == group).astype(jnp.int32) for r in range(routed)]
    )
    blocks = (jnp.sum(many, axis=1, keepdims=True) + (BLOCK - 1)) // BLOCK
    blocks = jnp.broadcast_to(blocks, (groups, TABLE))
    starts = [jnp.zeros((1, TABLE), jnp.int32)]
    for g in range(1, groups):
        starts.append(starts[-1] + blocks[g - 1 : g])
    place = lax.broadcasted_iota(jnp.int32, (1, TABLE), 1)
    source = place
    first_block = starts[0]
    for g in range(1, groups):
        source = source + jnp.where(place >= starts[g], per_block - blocks[g - 1 : g], 0)
        first_block = jnp.where(place >= g, starts[g], first_block)
    source = jnp.minimum(source, groups * per_block - 1)
    first_block = jnp.minimum(first_block, chunks * per_block)
    tab[...] = jnp.concatenate([source, first_block], axis=1)
    base = jnp.concatenate(starts, axis=0)[:, :1].astype(jnp.float32) * BLOCK
    rank = dot(count.astype(jnp.bfloat16), upper) + base
    rows = []
    for r in range(routed):
        rows.append(jnp.sum(hots[r] * rank, axis=0, keepdims=True))
        rank = rank + hots[r]
    slot_all = jnp.concatenate(rows, axis=0)
    slot_rows[...] = slot_all
    slots[...] = jnp.concatenate([slot_all] * (LANES // routed), axis=0).T

    ins[1].wait()
    wide[pl.ds(0, tokens * routed), :] = q_in[...].astype(jnp.float32).reshape(tokens * routed, width)
    token = lax.broadcasted_iota(jnp.int32, (tokens, width), 0).astype(jnp.float32).astype(jnp.bfloat16)
    for r in range(routed):
        rights[pl.ds(r * tokens, tokens), :width] = wide[pl.ds(r, tokens, stride=routed), :].astype(jnp.bfloat16)
        rights[pl.ds(r * tokens, tokens), width:] = token

    pl.semaphore_wait(barrier, 2 + below.astype(jnp.int32) + above.astype(jnp.int32))

    def rows_of(j):
        return pl.ds(j * per_block, per_block)

    def split(x):
        return x.reshape(x.shape[0] // BLOCK, BLOCK, width)

    def flat(x):
        return x.reshape(x.shape[0] * BLOCK, width)

    halves = 2
    part_rows = per_block // halves

    def part_of(h):
        return pl.ds(h * part_rows, part_rows)

    def query_part(j, h):
        return wq.at[1, pl.ds(j * per_block + h * part_rows, part_rows)]

    def query_down(j):
        return [
            remote(query_part(j, h), qd.at[j, part_of(h)], qd_send.at[0], qd_recv.at[j, h], down)
            for h in range(halves)
        ]

    def query_near(j):
        return [
            remote(query_part(j, h), qc.at[j, part_of(h)], qn_send.at[0], qc_recv.at[j, h], mate)
            for h in range(halves)
        ]

    def relay_part(j, h):
        return remote(qd.at[j, part_of(h)], qc.at[j, part_of(h)], relay_send.at[0], qc_recv.at[j, h], mate)

    def relay(j):
        return [relay_part(j, h) for h in range(halves)]

    def start(copies):
        for one in copies:
            one.start()

    def table_down():
        return remote(tab, tab_d, tab_far.at[0], tab_far.at[1], down)

    def table_near():
        return remote(tab, tab_c, tab_near.at[0], tab_near.at[1], mate)

    def table_relay():
        return remote(tab_d, tab_c, tab_relay.at[0], tab_near.at[1], mate)

    @pl.when(below)
    def _():
        table_down().start()

    @pl.when(odd)
    def _():
        table_near().start()

    place = lax.broadcasted_iota(jnp.int32, (capacity, tokens), 0).astype(jnp.float32)

    def pack(g, carry):
        at = (g * capacity).astype(jnp.float32)
        here = jnp.concatenate(
            [
                (place == slot_rows[r : r + 1] - at).astype(jnp.float32).astype(jnp.bfloat16)
                for r in range(routed)
            ],
            axis=1,
        )
        both = dot(here, rights[...])
        wq[1, rows_of(g)] = split(both[:, :width].astype(jnp.bfloat16))
        pos[rows_of(g)] = split(both[:, width:])

        @pl.when(below)
        def _():
            start(query_down(g))

        @pl.when(odd)
        def _():
            start(query_near(g))

        return carry

    soon = min(3, chunks)
    lax.fori_loop(0, soon, pack, 0)

    part = 128

    def turn(i, to):
        def body(s, carry):
            at = pl.multiple_of(s * part, part)
            wide[pl.ds(0, part * groups), :] = raw[i, pl.ds(at, part)].astype(jnp.float32).reshape(part * groups, width)
            for g in range(groups):
                to[g, k, pl.ds(at, part), :] = wide[pl.ds(g, part, stride=groups), :].astype(jnp.bfloat16)
            return carry

        lax.fori_loop(0, context // part, body, 0)

    def kv_copy(i):
        a = (kall, vall)[i]
        return remote(a.at[:, k], a.at[:, k], kv_send.at[i], kv_recv.at[i], partner)

    def kv_arrival(i):
        a = (kall, vall)[i]
        return remote(a.at[:, 1 - k], a.at[:, 1 - k], kv_send.at[i], kv_recv.at[i], partner)

    for i, to in enumerate((kall, vall)):
        raws[i].wait()
        turn(i, to)
        kv_copy(i).start()
    lax.fori_loop(soon, chunks, pack, 0)

    local = [
        pltpu.make_async_copy(a, b, tab_sem.at[i])
        for i, (a, b) in enumerate(((tab_d, at_d), (tab, at_own), (tab_c, at_c)))
    ]
    local[1].start()
    rest = (groups - chunks) * per_block
    wq[1, pl.ds(chunks * per_block, rest)] = jnp.zeros((rest, BLOCK, width), wq.dtype)
    pos[pl.ds(chunks * per_block, rest)] = jnp.zeros((rest, BLOCK, width), pos.dtype)
    wq[0, pl.ds(chunks * per_block, rest)] = jnp.zeros((rest, BLOCK, width), wq.dtype)
    wc[pl.ds(chunks * per_block, rest)] = jnp.zeros((rest, BLOCK, width), wc.dtype)

    @pl.when(jnp.logical_not(above))
    def _():
        wq[0] = jnp.zeros(wq.shape[1:], wq.dtype)

    @pl.when(jnp.logical_not(feeds))
    def _():
        wc[...] = jnp.zeros(wc.shape, wc.dtype)

    def each(a, b, body):
        def go(j, carry):
            body(j)
            return carry

        lax.fori_loop(a, b, go, 0)

    @pl.when(above)
    def _():
        remote(tab, tab_d, tab_far.at[0], tab_far.at[1], partner).wait_recv()

        @pl.when(even)
        def _():
            table_relay().start()

    @pl.when(jnp.logical_not(above))
    def _():
        tab_d[...] = tab[...]

    local[0].start()
    local[0].wait()
    local[1].wait()

    def far_chunk(j):
        @pl.when(jnp.logical_and(above, j < chunks))
        def _():
            for h in range(halves):
                remote(
                    qd.at[j, part_of(h)], qd.at[j, part_of(h)], qd_send.at[0], qd_recv.at[j, h], partner
                ).wait_recv()

                @pl.when(even)
                def _(h=h):
                    relay_part(j, h).start()

            wq[0, rows_of(j)] = qd[j]

    far_chunk(jnp.int32(0))

    far_chunk(jnp.int32(1))
    for i in range(2):
        kv_arrival(i).wait_recv()

    column = lax.broadcasted_iota(jnp.int32, (capacity, tokens), 1).astype(jnp.float32)

    def all_of(a, g):
        return a[g].reshape(2 * context, width)

    def window(table, g):
        return pl.ds(table[0, TABLE + g], per_block)

    def masked(bias):
        def of(g):
            limit = flat(pos[window(at_own, g)]) + bias
            limit = jnp.concatenate([limit] * (tokens // LANES), axis=1)

            def mask(x):
                free = x.shape[1] - tokens
                tail = jnp.where(column <= limit, x[:, free:], jnp.float32(LOW))
                return jnp.concatenate([x[:, :free], tail], axis=1)

            return mask

        return of

    first = masked(jnp.where(k == 1, jnp.float32(0), jnp.float32(2 * tokens)))
    second = masked(jnp.where(k == 0, jnp.float32(0), jnp.float32(2 * tokens)))

    def queries_of(which, g):
        at = jnp.where(which == 1, at_own[0, TABLE + g], at_d[0, TABLE + g])
        return flat(wq[which, pl.ds(at, per_block)])

    def both_shards(g):
        return attend(queries_of(k, g), all_of(kall, g), all_of(vall, g), scale, first(g))

    def one_shard(g):
        return attend(queries_of(1 - k, g), kall[g, k], vall[g, k], scale, second(g))

    def nearer(g):
        return attend(flat(wc[window(at_c, g)]), all_of(kall, g), all_of(vall, g), scale)

    def gather(ref, table, j, *lead):
        return jnp.concatenate([ref[(*lead, table[0, j * per_block + b])] for b in range(per_block)], axis=0)

    def c_near(g):
        return (
            remote(oc.at[g], rc.at[g], oc_send.at[0], rc_recv.at[g], mate),
            remote(tc.at[g], sc.at[g], tc_send.at[0], sc_recv.at[g], mate),
        )

    def c_relay(g):
        return (
            remote(oc.at[g], rx.at[g], oc_send.at[0], rx_recv.at[g], mate),
            remote(tc.at[g], sx.at[g], tc_send.at[0], sx_recv.at[g], mate),
        )

    def d_copies(g):
        return (
            remote(od.at[g], rd.at[g], od_send.at[0], rd_recv.at[g], up),
            remote(td.at[g], sd.at[g], td_send.at[0], sd_recv.at[g], up),
        )

    pair = 2
    steps = groups // pair

    def complete(p):
        if p == steps - 1:
            return chunks
        return max(0, tokens * routed - capacity * (groups - pair * (p + 1))) // capacity

    def pick(values, i):
        out_ = jnp.int32(values[-1])
        for at, value in enumerate(values[:-1]):
            out_ = jnp.where(i == at, jnp.int32(value), out_)
        return out_

    ends = [complete(p) for p in range(steps)]
    begins = [0] + ends[:-1]
    comes = [min(pair * p, chunks) for p in range(steps + 1)]

    def arrive_near(i):
        @pl.when(feeds)
        def _():
            def one(j):
                for h in range(halves):
                    remote(
                        qc.at[j, part_of(h)], qc.at[j, part_of(h)], qn_send.at[0], qc_recv.at[j, h], partner
                    ).wait_recv()
                wc[rows_of(j)] = qc[j]

            each(pick(comes[:-1], i), pick(comes[1:], i), one)

    loose = (chunks - 1) // pair - 1

    def far_results(i):
        @pl.when(jnp.logical_and(odd, above))
        def _():
            def one(j):
                od[j] = gather(op, at_d, j, 0).astype(jnp.bfloat16)
                td[j] = squeeze(gather(lp, at_d, j, 0), padded)

                @pl.when(i >= loose)
                def _():
                    start(d_copies(j))

            each(pick(begins, i), pick(ends, i), one)

    def near_results(i, free):
        def one(j):
            oc[j] = gather(cp, at_c, j)
            tc[j] = squeeze(gather(lc, at_c, j), padded)

            @pl.when(odd)
            def _():
                @pl.when(feeds)
                def _():
                    start(c_relay(j))

            @pl.when(jnp.logical_and(even, free))
            def _():
                start(c_near(j))

        each(pick(begins, i), pick(ends, i), one)

    def block_far(i):
        got = []
        for u in range(pair):
            g = i * pair + u
            got.append((k, g, both_shards(g)))
            got.append((1 - k, g, one_shard(g)))
        for at, g, (o, lse) in got:
            op[at, rows_of(g)] = split(o)
            lp[at, rows_of(g)] = split(lse)

    def block_near(i):
        got = [(i * pair + u, nearer(i * pair + u)) for u in range(pair)]
        for g, (o, lse) in got:
            cp[rows_of(g)] = split(o.astype(jnp.bfloat16))
            lc[rows_of(g)] = split(lse)

    @pl.when(feeds)
    def _():
        remote(tab, tab_c, tab_near.at[0], tab_near.at[1], partner).wait_recv()

    @pl.when(jnp.logical_not(feeds))
    def _():
        tab_c[...] = tab[...]

    local[2].start()
    local[2].wait()

    def join(g):
        @pl.when(jnp.logical_and(jnp.logical_and(even, above), g < chunks))
        def _():
            remote(oc.at[g], rx.at[g], oc_send.at[0], rx_recv.at[g], partner).wait_recv()
            remote(tc.at[g], sx.at[g], tc_send.at[0], sx_recv.at[g], partner).wait_recv()
            mine = (gather(op, at_d, g, 0), gather(lp, at_d, g, 0))
            o, lse = merge([mine, (rx[g], widen(sx[g], capacity))])
            od[g] = o.astype(jnp.bfloat16)
            td[g] = squeeze(lse, padded)
            start(d_copies(g))

    def step(i, carry):
        block_far(i)
        far_chunk(pair * i + pair)

        @pl.when(i == loose)
        def _():
            @pl.when(jnp.logical_and(odd, above))
            def _():
                each(0, ends[loose - 1], lambda j: start(d_copies(j)))

            @pl.when(jnp.logical_and(even, above))
            def _():
                each(0, ends[loose - 1], lambda j: start(c_near(j)))

        @pl.when(i == steps - 1)
        def _():
            join(jnp.int32(0))

        arrive_near(i)
        block_near(i)
        near_results(i, jnp.logical_or(i >= loose, jnp.logical_not(above)))
        far_chunk(pair * i + pair + 1)
        far_results(i)
        return carry

    lax.fori_loop(0, steps, step, 0)

    for i in range(2):
        kv_copy(i).wait_send()

    def sent(there, *flows):
        @pl.when(there)
        def _():
            for ref, sem in flows:
                remote(ref, ref, sem.at[0], sem.at[0], partner).wait_send()

    sent(below, (qd, qd_send))
    sent(odd, (qd, qn_send))
    sent(jnp.logical_and(even, above), (qd, relay_send))

    @pl.when(below)
    def _():
        table_down().wait_send()

    @pl.when(odd)
    def _():
        table_near().wait_send()

    @pl.when(jnp.logical_and(even, above))
    def _():
        table_relay().wait_send()

    def absent(o, t):
        o[...] = jnp.zeros(o.shape, o.dtype)
        t[...] = jnp.full(t.shape, LOW, t.dtype)

    @pl.when(even)
    def _():
        absent(rc, sc)

    @pl.when(jnp.logical_not(below))
    def _():
        absent(rd, sd)

    ahead = 3
    for g in range(1, ahead):
        join(jnp.int32(g))

    def finish(g, carry):
        join(g + ahead)

        @pl.when(odd)
        def _():
            remote(oc.at[g], rc.at[g], oc_send.at[0], rc_recv.at[g], partner).wait_recv()
            remote(tc.at[g], sc.at[g], tc_send.at[0], sc_recv.at[g], partner).wait_recv()

        @pl.when(below)
        def _():
            remote(od.at[g], rd.at[g], od_send.at[0], rd_recv.at[g], partner).wait_recv()
            remote(td.at[g], sd.at[g], td_send.at[0], sd_recv.at[g], partner).wait_recv()

        parts = [
            (gather(op, at_own, g, 1), gather(lp, at_own, g, 1)),
            (rc[g], widen(sc[g], capacity)),
            (rd[g], widen(sd[g], capacity)),
        ]
        fin[pl.ds(pl.multiple_of(g * capacity, BLOCK), capacity), :] = merge(parts)[0].astype(jnp.bfloat16)
        return carry

    sent(jnp.logical_and(odd, feeds), (oc, oc_send), (tc, tc_send))

    tile = 256
    tiles = fin.shape[0] // tile
    fin[pl.ds(chunks * capacity, tiles * tile - chunks * capacity), :] = jnp.zeros(
        (tiles * tile - chunks * capacity, width), fin.dtype
    )
    lane = lax.broadcasted_iota(jnp.int32, (tokens, tile), 1).astype(jnp.float32)
    done = 0
    stops = [*range(2, chunks, 2), chunks]
    for s, stop in enumerate(stops):
        lax.fori_loop(stops[s - 1] if s else 0, stop, finish, 0)
        last = stop == chunks
        upto = tiles if last else stop * capacity // tile
        for r in range(routed):
            slot = jnp.broadcast_to(slots[:, r : r + 1], (tokens, tile))
            here = jnp.concatenate(
                [
                    (lane + t * tile == slot).astype(jnp.float32).astype(jnp.bfloat16)
                    for t in range(done, upto)
                ],
                axis=1,
            )
            part_sum = dot(here, fin[done * tile : upto * tile, :])
            total = part_sum if s == 0 else acc[r] + part_sum
            if last:
                wide[pl.ds(r, tokens, stride=routed), :] = total
            else:
                acc[r] = total
        done = upto
    out[...] = wide[pl.ds(0, tokens * routed), :].reshape(tokens, routed, width).astype(jnp.bfloat16)

    sent(above, (od, od_send), (td, td_send))
    sent(even, (oc, oc_send), (tc, tc_send))


def shards(n, queries, keys, values, routes):
    tokens, routed, width = queries.shape
    context, groups, _ = keys.shape
    capacity = HEADS // groups * MOST
    padded = -(-capacity // LANES) * LANES
    count = -(-(tokens * routed + groups * BLOCK) // capacity)
    cut = (groups * capacity // BLOCK, BLOCK, width)
    vmem = pl.BlockSpec(memory_space=pltpu.VMEM)
    hbm = pl.BlockSpec(memory_space=pltpu.HBM)
    bf = lambda *shape: pltpu.VMEM(shape, jnp.bfloat16)
    f32 = lambda *shape: pltpu.VMEM(shape, jnp.float32)
    sem = lambda *shape: pltpu.SemaphoreType.DMA(shape)
    table = lambda: pltpu.VMEM((1, 2 * TABLE), jnp.int32)
    scalars = lambda: pltpu.SMEM((1, 2 * TABLE), jnp.int32)
    chunks = lambda: bf(count, capacity, width)
    stats = lambda: f32(count, 1, padded)
    return pl.pallas_call(
        functools.partial(kernel, n),
        out_shape=jax.ShapeDtypeStruct((tokens, routed, width), jnp.bfloat16),
        in_specs=[hbm] * 4,
        out_specs=vmem,
        scratch_shapes=[
            bf(tokens, routed, width), pltpu.VMEM((routed, tokens), jnp.int32),
            bf(2, context, groups, width), f32(max(tokens * routed, LANES * groups), width), bf(routed * tokens, 2 * width),
            f32(routed, tokens), f32(tokens, LANES), bf(2, *cut), bf(*cut), f32(*cut),
            bf(groups, 2, context, width), bf(groups, 2, context, width),
            table(), table(), table(), scalars(), scalars(), scalars(),
            bf(count, capacity // BLOCK, BLOCK, width), bf(count, capacity // BLOCK, BLOCK, width),
            f32(2, *cut), f32(2, *cut), bf(*cut), f32(*cut),
            chunks(), stats(), chunks(), stats(),
            chunks(), stats(), chunks(), stats(), chunks(), stats(),
            bf(-(-count * capacity // 256) * 256, width), f32(routed, tokens, width),
        ] + [sem(2), sem(3), sem(2), sem(2), sem(1)] + [sem(2)] * 3
        + [sem(1)] * 2 + [sem(count, 2)] * 2 + [sem(1)] * 5 + [sem(count)] * 6,
        compiler_params=pltpu.CompilerParams(
            collective_id=0, has_side_effects=True, vmem_limit_bytes=48 * 1024 * 1024
        ),
        name="fused",
    )(*(pltpu.with_memory_space_constraint(a, pltpu.HBM) for a in (queries, routes.T, keys, values)))


def solution(mesh):
    n = mesh.shape["seq"]
    placed = (P("seq", None, None), P("seq", None, None), P("seq", None, None), P("seq", None))
    return jax.shard_map(
        functools.partial(shards, n),
        mesh=mesh,
        in_specs=placed,
        out_specs=P("seq", None, None),
        check_vma=False,
    )
```

```python
import functools
import math

import jax
import jax.numpy as jnp
from jax import lax
from jax.experimental import pallas as pl
from jax.experimental.pallas import tpu as pltpu
from jax.sharding import PartitionSpec as P

HEADS = 64
MOST = 40
LANES = 128
LOW = -1e30
BLOCK = 16
TABLE = 256
MESH = pl.DeviceIdType.MESH


def dot(a, b):
    return lax.dot_general(a, b, (((1,), (0,)), ((), ())), preferred_element_type=jnp.float32)


def dot_t(a, b):
    return lax.dot_general(a, b, (((1,), (1,)), ((), ())), preferred_element_type=jnp.float32)


def remote(src, dst, send, recv, device):
    return pltpu.make_async_remote_copy(
        src_ref=src, dst_ref=dst, send_sem=send, recv_sem=recv,
        device_id=(device,), device_id_type=MESH,
    )


def attend(q, k, v, scale, mask=None):
    s = dot_t(q, k) * scale
    if mask is not None:
        s = mask(s)
    top = jnp.max(s, axis=1, keepdims=True)
    p = jnp.exp2(s - top).astype(jnp.bfloat16)
    ones = jnp.ones(v.shape, jnp.bfloat16)
    both = dot(p, jnp.concatenate([v, ones], axis=1))
    width = v.shape[1]
    total = both[:, width:]
    return both[:, :width] / total, top + jnp.log2(total)


def squeeze(lse, padded):
    rows = lse.shape[0]
    return jnp.concatenate([lse, jnp.zeros((padded - rows, LANES), jnp.float32)], axis=0).T[:1]


def widen(row, rows):
    return jnp.concatenate([jnp.broadcast_to(row, (8, row.shape[1]))] * (LANES // 8), axis=0).T[:rows]


def merge(parts):
    top = functools.reduce(jnp.maximum, [lse for _, lse in parts])
    weights = [jnp.exp2(lse - top) for _, lse in parts]
    total = functools.reduce(jnp.add, weights)
    mixed = functools.reduce(jnp.add, [o.astype(jnp.float32) * w for (o, _), w in zip(parts, weights)])
    return mixed / total, top + jnp.log2(total)


def kernel(
    n, q_hbm, routes_hbm, k_hbm, v_hbm, out,
    q_in, routes_t, raw, wide, rights, slot_rows, slots, wq, wc, pos, kall, vall,
    tab, tab_d, tab_c, at_own, at_d, at_c,
    qd, qc, op, lp, cp, lc, oc, tc, od, td, rx, sx, rc, sc, rd, sd, fin, acc,
    in_sem, tab_sem, tab_far, tab_near, tab_relay, raw_sem, kv_send, kv_recv, qn_send, qd_send, qc_recv, qd_recv, relay_send,
    oc_send, tc_send, od_send, td_send,
    rx_recv, sx_recv, rc_recv, sc_recv, rd_recv, sd_recv,
):
    tokens, routed, width = q_in.shape
    groups = kall.shape[0]
    chunks, per_block = qd.shape[:2]
    capacity = per_block * BLOCK
    context = kall.shape[2]
    padded = tc.shape[2]
    per_group = HEADS // groups
    chips = n // 2
    me = lax.axis_index("seq")
    c = me // 2
    k = me % 2
    partner = c * 2 + 1 - k
    even = c % 2 == 0
    odd = c % 2 == 1
    scale = jnp.float32(math.log2(math.e) / math.sqrt(width))
    below = c >= 2
    above = c + 2 < chips
    mate = jnp.where(even, c + 1, c - 1) * 2 + k
    feeds = jnp.logical_or(even, c + 1 < chips)
    down = (c - 2) * 2 + k
    up = (c + 2) * 2 + k

    barrier = pltpu.get_barrier_semaphore()

    def signal(device):
        pl.semaphore_signal(barrier, inc=1, device_id=(device,), device_id_type=MESH)

    signal(partner)
    signal(mate)

    @pl.when(below)
    def _():
        signal(down)

    @pl.when(above)
    def _():
        signal(up)

    ins = [
        pltpu.make_async_copy(a, b, in_sem.at[i])
        for i, (a, b) in enumerate(((routes_hbm, routes_t), (q_hbm, q_in)))
    ]
    raws = [pltpu.make_async_copy(a, raw.at[i], raw_sem.at[i]) for i, a in enumerate((k_hbm, v_hbm))]
    for one in ins:
        one.start()
    ins[0].wait()

    group_of = routes_t[...] // per_group
    group = lax.broadcasted_iota(jnp.int32, (groups, tokens), 0)
    hots = [(group_of[r : r + 1] == group).astype(jnp.float32) for r in range(routed)]
    count = functools.reduce(jnp.add, hots)
    row = lax.broadcasted_iota(jnp.int32, (tokens, tokens), 0)
    col = lax.broadcasted_iota(jnp.int32, (tokens, tokens), 1)
    upper = (row < col).astype(jnp.float32).astype(jnp.bfloat16)
    many = functools.reduce(
        jnp.add, [(group_of[r : r + 1] == group).astype(jnp.int32) for r in range(routed)]
    )
    blocks = (jnp.sum(many, axis=1, keepdims=True) + (BLOCK - 1)) // BLOCK
    blocks = jnp.broadcast_to(blocks, (groups, TABLE))
    starts = [jnp.zeros((1, TABLE), jnp.int32)]
    for g in range(1, groups):
        starts.append(starts[-1] + blocks[g - 1 : g])
    place = lax.broadcasted_iota(jnp.int32, (1, TABLE), 1)
    source = place
    first_block = starts[0]
    for g in range(1, groups):
        source = source + jnp.where(place >= starts[g], per_block - blocks[g - 1 : g], 0)
        first_block = jnp.where(place >= g, starts[g], first_block)
    source = jnp.minimum(source, groups * per_block - 1)
    first_block = jnp.minimum(first_block, chunks * per_block)
    tab[...] = jnp.concatenate([source, first_block], axis=1)
    base = jnp.concatenate(starts, axis=0)[:, :1].astype(jnp.float32) * BLOCK
    rank = dot(count.astype(jnp.bfloat16), upper) + base
    rows = []
    for r in range(routed):
        rows.append(jnp.sum(hots[r] * rank, axis=0, keepdims=True))
        rank = rank + hots[r]
    slot_all = jnp.concatenate(rows, axis=0)
    slot_rows[...] = slot_all
    slots[...] = jnp.concatenate([slot_all] * (LANES // routed), axis=0).T

    ins[1].wait()
    for one in raws:
        one.start()
    wide[pl.ds(0, tokens * routed), :] = q_in[...].astype(jnp.float32).reshape(tokens * routed, width)
    token = lax.broadcasted_iota(jnp.int32, (tokens, width), 0).astype(jnp.float32).astype(jnp.bfloat16)
    for r in range(routed):
        rights[pl.ds(r * tokens, tokens), :width] = wide[pl.ds(r, tokens, stride=routed), :].astype(jnp.bfloat16)
        rights[pl.ds(r * tokens, tokens), width:] = token


    def rows_of(j):
        return pl.ds(j * per_block, per_block)

    def split(x):
        return x.reshape(x.shape[0] // BLOCK, BLOCK, width)

    def flat(x):
        return x.reshape(x.shape[0] * BLOCK, width)

    halves = 2
    part_rows = per_block // halves

    def part_of(h):
        return pl.ds(h * part_rows, part_rows)

    def query_part(j, h):
        return wq.at[1, pl.ds(j * per_block + h * part_rows, part_rows)]

    def query_down(j):
        return [
            remote(query_part(j, h), qd.at[j, part_of(h)], qd_send.at[0], qd_recv.at[j, h], down)
            for h in range(halves)
        ]

    def query_near(j):
        return [
            remote(query_part(j, h), qc.at[j, part_of(h)], qn_send.at[0], qc_recv.at[j, h], mate)
            for h in range(halves)
        ]

    def relay_part(j, h):
        return remote(qd.at[j, part_of(h)], qc.at[j, part_of(h)], relay_send.at[0], qc_recv.at[j, h], mate)

    def relay(j):
        return [relay_part(j, h) for h in range(halves)]

    def start(copies):
        for one in copies:
            one.start()

    def table_down():
        return remote(tab, tab_d, tab_far.at[0], tab_far.at[1], down)

    def table_near():
        return remote(tab, tab_c, tab_near.at[0], tab_near.at[1], mate)

    def table_relay():
        return remote(tab_d, tab_c, tab_relay.at[0], tab_near.at[1], mate)

    place = lax.broadcasted_iota(jnp.int32, (capacity, tokens), 0).astype(jnp.float32)

    def pack_rows(g):
        at = (g * capacity).astype(jnp.float32)
        here = jnp.concatenate(
            [
                (place == slot_rows[r : r + 1] - at).astype(jnp.float32).astype(jnp.bfloat16)
                for r in range(routed)
            ],
            axis=1,
        )
        both = dot(here, rights[...])
        wq[1, rows_of(g)] = split(both[:, :width].astype(jnp.bfloat16))
        pos[rows_of(g)] = split(both[:, width:])

    def pack_send(g):
        @pl.when(below)
        def _():
            start(query_down(g))

        @pl.when(odd)
        def _():
            start(query_near(g))

    def pack(g, carry):
        pack_rows(g)
        pack_send(g)
        return carry

    pack_rows(jnp.int32(0))
    pl.semaphore_wait(barrier, 2 + below.astype(jnp.int32) + above.astype(jnp.int32))

    @pl.when(below)
    def _():
        table_down().start()

    @pl.when(odd)
    def _():
        table_near().start()

    pack_send(jnp.int32(0))
    soon = min(3, chunks)
    lax.fori_loop(1, soon, pack, 0)

    part = 128

    def turn(i, to):
        def body(s, carry):
            at = pl.multiple_of(s * part, part)
            wide[pl.ds(0, part * groups), :] = raw[i, pl.ds(at, part)].astype(jnp.float32).reshape(part * groups, width)
            for g in range(groups):
                to[g, k, pl.ds(at, part), :] = wide[pl.ds(g, part, stride=groups), :].astype(jnp.bfloat16)
            return carry

        lax.fori_loop(0, context // part, body, 0)

    def kv_copy(i):
        a = (kall, vall)[i]
        return remote(a.at[:, k], a.at[:, k], kv_send.at[i], kv_recv.at[i], partner)

    def kv_arrival(i):
        a = (kall, vall)[i]
        return remote(a.at[:, 1 - k], a.at[:, 1 - k], kv_send.at[i], kv_recv.at[i], partner)

    for i, to in enumerate((kall, vall)):
        raws[i].wait()
        turn(i, to)
        kv_copy(i).start()
    lax.fori_loop(soon, chunks, pack, 0)

    local = [
        pltpu.make_async_copy(a, b, tab_sem.at[i])
        for i, (a, b) in enumerate(((tab_d, at_d), (tab, at_own), (tab_c, at_c)))
    ]
    local[1].start()
    rest = (groups - chunks) * per_block
    wq[1, pl.ds(chunks * per_block, rest)] = jnp.zeros((rest, BLOCK, width), wq.dtype)
    pos[pl.ds(chunks * per_block, rest)] = jnp.zeros((rest, BLOCK, width), pos.dtype)
    wq[0, pl.ds(chunks * per_block, rest)] = jnp.zeros((rest, BLOCK, width), wq.dtype)
    wc[pl.ds(chunks * per_block, rest)] = jnp.zeros((rest, BLOCK, width), wc.dtype)

    @pl.when(jnp.logical_not(above))
    def _():
        wq[0] = jnp.zeros(wq.shape[1:], wq.dtype)

    @pl.when(jnp.logical_not(feeds))
    def _():
        wc[...] = jnp.zeros(wc.shape, wc.dtype)

    def each(a, b, body):
        def go(j, carry):
            body(j)
            return carry

        lax.fori_loop(a, b, go, 0)

    @pl.when(above)
    def _():
        remote(tab, tab_d, tab_far.at[0], tab_far.at[1], partner).wait_recv()

        @pl.when(even)
        def _():
            table_relay().start()

    @pl.when(jnp.logical_not(above))
    def _():
        tab_d[...] = tab[...]

    local[0].start()
    local[0].wait()
    local[1].wait()

    def far_chunk(j):
        @pl.when(jnp.logical_and(above, j < chunks))
        def _():
            for h in range(halves):
                remote(
                    qd.at[j, part_of(h)], qd.at[j, part_of(h)], qd_send.at[0], qd_recv.at[j, h], partner
                ).wait_recv()

                @pl.when(even)
                def _(h=h):
                    relay_part(j, h).start()

            wq[0, rows_of(j)] = qd[j]

    far_chunk(jnp.int32(0))

    far_chunk(jnp.int32(1))
    for i in range(2):
        kv_arrival(i).wait_recv()

    column = lax.broadcasted_iota(jnp.int32, (capacity, tokens), 1).astype(jnp.float32)

    def all_of(a, g):
        return a[g].reshape(2 * context, width)

    def window(table, g):
        return pl.ds(table[0, TABLE + g], per_block)

    def masked(bias):
        def of(g):
            limit = flat(pos[window(at_own, g)]) + bias
            limit = jnp.concatenate([limit] * (tokens // LANES), axis=1)

            def mask(x):
                free = x.shape[1] - tokens
                tail = jnp.where(column <= limit, x[:, free:], jnp.float32(LOW))
                return jnp.concatenate([x[:, :free], tail], axis=1)

            return mask

        return of

    first = masked(jnp.where(k == 1, jnp.float32(0), jnp.float32(2 * tokens)))
    second = masked(jnp.where(k == 0, jnp.float32(0), jnp.float32(2 * tokens)))

    def queries_of(which, g):
        at = jnp.where(which == 1, at_own[0, TABLE + g], at_d[0, TABLE + g])
        return flat(wq[which, pl.ds(at, per_block)])

    def both_shards(g):
        return attend(queries_of(k, g), all_of(kall, g), all_of(vall, g), scale, first(g))

    def one_shard(g):
        return attend(queries_of(1 - k, g), kall[g, k], vall[g, k], scale, second(g))

    def nearer(g):
        return attend(flat(wc[window(at_c, g)]), all_of(kall, g), all_of(vall, g), scale)

    def gather(ref, table, j, *lead):
        return jnp.concatenate([ref[(*lead, table[0, j * per_block + b])] for b in range(per_block)], axis=0)

    def c_near(g):
        return (
            remote(oc.at[g], rc.at[g], oc_send.at[0], rc_recv.at[g], mate),
            remote(tc.at[g], sc.at[g], tc_send.at[0], sc_recv.at[g], mate),
        )

    def c_relay(g):
        return (
            remote(oc.at[g], rx.at[g], oc_send.at[0], rx_recv.at[g], mate),
            remote(tc.at[g], sx.at[g], tc_send.at[0], sx_recv.at[g], mate),
        )

    def d_copies(g):
        return (
            remote(od.at[g], rd.at[g], od_send.at[0], rd_recv.at[g], up),
            remote(td.at[g], sd.at[g], td_send.at[0], sd_recv.at[g], up),
        )

    pair = 2
    steps = groups // pair

    def complete(p):
        if p == steps - 1:
            return chunks
        return max(0, tokens * routed - capacity * (groups - pair * (p + 1))) // capacity

    def pick(values, i):
        out_ = jnp.int32(values[-1])
        for at, value in enumerate(values[:-1]):
            out_ = jnp.where(i == at, jnp.int32(value), out_)
        return out_

    ends = [complete(p) for p in range(steps)]
    begins = [0] + ends[:-1]
    comes = [min(pair * p, chunks) for p in range(steps + 1)]

    def arrive_near(i):
        @pl.when(feeds)
        def _():
            def one(j):
                for h in range(halves):
                    remote(
                        qc.at[j, part_of(h)], qc.at[j, part_of(h)], qn_send.at[0], qc_recv.at[j, h], partner
                    ).wait_recv()
                wc[rows_of(j)] = qc[j]

            each(pick(comes[:-1], i), pick(comes[1:], i), one)

    loose = (chunks - 1) // pair - 1

    def far_results(i):
        @pl.when(jnp.logical_and(odd, above))
        def _():
            def one(j):
                od[j] = gather(op, at_d, j, 0).astype(jnp.bfloat16)
                td[j] = squeeze(gather(lp, at_d, j, 0), padded)

                @pl.when(i >= loose)
                def _():
                    start(d_copies(j))

            each(pick(begins, i), pick(ends, i), one)

    def near_results(i, free):
        def one(j):
            oc[j] = gather(cp, at_c, j)
            tc[j] = squeeze(gather(lc, at_c, j), padded)

            @pl.when(odd)
            def _():
                @pl.when(feeds)
                def _():
                    start(c_relay(j))

            @pl.when(jnp.logical_and(even, free))
            def _():
                start(c_near(j))

        each(pick(begins, i), pick(ends, i), one)

    def block_far(i):
        got = []
        for u in range(pair):
            g = i * pair + u
            got.append((k, g, both_shards(g)))
            got.append((1 - k, g, one_shard(g)))
        for at, g, (o, lse) in got:
            op[at, rows_of(g)] = split(o)
            lp[at, rows_of(g)] = split(lse)

    def block_near(i):
        got = [(i * pair + u, nearer(i * pair + u)) for u in range(pair)]
        for g, (o, lse) in got:
            cp[rows_of(g)] = split(o.astype(jnp.bfloat16))
            lc[rows_of(g)] = split(lse)

    @pl.when(feeds)
    def _():
        remote(tab, tab_c, tab_near.at[0], tab_near.at[1], partner).wait_recv()

    @pl.when(jnp.logical_not(feeds))
    def _():
        tab_c[...] = tab[...]

    local[2].start()
    local[2].wait()

    def join(g):
        @pl.when(jnp.logical_and(jnp.logical_and(even, above), g < chunks))
        def _():
            remote(oc.at[g], rx.at[g], oc_send.at[0], rx_recv.at[g], partner).wait_recv()
            remote(tc.at[g], sx.at[g], tc_send.at[0], sx_recv.at[g], partner).wait_recv()
            mine = (gather(op, at_d, g, 0), gather(lp, at_d, g, 0))
            o, lse = merge([mine, (rx[g], widen(sx[g], capacity))])
            od[g] = o.astype(jnp.bfloat16)
            td[g] = squeeze(lse, padded)
            start(d_copies(g))

    def step(i, carry):
        block_far(i)
        far_chunk(pair * i + pair)

        @pl.when(i == loose)
        def _():
            @pl.when(jnp.logical_and(odd, above))
            def _():
                each(0, ends[loose - 1], lambda j: start(d_copies(j)))

            @pl.when(jnp.logical_and(even, above))
            def _():
                each(0, ends[loose - 1], lambda j: start(c_near(j)))

        @pl.when(i == steps - 1)
        def _():
            join(jnp.int32(0))

        arrive_near(i)
        block_near(i)
        near_results(i, jnp.logical_or(i >= loose, jnp.logical_not(above)))
        far_chunk(pair * i + pair + 1)
        far_results(i)
        return carry

    lax.fori_loop(0, steps, step, 0)

    for i in range(2):
        kv_copy(i).wait_send()

    def sent(there, *flows):
        @pl.when(there)
        def _():
            for ref, sem in flows:
                remote(ref, ref, sem.at[0], sem.at[0], partner).wait_send()

    sent(below, (qd, qd_send))
    sent(odd, (qd, qn_send))
    sent(jnp.logical_and(even, above), (qd, relay_send))

    @pl.when(below)
    def _():
        table_down().wait_send()

    @pl.when(odd)
    def _():
        table_near().wait_send()

    @pl.when(jnp.logical_and(even, above))
    def _():
        table_relay().wait_send()

    def absent(o, t):
        o[...] = jnp.zeros(o.shape, o.dtype)
        t[...] = jnp.full(t.shape, LOW, t.dtype)

    @pl.when(even)
    def _():
        absent(rc, sc)

    @pl.when(jnp.logical_not(below))
    def _():
        absent(rd, sd)

    ahead = 3
    for g in range(1, ahead):
        join(jnp.int32(g))

    def finish(g, carry):
        join(g + ahead)

        @pl.when(odd)
        def _():
            remote(oc.at[g], rc.at[g], oc_send.at[0], rc_recv.at[g], partner).wait_recv()
            remote(tc.at[g], sc.at[g], tc_send.at[0], sc_recv.at[g], partner).wait_recv()

        @pl.when(below)
        def _():
            remote(od.at[g], rd.at[g], od_send.at[0], rd_recv.at[g], partner).wait_recv()
            remote(td.at[g], sd.at[g], td_send.at[0], sd_recv.at[g], partner).wait_recv()

        parts = [
            (gather(op, at_own, g, 1), gather(lp, at_own, g, 1)),
            (rc[g], widen(sc[g], capacity)),
            (rd[g], widen(sd[g], capacity)),
        ]
        fin[pl.ds(pl.multiple_of(g * capacity, BLOCK), capacity), :] = merge(parts)[0].astype(jnp.bfloat16)
        return carry

    sent(jnp.logical_and(odd, feeds), (oc, oc_send), (tc, tc_send))

    tile = 256
    tiles = fin.shape[0] // tile
    fin[pl.ds(chunks * capacity, tiles * tile - chunks * capacity), :] = jnp.zeros(
        (tiles * tile - chunks * capacity, width), fin.dtype
    )
    lane = lax.broadcasted_iota(jnp.int32, (tokens, tile), 1).astype(jnp.float32)
    done = 0
    stops = [*range(2, chunks, 2), chunks]
    for s, stop in enumerate(stops):
        lax.fori_loop(stops[s - 1] if s else 0, stop, finish, 0)
        last = stop == chunks
        upto = tiles if last else stop * capacity // tile
        for r in range(routed):
            slot = jnp.broadcast_to(slots[:, r : r + 1], (tokens, tile))
            here = jnp.concatenate(
                [
                    (lane + t * tile == slot).astype(jnp.float32).astype(jnp.bfloat16)
                    for t in range(done, upto)
                ],
                axis=1,
            )
            part_sum = dot(here, fin[done * tile : upto * tile, :])
            total = part_sum if s == 0 else acc[r] + part_sum
            if last:
                wide[pl.ds(r, tokens, stride=routed), :] = total
            else:
                acc[r] = total
        done = upto
    out[...] = wide[pl.ds(0, tokens * routed), :].reshape(tokens, routed, width).astype(jnp.bfloat16)

    sent(above, (od, od_send), (td, td_send))
    sent(even, (oc, oc_send), (tc, tc_send))


def shards(n, queries, keys, values, routes):
    tokens, routed, width = queries.shape
    context, groups, _ = keys.shape
    capacity = HEADS // groups * MOST
    padded = -(-capacity // LANES) * LANES
    count = -(-(tokens * routed + groups * BLOCK) // capacity)
    cut = (groups * capacity // BLOCK, BLOCK, width)
    vmem = pl.BlockSpec(memory_space=pltpu.VMEM)
    hbm = pl.BlockSpec(memory_space=pltpu.HBM)
    bf = lambda *shape: pltpu.VMEM(shape, jnp.bfloat16)
    f32 = lambda *shape: pltpu.VMEM(shape, jnp.float32)
    sem = lambda *shape: pltpu.SemaphoreType.DMA(shape)
    table = lambda: pltpu.VMEM((1, 2 * TABLE), jnp.int32)
    scalars = lambda: pltpu.SMEM((1, 2 * TABLE), jnp.int32)
    chunks = lambda: bf(count, capacity, width)
    stats = lambda: f32(count, 1, padded)
    return pl.pallas_call(
        functools.partial(kernel, n),
        out_shape=jax.ShapeDtypeStruct((tokens, routed, width), jnp.bfloat16),
        in_specs=[hbm] * 4,
        out_specs=vmem,
        scratch_shapes=[
            bf(tokens, routed, width), pltpu.VMEM((routed, tokens), jnp.int32),
            bf(2, context, groups, width), f32(max(tokens * routed, LANES * groups), width), bf(routed * tokens, 2 * width),
            f32(routed, tokens), f32(tokens, LANES), bf(2, *cut), bf(*cut), f32(*cut),
            bf(groups, 2, context, width), bf(groups, 2, context, width),
            table(), table(), table(), scalars(), scalars(), scalars(),
            bf(count, capacity // BLOCK, BLOCK, width), bf(count, capacity // BLOCK, BLOCK, width),
            f32(2, *cut), f32(2, *cut), bf(*cut), f32(*cut),
            chunks(), stats(), chunks(), stats(),
            chunks(), stats(), chunks(), stats(), chunks(), stats(),
            bf(-(-count * capacity // 256) * 256, width), f32(routed, tokens, width),
        ] + [sem(2), sem(3), sem(2), sem(2), sem(1)] + [sem(2)] * 3
        + [sem(1)] * 2 + [sem(count, 2)] * 2 + [sem(1)] * 5 + [sem(count)] * 6,
        compiler_params=pltpu.CompilerParams(
            collective_id=0, has_side_effects=True, vmem_limit_bytes=48 * 1024 * 1024
        ),
        name="fused",
    )(*(pltpu.with_memory_space_constraint(a, pltpu.HBM) for a in (queries, routes.T, keys, values)))


def solution(mesh):
    n = mesh.shape["seq"]
    placed = (P("seq", None, None), P("seq", None, None), P("seq", None, None), P("seq", None))
    return jax.shard_map(
        functools.partial(shards, n),
        mesh=mesh,
        in_specs=placed,
        out_specs=P("seq", None, None),
        check_vma=False,
    )
```

```python
import functools
import math

import jax
import jax.numpy as jnp
from jax import lax
from jax.experimental import pallas as pl
from jax.experimental.pallas import tpu as pltpu
from jax.sharding import PartitionSpec as P

HEADS = 64
MOST = 40
LANES = 128
LOW = -1e30
BLOCK = 16
TABLE = 256
MESH = pl.DeviceIdType.MESH


def dot(a, b):
    return lax.dot_general(a, b, (((1,), (0,)), ((), ())), preferred_element_type=jnp.float32)


def dot_t(a, b):
    return lax.dot_general(a, b, (((1,), (1,)), ((), ())), preferred_element_type=jnp.float32)


def remote(src, dst, send, recv, device):
    return pltpu.make_async_remote_copy(
        src_ref=src, dst_ref=dst, send_sem=send, recv_sem=recv,
        device_id=(device,), device_id_type=MESH,
    )


def attend(q, k, v, scale, mask=None):
    s = dot_t(q, k) * scale
    if mask is not None:
        s = mask(s)
    top = jnp.max(s, axis=1, keepdims=True)
    p = jnp.exp2(s - top).astype(jnp.bfloat16)
    ones = jnp.ones(v.shape, jnp.bfloat16)
    both = dot(p, jnp.concatenate([v, ones], axis=1))
    width = v.shape[1]
    total = both[:, width:]
    return both[:, :width] / total, top + jnp.log2(total)


def squeeze(lse, padded):
    rows = lse.shape[0]
    return jnp.concatenate([lse, jnp.zeros((padded - rows, LANES), jnp.float32)], axis=0).T[:1]


def widen(row, rows):
    return jnp.concatenate([jnp.broadcast_to(row, (8, row.shape[1]))] * (LANES // 8), axis=0).T[:rows]


def merge(parts):
    top = functools.reduce(jnp.maximum, [lse for _, lse in parts])
    weights = [jnp.exp2(lse - top) for _, lse in parts]
    total = functools.reduce(jnp.add, weights)
    mixed = functools.reduce(jnp.add, [o.astype(jnp.float32) * w for (o, _), w in zip(parts, weights)])
    return mixed / total, top + jnp.log2(total)


def kernel(
    n, q_hbm, routes_hbm, k_hbm, v_hbm, out,
    q_in, routes_t, raw, wide, rights, slot_rows, slots, wq, wc, pos, kall, vall,
    tab, tab_d, tab_c, at_own, at_d, at_c,
    qd, qc, op, lp, cp, lc, oc, tc, od, td, rx, sx, rc, sc, rd, sd, fin, acc,
    in_sem, tab_sem, tab_far, tab_near, tab_relay, raw_sem, kv_send, kv_recv, qn_send, qd_send, qc_recv, qd_recv, relay_send,
    oc_send, tc_send, od_send, td_send,
    rx_recv, sx_recv, rc_recv, sc_recv, rd_recv, sd_recv,
):
    tokens, routed, width = q_in.shape
    groups = kall.shape[0]
    chunks, per_block = qd.shape[:2]
    capacity = per_block * BLOCK
    context = kall.shape[2]
    padded = tc.shape[2]
    per_group = HEADS // groups
    chips = n // 2
    me = lax.axis_index("seq")
    c = me // 2
    k = me % 2
    partner = c * 2 + 1 - k
    even = c % 2 == 0
    odd = c % 2 == 1
    scale = jnp.float32(math.log2(math.e) / math.sqrt(width))
    below = c >= 2
    above = c + 2 < chips
    mate = jnp.where(even, c + 1, c - 1) * 2 + k
    feeds = jnp.logical_or(even, c + 1 < chips)
    down = (c - 2) * 2 + k
    up = (c + 2) * 2 + k

    barrier = pltpu.get_barrier_semaphore()

    def signal(device):
        pl.semaphore_signal(barrier, inc=1, device_id=(device,), device_id_type=MESH)

    signal(partner)
    signal(mate)

    @pl.when(below)
    def _():
        signal(down)

    @pl.when(above)
    def _():
        signal(up)

    ins = [
        pltpu.make_async_copy(a, b, in_sem.at[i])
        for i, (a, b) in enumerate(((routes_hbm, routes_t), (q_hbm, q_in)))
    ]
    raws = [pltpu.make_async_copy(a, raw.at[i], raw_sem.at[i]) for i, a in enumerate((k_hbm, v_hbm))]
    for one in ins:
        one.start()
    ins[0].wait()

    group_of = routes_t[...] // per_group
    group = lax.broadcasted_iota(jnp.int32, (groups, tokens), 0)
    hots = [(group_of[r : r + 1] == group).astype(jnp.float32) for r in range(routed)]
    count = functools.reduce(jnp.add, hots)
    row = lax.broadcasted_iota(jnp.int32, (tokens, tokens), 0)
    col = lax.broadcasted_iota(jnp.int32, (tokens, tokens), 1)
    upper = (row < col).astype(jnp.float32).astype(jnp.bfloat16)
    many = functools.reduce(
        jnp.add, [(group_of[r : r + 1] == group).astype(jnp.int32) for r in range(routed)]
    )
    blocks = (jnp.sum(many, axis=1, keepdims=True) + (BLOCK - 1)) // BLOCK
    blocks = jnp.broadcast_to(blocks, (groups, TABLE))
    starts = [jnp.zeros((1, TABLE), jnp.int32)]
    for g in range(1, groups):
        starts.append(starts[-1] + blocks[g - 1 : g])
    place = lax.broadcasted_iota(jnp.int32, (1, TABLE), 1)
    source = place
    first_block = starts[0]
    for g in range(1, groups):
        source = source + jnp.where(place >= starts[g], per_block - blocks[g - 1 : g], 0)
        first_block = jnp.where(place >= g, starts[g], first_block)
    source = jnp.minimum(source, groups * per_block - 1)
    first_block = jnp.minimum(first_block, chunks * per_block)
    tab[...] = jnp.concatenate([source, first_block], axis=1)
    base = jnp.concatenate(starts, axis=0)[:, :1].astype(jnp.float32) * BLOCK
    rank = dot(count.astype(jnp.bfloat16), upper) + base
    rows = []
    for r in range(routed):
        rows.append(jnp.sum(hots[r] * rank, axis=0, keepdims=True))
        rank = rank + hots[r]
    slot_all = jnp.concatenate(rows, axis=0)
    slot_rows[...] = slot_all
    slots[...] = jnp.concatenate([slot_all] * (LANES // routed), axis=0).T

    ins[1].wait()
    for one in raws:
        one.start()
    wide[pl.ds(0, tokens * routed), :] = q_in[...].astype(jnp.float32).reshape(tokens * routed, width)
    token = lax.broadcasted_iota(jnp.int32, (tokens, width), 0).astype(jnp.float32).astype(jnp.bfloat16)
    for r in range(routed):
        rights[pl.ds(r * tokens, tokens), :width] = wide[pl.ds(r, tokens, stride=routed), :].astype(jnp.bfloat16)
        rights[pl.ds(r * tokens, tokens), width:] = token


    def rows_of(j):
        return pl.ds(j * per_block, per_block)

    def split(x):
        return x.reshape(x.shape[0] // BLOCK, BLOCK, width)

    def flat(x):
        return x.reshape(x.shape[0] * BLOCK, width)

    halves = 2
    part_rows = per_block // halves

    def part_of(h):
        return pl.ds(h * part_rows, part_rows)

    def query_part(j, h):
        return wq.at[1, pl.ds(j * per_block + h * part_rows, part_rows)]

    def query_down(j):
        return [
            remote(query_part(j, h), qd.at[j, part_of(h)], qd_send.at[0], qd_recv.at[j, h], down)
            for h in range(halves)
        ]

    def query_near(j):
        return [
            remote(query_part(j, h), qc.at[j, part_of(h)], qn_send.at[0], qc_recv.at[j, h], mate)
            for h in range(halves)
        ]

    def relay_part(j, h):
        return remote(qd.at[j, part_of(h)], qc.at[j, part_of(h)], relay_send.at[0], qc_recv.at[j, h], mate)

    def relay(j):
        return [relay_part(j, h) for h in range(halves)]

    def start(copies):
        for one in copies:
            one.start()

    def table_down():
        return remote(tab, tab_d, tab_far.at[0], tab_far.at[1], down)

    def table_near():
        return remote(tab, tab_c, tab_near.at[0], tab_near.at[1], mate)

    def table_relay():
        return remote(tab_d, tab_c, tab_relay.at[0], tab_near.at[1], mate)

    place = lax.broadcasted_iota(jnp.int32, (capacity, tokens), 0).astype(jnp.float32)

    def pack_rows(g):
        at = (g * capacity).astype(jnp.float32)
        here = jnp.concatenate(
            [
                (place == slot_rows[r : r + 1] - at).astype(jnp.float32).astype(jnp.bfloat16)
                for r in range(routed)
            ],
            axis=1,
        )
        both = dot(here, rights[...])
        wq[1, rows_of(g)] = split(both[:, :width].astype(jnp.bfloat16))
        pos[rows_of(g)] = split(both[:, width:])

    def pack_send(g):
        @pl.when(below)
        def _():
            start(query_down(g))

        @pl.when(odd)
        def _():
            start(query_near(g))

    def pack(g, carry):
        pack_rows(g)
        pack_send(g)
        return carry

    pack_rows(jnp.int32(0))
    pl.semaphore_wait(barrier, 2 + below.astype(jnp.int32) + above.astype(jnp.int32))

    @pl.when(below)
    def _():
        table_down().start()

    @pl.when(odd)
    def _():
        table_near().start()

    pack_send(jnp.int32(0))
    soon = min(3, chunks)
    lax.fori_loop(1, soon, pack, 0)

    part = 128

    def turn(i, to):
        def body(s, carry):
            at = pl.multiple_of(s * part, part)
            wide[pl.ds(0, part * groups), :] = raw[i, pl.ds(at, part)].astype(jnp.float32).reshape(part * groups, width)
            for g in range(groups):
                to[g, k, pl.ds(at, part), :] = wide[pl.ds(g, part, stride=groups), :].astype(jnp.bfloat16)
            return carry

        lax.fori_loop(0, context // part, body, 0)

    def kv_copy(i):
        a = (kall, vall)[i]
        return remote(a.at[:, k], a.at[:, k], kv_send.at[i], kv_recv.at[i], partner)

    def kv_arrival(i):
        a = (kall, vall)[i]
        return remote(a.at[:, 1 - k], a.at[:, 1 - k], kv_send.at[i], kv_recv.at[i], partner)

    for i, to in enumerate((kall, vall)):
        raws[i].wait()
        turn(i, to)
        kv_copy(i).start()
    lax.fori_loop(soon, chunks, pack, 0)

    used = -(-tokens * routed // BLOCK) + groups
    last_rows = (used - (chunks - 1) * per_block) * BLOCK

    for to in (rx, rc, rd):
        to[chunks - 1, last_rows:, :] = jnp.zeros((capacity - last_rows, width), to.dtype)

    local = [
        pltpu.make_async_copy(a, b, tab_sem.at[i])
        for i, (a, b) in enumerate(((tab_d, at_d), (tab, at_own), (tab_c, at_c)))
    ]
    local[1].start()
    rest = (groups - chunks) * per_block
    wq[1, pl.ds(chunks * per_block, rest)] = jnp.zeros((rest, BLOCK, width), wq.dtype)
    pos[pl.ds(chunks * per_block, rest)] = jnp.zeros((rest, BLOCK, width), pos.dtype)
    wq[0, pl.ds(chunks * per_block, rest)] = jnp.zeros((rest, BLOCK, width), wq.dtype)
    wc[pl.ds(chunks * per_block, rest)] = jnp.zeros((rest, BLOCK, width), wc.dtype)

    @pl.when(jnp.logical_not(above))
    def _():
        wq[0] = jnp.zeros(wq.shape[1:], wq.dtype)

    @pl.when(jnp.logical_not(feeds))
    def _():
        wc[...] = jnp.zeros(wc.shape, wc.dtype)

    def each(a, b, body):
        def go(j, carry):
            body(j)
            return carry

        lax.fori_loop(a, b, go, 0)

    @pl.when(above)
    def _():
        remote(tab, tab_d, tab_far.at[0], tab_far.at[1], partner).wait_recv()

        @pl.when(even)
        def _():
            table_relay().start()

    @pl.when(jnp.logical_not(above))
    def _():
        tab_d[...] = tab[...]

    local[0].start()
    local[0].wait()
    local[1].wait()

    def far_chunk(j):
        @pl.when(jnp.logical_and(above, j < chunks))
        def _():
            for h in range(halves):
                remote(
                    qd.at[j, part_of(h)], qd.at[j, part_of(h)], qd_send.at[0], qd_recv.at[j, h], partner
                ).wait_recv()

                @pl.when(even)
                def _(h=h):
                    relay_part(j, h).start()

            wq[0, rows_of(j)] = qd[j]

    far_chunk(jnp.int32(0))

    far_chunk(jnp.int32(1))
    for i in range(2):
        kv_arrival(i).wait_recv()

    column = lax.broadcasted_iota(jnp.int32, (capacity, tokens), 1).astype(jnp.float32)

    def all_of(a, g):
        return a[g].reshape(2 * context, width)

    def window(table, g):
        return pl.ds(table[0, TABLE + g], per_block)

    def masked(bias):
        def of(g):
            limit = flat(pos[window(at_own, g)]) + bias
            limit = jnp.concatenate([limit] * (tokens // LANES), axis=1)

            def mask(x):
                free = x.shape[1] - tokens
                tail = jnp.where(column <= limit, x[:, free:], jnp.float32(LOW))
                return jnp.concatenate([x[:, :free], tail], axis=1)

            return mask

        return of

    first = masked(jnp.where(k == 1, jnp.float32(0), jnp.float32(2 * tokens)))
    second = masked(jnp.where(k == 0, jnp.float32(0), jnp.float32(2 * tokens)))

    def queries_of(which, g):
        at = jnp.where(which == 1, at_own[0, TABLE + g], at_d[0, TABLE + g])
        return flat(wq[which, pl.ds(at, per_block)])

    def both_shards(g):
        return attend(queries_of(k, g), all_of(kall, g), all_of(vall, g), scale, first(g))

    def one_shard(g):
        return attend(queries_of(1 - k, g), kall[g, k], vall[g, k], scale, second(g))

    def nearer(g):
        return attend(flat(wc[window(at_c, g)]), all_of(kall, g), all_of(vall, g), scale)

    def gather(ref, table, j, *lead):
        return jnp.concatenate([ref[(*lead, table[0, j * per_block + b])] for b in range(per_block)], axis=0)

    def results(o_from, t_from, o_to, t_to, o_send, t_send, o_recv, t_recv, to):
        def make(g, act):
            def go(rows):
                act(
                    remote(
                        o_from.at[g, pl.ds(0, rows)], o_to.at[g, pl.ds(0, rows)],
                        o_send.at[0], o_recv.at[g], to,
                    )
                )

            @pl.when(g < chunks - 1)
            def _():
                go(capacity)

            @pl.when(g == chunks - 1)
            def _():
                go(last_rows)

            act(remote(t_from.at[g], t_to.at[g], t_send.at[0], t_recv.at[g], to))

        return make

    c_near = results(oc, tc, rc, sc, oc_send, tc_send, rc_recv, sc_recv, mate)
    c_relay = results(oc, tc, rx, sx, oc_send, tc_send, rx_recv, sx_recv, mate)
    d_copies = results(od, td, rd, sd, od_send, td_send, rd_recv, sd_recv, up)

    def begin(one):
        one.start()

    def arrived(one):
        one.wait_recv()

    pair = 2
    steps = groups // pair

    def complete(p):
        if p == steps - 1:
            return chunks
        return max(0, tokens * routed - capacity * (groups - pair * (p + 1))) // capacity

    def pick(values, i):
        out_ = jnp.int32(values[-1])
        for at, value in enumerate(values[:-1]):
            out_ = jnp.where(i == at, jnp.int32(value), out_)
        return out_

    ends = [complete(p) for p in range(steps)]
    begins = [0] + ends[:-1]
    comes = [min(pair * p, chunks) for p in range(steps + 1)]

    def arrive_near(i):
        @pl.when(feeds)
        def _():
            def one(j):
                for h in range(halves):
                    remote(
                        qc.at[j, part_of(h)], qc.at[j, part_of(h)], qn_send.at[0], qc_recv.at[j, h], partner
                    ).wait_recv()
                wc[rows_of(j)] = qc[j]

            each(pick(comes[:-1], i), pick(comes[1:], i), one)

    loose = (chunks - 1) // pair - 1

    def far_results(i):
        @pl.when(jnp.logical_and(odd, above))
        def _():
            def one(j):
                od[j] = gather(op, at_d, j, 0).astype(jnp.bfloat16)
                td[j] = squeeze(gather(lp, at_d, j, 0), padded)

                @pl.when(i >= loose)
                def _():
                    d_copies(j, begin)

            each(pick(begins, i), pick(ends, i), one)

    def near_results(i, free):
        def one(j):
            oc[j] = gather(cp, at_c, j)
            tc[j] = squeeze(gather(lc, at_c, j), padded)

            @pl.when(odd)
            def _():
                @pl.when(feeds)
                def _():
                    c_relay(j, begin)

            @pl.when(jnp.logical_and(even, free))
            def _():
                c_near(j, begin)

        each(pick(begins, i), pick(ends, i), one)

    def block_far(i):
        got = []
        for u in range(pair):
            g = i * pair + u
            got.append((k, g, both_shards(g)))
            got.append((1 - k, g, one_shard(g)))
        for at, g, (o, lse) in got:
            op[at, rows_of(g)] = split(o)
            lp[at, rows_of(g)] = split(lse)

    def block_near(i):
        got = [(i * pair + u, nearer(i * pair + u)) for u in range(pair)]
        for g, (o, lse) in got:
            cp[rows_of(g)] = split(o.astype(jnp.bfloat16))
            lc[rows_of(g)] = split(lse)

    @pl.when(feeds)
    def _():
        remote(tab, tab_c, tab_near.at[0], tab_near.at[1], partner).wait_recv()

    @pl.when(jnp.logical_not(feeds))
    def _():
        tab_c[...] = tab[...]

    local[2].start()
    local[2].wait()

    def join(g):
        @pl.when(jnp.logical_and(jnp.logical_and(even, above), g < chunks))
        def _():
            c_relay(g, arrived)
            mine = (gather(op, at_d, g, 0), gather(lp, at_d, g, 0))
            o, lse = merge([mine, (rx[g], widen(sx[g], capacity))])
            od[g] = o.astype(jnp.bfloat16)
            td[g] = squeeze(lse, padded)
            d_copies(g, begin)

    def step(i, carry):
        block_far(i)
        far_chunk(pair * i + pair)

        @pl.when(i == loose)
        def _():
            @pl.when(jnp.logical_and(odd, above))
            def _():
                each(0, ends[loose - 1], lambda j: d_copies(j, begin))

            @pl.when(jnp.logical_and(even, above))
            def _():
                each(0, ends[loose - 1], lambda j: c_near(j, begin))

        @pl.when(i == steps - 1)
        def _():
            join(jnp.int32(0))

        arrive_near(i)
        block_near(i)
        near_results(i, jnp.logical_or(i >= loose, jnp.logical_not(above)))
        far_chunk(pair * i + pair + 1)
        far_results(i)
        return carry

    lax.fori_loop(0, steps, step, 0)

    for i in range(2):
        kv_copy(i).wait_send()

    spent = wq.at[1, pl.ds(0, used)]

    def sent(there, *flows):
        @pl.when(there)
        def _():
            for ref, sem in flows:
                remote(ref, ref, sem.at[0], sem.at[0], partner).wait_send()

    sent(below, (qd, qd_send))
    sent(odd, (qd, qn_send))
    sent(jnp.logical_and(even, above), (qd, relay_send))

    @pl.when(below)
    def _():
        table_down().wait_send()

    @pl.when(odd)
    def _():
        table_near().wait_send()

    @pl.when(jnp.logical_and(even, above))
    def _():
        table_relay().wait_send()

    def absent(o, t):
        o[...] = jnp.zeros(o.shape, o.dtype)
        t[...] = jnp.full(t.shape, LOW, t.dtype)

    @pl.when(even)
    def _():
        absent(rc, sc)

    @pl.when(jnp.logical_not(below))
    def _():
        absent(rd, sd)

    ahead = 3
    for g in range(1, ahead):
        join(jnp.int32(g))

    def finish(g, carry):
        join(g + ahead)

        @pl.when(odd)
        def _():
            c_near(g, arrived)

        @pl.when(below)
        def _():
            d_copies(g, arrived)

        parts = [
            (gather(op, at_own, g, 1), gather(lp, at_own, g, 1)),
            (rc[g], widen(sc[g], capacity)),
            (rd[g], widen(sd[g], capacity)),
        ]
        fin[pl.ds(pl.multiple_of(g * capacity, BLOCK), capacity), :] = merge(parts)[0].astype(jnp.bfloat16)
        return carry

    sent(jnp.logical_and(odd, feeds), (spent, oc_send), (tc, tc_send))

    tile = 256
    tiles = fin.shape[0] // tile
    fin[pl.ds(chunks * capacity, tiles * tile - chunks * capacity), :] = jnp.zeros(
        (tiles * tile - chunks * capacity, width), fin.dtype
    )
    lane = lax.broadcasted_iota(jnp.int32, (tokens, tile), 1).astype(jnp.float32)
    done = 0
    stops = [*range(2, chunks, 2), chunks]
    for s, stop in enumerate(stops):
        lax.fori_loop(stops[s - 1] if s else 0, stop, finish, 0)
        last = stop == chunks
        upto = tiles if last else stop * capacity // tile
        for r in range(routed):
            slot = jnp.broadcast_to(slots[:, r : r + 1], (tokens, tile))
            here = jnp.concatenate(
                [
                    (lane + t * tile == slot).astype(jnp.float32).astype(jnp.bfloat16)
                    for t in range(done, upto)
                ],
                axis=1,
            )
            part_sum = dot(here, fin[done * tile : upto * tile, :])
            total = part_sum if s == 0 else acc[r] + part_sum
            if last:
                wide[pl.ds(r, tokens, stride=routed), :] = total
            else:
                acc[r] = total
        done = upto
    out[...] = wide[pl.ds(0, tokens * routed), :].reshape(tokens, routed, width).astype(jnp.bfloat16)

    sent(above, (spent, od_send), (td, td_send))
    sent(even, (spent, oc_send), (tc, tc_send))


def shards(n, queries, keys, values, routes):
    tokens, routed, width = queries.shape
    context, groups, _ = keys.shape
    capacity = HEADS // groups * MOST
    padded = -(-capacity // LANES) * LANES
    count = -(-(tokens * routed + groups * BLOCK) // capacity)
    cut = (groups * capacity // BLOCK, BLOCK, width)
    vmem = pl.BlockSpec(memory_space=pltpu.VMEM)
    hbm = pl.BlockSpec(memory_space=pltpu.HBM)
    bf = lambda *shape: pltpu.VMEM(shape, jnp.bfloat16)
    f32 = lambda *shape: pltpu.VMEM(shape, jnp.float32)
    sem = lambda *shape: pltpu.SemaphoreType.DMA(shape)
    table = lambda: pltpu.VMEM((1, 2 * TABLE), jnp.int32)
    scalars = lambda: pltpu.SMEM((1, 2 * TABLE), jnp.int32)
    chunks = lambda: bf(count, capacity, width)
    stats = lambda: f32(count, 1, padded)
    return pl.pallas_call(
        functools.partial(kernel, n),
        out_shape=jax.ShapeDtypeStruct((tokens, routed, width), jnp.bfloat16),
        in_specs=[hbm] * 4,
        out_specs=vmem,
        scratch_shapes=[
            bf(tokens, routed, width), pltpu.VMEM((routed, tokens), jnp.int32),
            bf(2, context, groups, width), f32(max(tokens * routed, LANES * groups), width), bf(routed * tokens, 2 * width),
            f32(routed, tokens), f32(tokens, LANES), bf(2, *cut), bf(*cut), f32(*cut),
            bf(groups, 2, context, width), bf(groups, 2, context, width),
            table(), table(), table(), scalars(), scalars(), scalars(),
            bf(count, capacity // BLOCK, BLOCK, width), bf(count, capacity // BLOCK, BLOCK, width),
            f32(2, *cut), f32(2, *cut), bf(*cut), f32(*cut),
            chunks(), stats(), chunks(), stats(),
            chunks(), stats(), chunks(), stats(), chunks(), stats(),
            bf(-(-count * capacity // 256) * 256, width), f32(routed, tokens, width),
        ] + [sem(2), sem(3), sem(2), sem(2), sem(1)] + [sem(2)] * 3
        + [sem(1)] * 2 + [sem(count, 2)] * 2 + [sem(1)] * 5 + [sem(count)] * 6,
        compiler_params=pltpu.CompilerParams(
            collective_id=0, has_side_effects=True, vmem_limit_bytes=48 * 1024 * 1024
        ),
        name="fused",
    )(*(pltpu.with_memory_space_constraint(a, pltpu.HBM) for a in (queries, routes.T, keys, values)))


def solution(mesh):
    n = mesh.shape["seq"]
    placed = (P("seq", None, None), P("seq", None, None), P("seq", None, None), P("seq", None))
    return jax.shard_map(
        functools.partial(shards, n),
        mesh=mesh,
        in_specs=placed,
        out_specs=P("seq", None, None),
        check_vma=False,
    )
```

```python
import functools
import math

import jax
import jax.numpy as jnp
from jax import lax
from jax.experimental import pallas as pl
from jax.experimental.pallas import tpu as pltpu
from jax.sharding import PartitionSpec as P

HEADS = 64
MOST = 40
LANES = 128
LOW = -1e30
BLOCK = 16
TABLE = 256
MESH = pl.DeviceIdType.MESH


def dot(a, b):
    return lax.dot_general(a, b, (((1,), (0,)), ((), ())), preferred_element_type=jnp.float32)


def dot_t(a, b):
    return lax.dot_general(a, b, (((1,), (1,)), ((), ())), preferred_element_type=jnp.float32)


def remote(src, dst, send, recv, device):
    return pltpu.make_async_remote_copy(
        src_ref=src, dst_ref=dst, send_sem=send, recv_sem=recv,
        device_id=(device,), device_id_type=MESH,
    )


def attend(q, k, v, scale, mask=None):
    s = dot_t(q, k) * scale
    if mask is not None:
        s = mask(s)
    top = jnp.max(s, axis=1, keepdims=True)
    p = jnp.exp2(s - top).astype(jnp.bfloat16)
    ones = jnp.ones(v.shape, jnp.bfloat16)
    both = dot(p, jnp.concatenate([v, ones], axis=1))
    width = v.shape[1]
    total = both[:, width:]
    return both[:, :width] / total, top + jnp.log2(total)


def squeeze(lse, padded):
    rows = lse.shape[0]
    return jnp.concatenate([lse, jnp.zeros((padded - rows, LANES), jnp.float32)], axis=0).T[:1]


def widen(row, rows):
    return jnp.concatenate([jnp.broadcast_to(row, (8, row.shape[1]))] * (LANES // 8), axis=0).T[:rows]


def merge(parts):
    top = functools.reduce(jnp.maximum, [lse for _, lse in parts])
    weights = [jnp.exp2(lse - top) for _, lse in parts]
    total = functools.reduce(jnp.add, weights)
    mixed = functools.reduce(jnp.add, [o.astype(jnp.float32) * w for (o, _), w in zip(parts, weights)])
    return mixed / total, top + jnp.log2(total)


def kernel(
    n, q_hbm, routes_hbm, k_hbm, v_hbm, out,
    q_in, routes_t, raw, wide, rights, slot_rows, slots, wq, wc, pos, kall, vall,
    tab, tab_d, tab_c, at_own, at_d, at_c,
    qd, qc, op, lp, cp, lc, oc, tc, od, td, rx, sx, rc, sc, rd, sd, fin, acc,
    in_sem, tab_sem, tab_far, tab_near, tab_relay, raw_sem, kv_send, kv_recv, qn_send, qd_send, qc_recv, qd_recv, relay_send,
    oc_send, tc_send, od_send, td_send,
    rx_recv, sx_recv, rc_recv, sc_recv, rd_recv, sd_recv,
):
    tokens, routed, width = q_in.shape
    groups = kall.shape[0]
    chunks, per_block = qd.shape[:2]
    capacity = per_block * BLOCK
    context = kall.shape[2]
    padded = tc.shape[2]
    per_group = HEADS // groups
    chips = n // 2
    me = lax.axis_index("seq")
    c = me // 2
    k = me % 2
    partner = c * 2 + 1 - k
    even = c % 2 == 0
    odd = c % 2 == 1
    scale = jnp.float32(math.log2(math.e) / math.sqrt(width))
    below = c >= 2
    above = c + 2 < chips
    mate = jnp.where(even, c + 1, c - 1) * 2 + k
    feeds = jnp.logical_or(even, c + 1 < chips)
    down = (c - 2) * 2 + k
    up = (c + 2) * 2 + k

    barrier = pltpu.get_barrier_semaphore()

    def signal(device):
        pl.semaphore_signal(barrier, inc=1, device_id=(device,), device_id_type=MESH)

    signal(partner)
    signal(mate)

    @pl.when(below)
    def _():
        signal(down)

    @pl.when(above)
    def _():
        signal(up)

    ins = [
        pltpu.make_async_copy(a, b, in_sem.at[i])
        for i, (a, b) in enumerate(((routes_hbm, routes_t), (q_hbm, q_in)))
    ]
    raws = [pltpu.make_async_copy(a, raw.at[i], raw_sem.at[i]) for i, a in enumerate((k_hbm, v_hbm))]
    for one in ins:
        one.start()
    ins[0].wait()

    group_of = routes_t[...] // per_group
    group = lax.broadcasted_iota(jnp.int32, (groups, tokens), 0)
    hots = [(group_of[r : r + 1] == group).astype(jnp.float32) for r in range(routed)]
    count = functools.reduce(jnp.add, hots)
    row = lax.broadcasted_iota(jnp.int32, (tokens, tokens), 0)
    col = lax.broadcasted_iota(jnp.int32, (tokens, tokens), 1)
    upper = (row < col).astype(jnp.float32).astype(jnp.bfloat16)
    many = functools.reduce(
        jnp.add, [(group_of[r : r + 1] == group).astype(jnp.int32) for r in range(routed)]
    )
    blocks = (jnp.sum(many, axis=1, keepdims=True) + (BLOCK - 1)) // BLOCK
    blocks = jnp.broadcast_to(blocks, (groups, TABLE))
    starts = [jnp.zeros((1, TABLE), jnp.int32)]
    for g in range(1, groups):
        starts.append(starts[-1] + blocks[g - 1 : g])
    place = lax.broadcasted_iota(jnp.int32, (1, TABLE), 1)
    source = place
    first_block = starts[0]
    for g in range(1, groups):
        source = source + jnp.where(place >= starts[g], per_block - blocks[g - 1 : g], 0)
        first_block = jnp.where(place >= g, starts[g], first_block)
    source = jnp.minimum(source, groups * per_block - 1)
    first_block = jnp.minimum(first_block, chunks * per_block)
    tab[...] = jnp.concatenate([source, first_block], axis=1)
    base = jnp.concatenate(starts, axis=0)[:, :1].astype(jnp.float32) * BLOCK
    rank = dot(count.astype(jnp.bfloat16), upper) + base
    rows = []
    for r in range(routed):
        rows.append(jnp.sum(hots[r] * rank, axis=0, keepdims=True))
        rank = rank + hots[r]
    slot_all = jnp.concatenate(rows, axis=0)
    slot_rows[...] = slot_all
    slots[...] = jnp.concatenate([slot_all] * (LANES // routed), axis=0).T

    ins[1].wait()
    for one in raws:
        one.start()
    wide[pl.ds(0, tokens * routed), :] = q_in[...].astype(jnp.float32).reshape(tokens * routed, width)
    token = lax.broadcasted_iota(jnp.int32, (tokens, width), 0).astype(jnp.float32).astype(jnp.bfloat16)
    for r in range(routed):
        rights[pl.ds(r * tokens, tokens), :width] = wide[pl.ds(r, tokens, stride=routed), :].astype(jnp.bfloat16)
        rights[pl.ds(r * tokens, tokens), width:] = token


    def rows_of(j):
        return pl.ds(j * per_block, per_block)

    def split(x):
        return x.reshape(x.shape[0] // BLOCK, BLOCK, width)

    def flat(x):
        return x.reshape(x.shape[0] * BLOCK, width)

    halves = 4
    part_rows = per_block // halves

    def part_of(h):
        return pl.ds(h * part_rows, part_rows)

    def query_part(j, h):
        return wq.at[1, pl.ds(j * per_block + h * part_rows, part_rows)]

    def query_down(j):
        return [
            remote(query_part(j, h), qd.at[j, part_of(h)], qd_send.at[0], qd_recv.at[j, h], down)
            for h in range(halves)
        ]

    def query_near(j):
        return [
            remote(query_part(j, h), qc.at[j, part_of(h)], qn_send.at[0], qc_recv.at[j, h], mate)
            for h in range(halves)
        ]

    def relay_part(j, h):
        return remote(qd.at[j, part_of(h)], qc.at[j, part_of(h)], relay_send.at[0], qc_recv.at[j, h], mate)

    def relay(j):
        return [relay_part(j, h) for h in range(halves)]

    def start(copies):
        for one in copies:
            one.start()

    def table_down():
        return remote(tab, tab_d, tab_far.at[0], tab_far.at[1], down)

    def table_near():
        return remote(tab, tab_c, tab_near.at[0], tab_near.at[1], mate)

    def table_relay():
        return remote(tab_d, tab_c, tab_relay.at[0], tab_near.at[1], mate)

    place = lax.broadcasted_iota(jnp.int32, (capacity, tokens), 0).astype(jnp.float32)

    def pack_rows(g):
        at = (g * capacity).astype(jnp.float32)
        here = jnp.concatenate(
            [
                (place == slot_rows[r : r + 1] - at).astype(jnp.float32).astype(jnp.bfloat16)
                for r in range(routed)
            ],
            axis=1,
        )
        both = dot(here, rights[...])
        wq[1, rows_of(g)] = split(both[:, :width].astype(jnp.bfloat16))
        pos[rows_of(g)] = split(both[:, width:])

    def pack_send(g):
        @pl.when(below)
        def _():
            start(query_down(g))

        @pl.when(odd)
        def _():
            start(query_near(g))

    def pack(g, carry):
        pack_rows(g)
        pack_send(g)
        return carry

    pack_rows(jnp.int32(0))
    pl.semaphore_wait(barrier, 2 + below.astype(jnp.int32) + above.astype(jnp.int32))

    @pl.when(below)
    def _():
        table_down().start()

    @pl.when(odd)
    def _():
        table_near().start()

    pack_send(jnp.int32(0))
    soon = min(3, chunks)
    lax.fori_loop(1, soon, pack, 0)

    part = 128

    def turn(i, to):
        def body(s, carry):
            at = pl.multiple_of(s * part, part)
            wide[pl.ds(0, part * groups), :] = raw[i, pl.ds(at, part)].astype(jnp.float32).reshape(part * groups, width)
            for g in range(groups):
                to[g, k, pl.ds(at, part), :] = wide[pl.ds(g, part, stride=groups), :].astype(jnp.bfloat16)
            return carry

        lax.fori_loop(0, context // part, body, 0)

    def kv_copy(i):
        a = (kall, vall)[i]
        return remote(a.at[:, k], a.at[:, k], kv_send.at[i], kv_recv.at[i], partner)

    def kv_arrival(i):
        a = (kall, vall)[i]
        return remote(a.at[:, 1 - k], a.at[:, 1 - k], kv_send.at[i], kv_recv.at[i], partner)

    for i, to in enumerate((kall, vall)):
        raws[i].wait()
        turn(i, to)
        kv_copy(i).start()
    lax.fori_loop(soon, chunks, pack, 0)

    used = -(-tokens * routed // BLOCK) + groups
    last_rows = (used - (chunks - 1) * per_block) * BLOCK

    for to in (rx, rc, rd):
        to[chunks - 1, last_rows:, :] = jnp.zeros((capacity - last_rows, width), to.dtype)

    local = [
        pltpu.make_async_copy(a, b, tab_sem.at[i])
        for i, (a, b) in enumerate(((tab_d, at_d), (tab, at_own), (tab_c, at_c)))
    ]
    local[1].start()
    rest = (groups - chunks) * per_block
    wq[1, pl.ds(chunks * per_block, rest)] = jnp.zeros((rest, BLOCK, width), wq.dtype)
    pos[pl.ds(chunks * per_block, rest)] = jnp.zeros((rest, BLOCK, width), pos.dtype)
    wq[0, pl.ds(chunks * per_block, rest)] = jnp.zeros((rest, BLOCK, width), wq.dtype)
    wc[pl.ds(chunks * per_block, rest)] = jnp.zeros((rest, BLOCK, width), wc.dtype)

    @pl.when(jnp.logical_not(above))
    def _():
        wq[0] = jnp.zeros(wq.shape[1:], wq.dtype)

    @pl.when(jnp.logical_not(feeds))
    def _():
        wc[...] = jnp.zeros(wc.shape, wc.dtype)

    def each(a, b, body):
        def go(j, carry):
            body(j)
            return carry

        lax.fori_loop(a, b, go, 0)

    @pl.when(above)
    def _():
        remote(tab, tab_d, tab_far.at[0], tab_far.at[1], partner).wait_recv()

        @pl.when(even)
        def _():
            table_relay().start()

    @pl.when(jnp.logical_not(above))
    def _():
        tab_d[...] = tab[...]

    local[0].start()
    local[0].wait()
    local[1].wait()

    def far_chunk(j):
        @pl.when(jnp.logical_and(above, j < chunks))
        def _():
            for h in range(halves):
                remote(
                    qd.at[j, part_of(h)], qd.at[j, part_of(h)], qd_send.at[0], qd_recv.at[j, h], partner
                ).wait_recv()

                @pl.when(even)
                def _(h=h):
                    relay_part(j, h).start()

            wq[0, rows_of(j)] = qd[j]

    far_chunk(jnp.int32(0))

    far_chunk(jnp.int32(1))
    for i in range(2):
        kv_arrival(i).wait_recv()

    column = lax.broadcasted_iota(jnp.int32, (capacity, tokens), 1).astype(jnp.float32)

    def all_of(a, g):
        return a[g].reshape(2 * context, width)

    def window(table, g):
        return pl.ds(table[0, TABLE + g], per_block)

    def masked(bias):
        def of(g):
            limit = flat(pos[window(at_own, g)]) + bias
            limit = jnp.concatenate([limit] * (tokens // LANES), axis=1)

            def mask(x):
                free = x.shape[1] - tokens
                tail = jnp.where(column <= limit, x[:, free:], jnp.float32(LOW))
                return jnp.concatenate([x[:, :free], tail], axis=1)

            return mask

        return of

    first = masked(jnp.where(k == 1, jnp.float32(0), jnp.float32(2 * tokens)))
    second = masked(jnp.where(k == 0, jnp.float32(0), jnp.float32(2 * tokens)))

    def queries_of(which, g):
        at = jnp.where(which == 1, at_own[0, TABLE + g], at_d[0, TABLE + g])
        return flat(wq[which, pl.ds(at, per_block)])

    def both_shards(g):
        return attend(queries_of(k, g), all_of(kall, g), all_of(vall, g), scale, first(g))

    def one_shard(g):
        return attend(queries_of(1 - k, g), kall[g, k], vall[g, k], scale, second(g))

    def nearer(g):
        return attend(flat(wc[window(at_c, g)]), all_of(kall, g), all_of(vall, g), scale)

    def gather(ref, table, j, *lead):
        return jnp.concatenate([ref[(*lead, table[0, j * per_block + b])] for b in range(per_block)], axis=0)

    def results(o_from, t_from, o_to, t_to, o_send, t_send, o_recv, t_recv, to):
        def make(g, act):
            def go(rows):
                act(
                    remote(
                        o_from.at[g, pl.ds(0, rows)], o_to.at[g, pl.ds(0, rows)],
                        o_send.at[0], o_recv.at[g], to,
                    )
                )

            @pl.when(g < chunks - 1)
            def _():
                go(capacity)

            @pl.when(g == chunks - 1)
            def _():
                go(last_rows)

            act(remote(t_from.at[g], t_to.at[g], t_send.at[0], t_recv.at[g], to))

        return make

    c_near = results(oc, tc, rc, sc, oc_send, tc_send, rc_recv, sc_recv, mate)
    c_relay = results(oc, tc, rx, sx, oc_send, tc_send, rx_recv, sx_recv, mate)
    d_copies = results(od, td, rd, sd, od_send, td_send, rd_recv, sd_recv, up)

    def begin(one):
        one.start()

    def arrived(one):
        one.wait_recv()

    pair = 2
    steps = groups // pair

    def complete(p):
        if p == steps - 1:
            return chunks
        return max(0, tokens * routed - capacity * (groups - pair * (p + 1))) // capacity

    def pick(values, i):
        out_ = jnp.int32(values[-1])
        for at, value in enumerate(values[:-1]):
            out_ = jnp.where(i == at, jnp.int32(value), out_)
        return out_

    ends = [complete(p) for p in range(steps)]
    begins = [0] + ends[:-1]
    comes = [min(pair * p, chunks) for p in range(steps + 1)]

    def arrive_near(i):
        @pl.when(feeds)
        def _():
            def one(j):
                for h in range(halves):
                    remote(
                        qc.at[j, part_of(h)], qc.at[j, part_of(h)], qn_send.at[0], qc_recv.at[j, h], partner
                    ).wait_recv()
                wc[rows_of(j)] = qc[j]

            each(pick(comes[:-1], i), pick(comes[1:], i), one)

    loose = (chunks - 1) // pair - 1

    def far_results(i):
        @pl.when(jnp.logical_and(odd, above))
        def _():
            def one(j):
                od[j] = gather(op, at_d, j, 0).astype(jnp.bfloat16)
                td[j] = squeeze(gather(lp, at_d, j, 0), padded)

                @pl.when(i >= loose)
                def _():
                    d_copies(j, begin)

            each(pick(begins, i), pick(ends, i), one)

    def near_results(i, free):
        def one(j):
            oc[j] = gather(cp, at_c, j)
            tc[j] = squeeze(gather(lc, at_c, j), padded)

            @pl.when(odd)
            def _():
                @pl.when(feeds)
                def _():
                    c_relay(j, begin)

            @pl.when(jnp.logical_and(even, free))
            def _():
                c_near(j, begin)

        each(pick(begins, i), pick(ends, i), one)

    def block_far(i):
        got = []
        for u in range(pair):
            g = i * pair + u
            got.append((k, g, both_shards(g)))
            got.append((1 - k, g, one_shard(g)))
        for at, g, (o, lse) in got:
            op[at, rows_of(g)] = split(o)
            lp[at, rows_of(g)] = split(lse)

    def block_near(i):
        got = [(i * pair + u, nearer(i * pair + u)) for u in range(pair)]
        for g, (o, lse) in got:
            cp[rows_of(g)] = split(o.astype(jnp.bfloat16))
            lc[rows_of(g)] = split(lse)

    @pl.when(feeds)
    def _():
        remote(tab, tab_c, tab_near.at[0], tab_near.at[1], partner).wait_recv()

    @pl.when(jnp.logical_not(feeds))
    def _():
        tab_c[...] = tab[...]

    local[2].start()
    local[2].wait()

    def join(g):
        @pl.when(jnp.logical_and(jnp.logical_and(even, above), g < chunks))
        def _():
            c_relay(g, arrived)
            mine = (gather(op, at_d, g, 0), gather(lp, at_d, g, 0))
            o, lse = merge([mine, (rx[g], widen(sx[g], capacity))])
            od[g] = o.astype(jnp.bfloat16)
            td[g] = squeeze(lse, padded)
            d_copies(g, begin)

    def step(i, carry):
        block_far(i)
        far_chunk(pair * i + pair)

        @pl.when(i == loose)
        def _():
            @pl.when(jnp.logical_and(odd, above))
            def _():
                each(0, ends[loose - 1], lambda j: d_copies(j, begin))

            @pl.when(jnp.logical_and(even, above))
            def _():
                each(0, ends[loose - 1], lambda j: c_near(j, begin))

        @pl.when(i == steps - 1)
        def _():
            join(jnp.int32(0))

        arrive_near(i)
        block_near(i)
        near_results(i, jnp.logical_or(i >= loose, jnp.logical_not(above)))
        far_chunk(pair * i + pair + 1)
        far_results(i)
        return carry

    lax.fori_loop(0, steps, step, 0)

    for i in range(2):
        kv_copy(i).wait_send()

    spent = wq.at[1, pl.ds(0, used)]

    def sent(there, *flows):
        @pl.when(there)
        def _():
            for ref, sem in flows:
                remote(ref, ref, sem.at[0], sem.at[0], partner).wait_send()

    sent(below, (qd, qd_send))
    sent(odd, (qd, qn_send))
    sent(jnp.logical_and(even, above), (qd, relay_send))

    @pl.when(below)
    def _():
        table_down().wait_send()

    @pl.when(odd)
    def _():
        table_near().wait_send()

    @pl.when(jnp.logical_and(even, above))
    def _():
        table_relay().wait_send()

    def absent(o, t):
        o[...] = jnp.zeros(o.shape, o.dtype)
        t[...] = jnp.full(t.shape, LOW, t.dtype)

    @pl.when(even)
    def _():
        absent(rc, sc)

    @pl.when(jnp.logical_not(below))
    def _():
        absent(rd, sd)

    ahead = 3
    for g in range(1, ahead):
        join(jnp.int32(g))

    def finish(g, carry):
        join(g + ahead)

        @pl.when(odd)
        def _():
            c_near(g, arrived)

        @pl.when(below)
        def _():
            d_copies(g, arrived)

        parts = [
            (gather(op, at_own, g, 1), gather(lp, at_own, g, 1)),
            (rc[g], widen(sc[g], capacity)),
            (rd[g], widen(sd[g], capacity)),
        ]
        fin[pl.ds(pl.multiple_of(g * capacity, BLOCK), capacity), :] = merge(parts)[0].astype(jnp.bfloat16)
        return carry

    sent(jnp.logical_and(odd, feeds), (spent, oc_send), (tc, tc_send))

    tile = 256
    tiles = fin.shape[0] // tile
    fin[pl.ds(chunks * capacity, tiles * tile - chunks * capacity), :] = jnp.zeros(
        (tiles * tile - chunks * capacity, width), fin.dtype
    )
    lane = lax.broadcasted_iota(jnp.int32, (tokens, tile), 1).astype(jnp.float32)
    done = 0
    stops = [*range(2, chunks, 2), chunks]
    for s, stop in enumerate(stops):
        lax.fori_loop(stops[s - 1] if s else 0, stop, finish, 0)
        last = stop == chunks
        upto = tiles if last else stop * capacity // tile
        for r in range(routed):
            slot = jnp.broadcast_to(slots[:, r : r + 1], (tokens, tile))
            here = jnp.concatenate(
                [
                    (lane + t * tile == slot).astype(jnp.float32).astype(jnp.bfloat16)
                    for t in range(done, upto)
                ],
                axis=1,
            )
            part_sum = dot(here, fin[done * tile : upto * tile, :])
            total = part_sum if s == 0 else acc[r] + part_sum
            if last:
                wide[pl.ds(r, tokens, stride=routed), :] = total
            else:
                acc[r] = total
        done = upto
    out[...] = wide[pl.ds(0, tokens * routed), :].reshape(tokens, routed, width).astype(jnp.bfloat16)

    sent(above, (spent, od_send), (td, td_send))
    sent(even, (spent, oc_send), (tc, tc_send))


def shards(n, queries, keys, values, routes):
    tokens, routed, width = queries.shape
    context, groups, _ = keys.shape
    capacity = HEADS // groups * MOST
    padded = -(-capacity // LANES) * LANES
    count = -(-(tokens * routed + groups * BLOCK) // capacity)
    cut = (groups * capacity // BLOCK, BLOCK, width)
    vmem = pl.BlockSpec(memory_space=pltpu.VMEM)
    hbm = pl.BlockSpec(memory_space=pltpu.HBM)
    bf = lambda *shape: pltpu.VMEM(shape, jnp.bfloat16)
    f32 = lambda *shape: pltpu.VMEM(shape, jnp.float32)
    sem = lambda *shape: pltpu.SemaphoreType.DMA(shape)
    table = lambda: pltpu.VMEM((1, 2 * TABLE), jnp.int32)
    scalars = lambda: pltpu.SMEM((1, 2 * TABLE), jnp.int32)
    chunks = lambda: bf(count, capacity, width)
    stats = lambda: f32(count, 1, padded)
    return pl.pallas_call(
        functools.partial(kernel, n),
        out_shape=jax.ShapeDtypeStruct((tokens, routed, width), jnp.bfloat16),
        in_specs=[hbm] * 4,
        out_specs=vmem,
        scratch_shapes=[
            bf(tokens, routed, width), pltpu.VMEM((routed, tokens), jnp.int32),
            bf(2, context, groups, width), f32(max(tokens * routed, LANES * groups), width), bf(routed * tokens, 2 * width),
            f32(routed, tokens), f32(tokens, LANES), bf(2, *cut), bf(*cut), f32(*cut),
            bf(groups, 2, context, width), bf(groups, 2, context, width),
            table(), table(), table(), scalars(), scalars(), scalars(),
            bf(count, capacity // BLOCK, BLOCK, width), bf(count, capacity // BLOCK, BLOCK, width),
            f32(2, *cut), f32(2, *cut), bf(*cut), f32(*cut),
            chunks(), stats(), chunks(), stats(),
            chunks(), stats(), chunks(), stats(), chunks(), stats(),
            bf(-(-count * capacity // 256) * 256, width), f32(routed, tokens, width),
        ] + [sem(2), sem(3), sem(2), sem(2), sem(1)] + [sem(2)] * 3
        + [sem(1)] * 2 + [sem(count, 4)] * 2 + [sem(1)] * 5 + [sem(count)] * 6,
        compiler_params=pltpu.CompilerParams(
            collective_id=0, has_side_effects=True, vmem_limit_bytes=48 * 1024 * 1024
        ),
        name="fused",
    )(*(pltpu.with_memory_space_constraint(a, pltpu.HBM) for a in (queries, routes.T, keys, values)))


def solution(mesh):
    n = mesh.shape["seq"]
    placed = (P("seq", None, None), P("seq", None, None), P("seq", None, None), P("seq", None))
    return jax.shard_map(
        functools.partial(shards, n),
        mesh=mesh,
        in_specs=placed,
        out_specs=P("seq", None, None),
        check_vma=False,
    )
```
